32 devices in a mesh: gx: 2 (over y), gy: 4 (over x, core), gz: 4 (over z).
Axes of the slice: x: 2, y: 2, z: 4, core: 2. Of those that a mesh axis runs over, the one named last changes fastest.
Arguments:
- rhs_velocity: float32 [3, 8, 32, 512], P(None, 'gx', 'gy', 'gz'), may hold values from -6 to 6
- rhs_pressure: float32 [8, 32, 512], P('gx', 'gy', 'gz'), may hold values from -6 to 6
- layer_ids: int32 [8, 32, 512], P('gx', 'gy', 'gz'), may hold values from 0 to 7
- visc_table: float32 [8], replicated, may hold values from 0.5 to 8
- stencil: float32 [27, 3, 3], replicated, as said below
Outputs:
- velocity_out: float32 [3, 8, 32, 512], P(None, 'gx', 'gy', 'gz')
- pressure_out: float32 [8, 32, 512], P('gx', 'gy', 'gz')
The draws below stay inside these ranges and needn't reach their ends.
Inputs may be any that keep to these rules, and one draw needn't show every extreme that they name: The block stencil[13] has a positive diagonal that dominates its row together with all other blocks' entries.
All inputs are finite; a program needn't handle non-finite values.
Results may differ from the reference program's by a relative error of at most 0.00015.
Values sent between devices are 32-bit elements; how exact they have to be, the bound alone decides.
No kernel may reach another device: no remote copies, remote signals or barrier semaphores. Data moves between devices by JAX's collectives and lax.ppermute only.
A program may use at most 64 MiB of HBM per device.

```python
import math
import jax
import jax.numpy as jnp
from jax import lax

LAYERS = 8
NX = 8
NY = 32
NZ = 512


def draw_stencil(key, part):
    key_off = jax.random.fold_in(key, 11)
    key_mid = jax.random.fold_in(key, 12)
    key_diag = jax.random.fold_in(key, 13)
    spread = 0.03
    others = jax.random.normal(key_off, (27, 3, 3), jnp.float32) * spread
    center_off = jax.random.normal(key_mid, (3, 3), jnp.float32) * 0.1
    picker = (jnp.arange(27) == 13).astype(jnp.float32)[:, None, None]
    others = others * (1.0 - picker)
    eye = jnp.eye(3, dtype=jnp.float32)
    row_mass = jnp.sum(jnp.abs(others), axis=(0, 2)) + jnp.sum(jnp.abs(center_off * (1.0 - eye)), axis=1)
    extra = jax.random.uniform(key_diag, (3,), jnp.float32, 0.0, 0.5)
    center = center_off * (1.0 - eye) + eye * (1.0 + row_mass + extra)[:, None]
    return others + picker * center[None]


def place_ends(drawn, rng, low, largest):
    shape = drawn.shape
    index_at = [jax.random.randint(jax.random.fold_in(rng, axis), (), 0, shape[axis]) for axis in range(len(shape))]
    drawn = drawn.at[tuple(index_at)].set(low)
    longest = shape.index(max(shape))
    index_at[longest] = (index_at[longest] + 1) % shape[longest]
    return drawn.at[tuple(index_at)].set(largest)


def block_scale(rng, extent, shards, low, largest):
    gain = 1.0
    for dim, shards_of in shards:
        heights = jax.random.uniform(jax.random.fold_in(jax.random.fold_in(rng, 6), dim), (shards_of,), jnp.float32, low / len(shards), largest / len(shards))
        gain = gain * jnp.repeat(jnp.exp(heights), extent[dim] // shards_of).reshape((-1,) + (1,) * (len(extent) - 1 - dim))
    return gain


def normal_values(key, dims, scale, bound, shards=(), held_as=jnp.bfloat16):
    factor_of = block_scale(key, dims, shards, -0.22, 0.18) if shards else 1.0
    values = jax.random.normal(key, dims, jnp.float32) * scale * factor_of
    return jnp.minimum(jnp.maximum(values, -bound), bound).astype(held_as)


def setup_inputs(seed: int = 0) -> dict:
    arg_keys = jax.random.split(jax.random.key(seed), 6)
    return {
        "rhs_velocity": normal_values(arg_keys[0], (3, NX, NY, NZ), 1.0, 6.0, ((1, 2), (2, 4), (3, 4)), jnp.float32),
        "rhs_pressure": normal_values(arg_keys[1], (NX, NY, NZ), 1.0, 6.0, ((0, 2), (1, 4), (2, 4)), jnp.float32),
        "layer_ids": place_ends(jax.random.randint(arg_keys[2], (NX, NY, NZ), 0, LAYERS), jax.random.fold_in(arg_keys[2], 1), 0, LAYERS - 1).astype(jnp.int32),
        "visc_table": jnp.clip(jnp.exp(jax.random.uniform(arg_keys[3], (LAYERS,), jnp.float32, math.log(0.5), math.log(8.0))), 0.5, 8.0),
        "stencil": draw_stencil(jax.random.fold_in(arg_keys[5], 71), 0),
    }


LOW_BOUND = 0.2
HIGH_BOUND = 1.8
OMEGA = 2.0 / 3.0


def cheb_consts():
    theta = (HIGH_BOUND + LOW_BOUND) / 2.0
    delta = (HIGH_BOUND - LOW_BOUND) / 2.0
    sigma = theta / delta
    rho_zero = 1.0 / sigma
    rho_one = 1.0 / (2.0 * sigma - rho_zero)
    return theta, delta, rho_zero, rho_one


def stencil_sum(padded, stencil):
    sizes = (padded.shape[1] - 2, padded.shape[2] - 2, padded.shape[3] - 2)
    total = jnp.zeros((3,) + sizes, jnp.float32)
    for first in range(3):
        for second in range(3):
            for third in range(3):
                slab = padded[:, first:first + sizes[0], second:second + sizes[1], third:third + sizes[2]]
                block = stencil[first * 9 + second * 3 + third]
                total = total + jnp.einsum("ij,jxyz->ixyz", block, slab, precision=lax.Precision.HIGHEST)
    return total


def lookup(layer_ids, visc_table):
    eta = jnp.zeros(layer_ids.shape, jnp.float32)
    for layer in range(visc_table.shape[0]):
        eta = eta + jnp.where(layer_ids == layer, visc_table[layer], 0.0)
    return eta


def apply_field(field, scale, stencil):
    padded = jnp.pad(field, ((0, 0), (1, 1), (1, 1), (1, 1)))
    return scale[None] * stencil_sum(padded, stencil)


def smooth_zero(rhs, scale, dinv, stencil):
    theta, delta, rho_zero, rho_one = cheb_consts()
    first = dinv[None] * rhs / theta
    resid = rhs - apply_field(first, scale, stencil)
    second = rho_one * rho_zero * first + (2.0 * rho_one / delta) * dinv[None] * resid
    return first + second


def coarsen(field):
    shape = field.shape
    blocks = field.reshape(shape[:-3] + (shape[-3] // 2, 2, shape[-2] // 2, 2, shape[-1] // 2, 2))
    count = len(shape)
    return jnp.mean(blocks, axis=(count - 2, count, count + 2))


def refine(field):
    return jnp.repeat(jnp.repeat(jnp.repeat(field, 2, axis=1), 2, axis=2), 2, axis=3)


def reference(rhs_velocity, rhs_pressure, layer_ids, visc_table, stencil):
    theta, delta, rho_zero, rho_one = cheb_consts()
    eta = lookup(layer_ids, visc_table)
    kc = (stencil[13, 0, 0] + stencil[13, 1, 1] + stencil[13, 2, 2]) / 3.0
    dinv = 1.0 / (eta * kc)
    smoothed = smooth_zero(rhs_velocity, eta, dinv, stencil)
    residual = rhs_velocity - apply_field(smoothed, eta, stencil)
    coarse_res = coarsen(residual)
    eta_coarse = coarsen(eta)
    scale_coarse = 0.25 * eta_coarse
    dinv_coarse = 1.0 / (scale_coarse * kc)
    correction = smooth_zero(coarse_res, scale_coarse, dinv_coarse, stencil)
    start = smoothed + refine(correction)
    resid = rhs_velocity - apply_field(start, eta, stencil)
    first = dinv[None] * resid / theta
    middle = start + first
    resid = rhs_velocity - apply_field(middle, eta, stencil)
    second = rho_one * rho_zero * first + (2.0 * rho_one / delta) * dinv[None] * resid
    velocity_out = middle + second
    weight = 1.0 / eta
    pinv = 1.0 / (6.0 * weight)
    pressure = OMEGA * pinv * rhs_pressure
    for sweep in range(2):
        padded = jnp.pad(pressure, 1)
        beside = padded[2:, 1:-1, 1:-1] + padded[:-2, 1:-1, 1:-1]
        beside = beside + padded[1:-1, 2:, 1:-1] + padded[1:-1, :-2, 1:-1]
        beside = beside + padded[1:-1, 1:-1, 2:] + padded[1:-1, 1:-1, :-2]
        applied = weight * (6.0 * pressure - beside)
        pressure = pressure + OMEGA * pinv * (rhs_pressure - applied)
    return velocity_out, pressure
```

```python
import functools

import jax
import jax.numpy as jnp
from jax import lax
from jax.experimental import pallas as pl
from jax.experimental.pallas import tpu as pltpu
from jax.sharding import PartitionSpec as P

LOW_BOUND = 0.2
HIGH_BOUND = 1.8

SUB = 8
LANES = 128
COLS = 8
REACH = 6
FIELDS = 5
PAD = 3
ROWS = 5 * SUB
OWN = 2 * SUB


def cheb_consts():
    theta = (HIGH_BOUND + LOW_BOUND) / 2.0
    delta = (HIGH_BOUND - LOW_BOUND) / 2.0
    sigma = theta / delta
    rho_zero = 1.0 / sigma
    rho_one = 1.0 / (2.0 * sigma - rho_zero)
    return (theta, delta, rho_zero, rho_one)


def first_pairs(count):
    return [(i, i ^ 1) for i in range(count) if i ^ 1 < count]


def second_pairs(count):
    pairs = []
    for i in range(1, count - 1, 2):
        pairs += [(i, i + 1), (i + 1, i)]
    return pairs


def matched(block, axis, pairs):
    if not pairs:
        return jnp.zeros_like(block)
    return lax.ppermute(block, axis, pairs)


def lane_iota():
    return lax.broadcasted_iota(jnp.int32, (SUB, LANES), 1)


def pack_kernel(planes, tab_ref, rhs_ref, press_ref, ids_ref, main_ref, a_ref, b_ref):
    lane = lane_iota()
    odd = lax.axis_index("gz") % 2 == 1
    layers = tab_ref.shape[1]
    for f in range(FIELDS):
        a_ref[f] = jnp.zeros((SUB, LANES), jnp.float32)
        b_ref[f] = jnp.zeros((SUB, LANES), jnp.float32)
    up = [jnp.zeros((SUB, LANES), jnp.float32)] * FIELDS
    down = [jnp.zeros((SUB, LANES), jnp.float32)] * FIELDS
    width = 2 * COLS
    for p in range(planes):
        ids = ids_ref[p]
        eta = jnp.zeros((SUB, LANES), jnp.float32)
        dinv = jnp.zeros((SUB, LANES), jnp.float32)
        for layer in range(layers):
            hit = ids == layer
            eta = jnp.where(hit, tab_ref[0, layer], eta)
            dinv = jnp.where(hit, tab_ref[1, layer], dinv)
        values = [rhs_ref[j, p] * dinv for j in range(3)]
        values += [eta, eta * press_ref[p] * (1.0 / 9.0)]
        for f in range(FIELDS):
            main_ref[f * planes + p] = values[f]
            high = pltpu.roll(values[f], (p * width + COLS) % LANES, 1)
            up[f] = jnp.where((lane >= p * width) & (lane < p * width + COLS), high, up[f])
            low = pltpu.roll(values[f], (p * width + COLS) % LANES, 1)
            down[f] = jnp.where(
                (lane >= p * width + COLS) & (lane < (p + 1) * width), low, down[f]
            )
    for f in range(FIELDS):
        a_ref[f] = jnp.where(odd, down[f], up[f])
        b_ref[f] = jnp.where(odd, up[f], down[f])


def tile_span(planes_from, planes_to, stride):
    first = planes_from * stride // LANES
    last = ((planes_to + 1) * stride - 1) // LANES
    return first, last - first + 1


def cycle_kernel(
    planes,
    blocks,
    paired,
    own_ref,
    a_ref,
    b_ref,
    coef_ref,
    vel_ref,
    press_ref,
    fields,
    work,
    shifted,
    second_x,
    resid,
    sums,
    press,
    out,
):
    theta, delta, rho_zero, rho_one = cheb_consts()
    weight = 2.0 * rho_one / delta
    carry = rho_one * rho_zero
    total = planes * blocks
    stride = LANES + 2 * COLS
    tiles = fields.shape[1]
    lane = lane_iota()
    zero = jnp.zeros((SUB, LANES), jnp.float32)
    gx = lax.axis_index("gx")
    y_odd = lax.axis_index("gy") % 2 == 1

    def span(grow):
        if paired:
            low = tile_span(0, min(planes - 1 + grow, total - 1), stride)
            high = tile_span(max(planes - grow, 0), total - 1, stride)
            count = max(low[1], high[1])
            return low[0] + gx * (high[0] - low[0]), count
        own = blocks // 2
        lo = max(own * planes - grow, 0)
        hi = min((own + 1) * planes - 1 + grow, total - 1)
        return tile_span(lo, hi, stride)

    def slot(q):
        return (q + gx) % 2 if paired else q

    for k in list(range(PAD)) + list(range(PAD + tiles, 2 * PAD + tiles)):
        for r in range(1, 4):
            for j in range(3):
                work[j, k, r * SUB : (r + 1) * SUB, :] = zero
            press[k, r * SUB : (r + 1) * SUB, :] = zero

    def assemble(src, row):
        for f in range(FIELDS):
            halo = {}
            for q in range(blocks):
                tile = src[slot(q), FIELDS * planes + f]
                turn = (q * planes * 2 * COLS) % LANES
                halo[q] = pltpu.roll(tile, turn, 1) if turn else tile
            mains = {}
            for k in range(tiles):
                pieces = []
                for plane in range(total):
                    q, p = divmod(plane, planes)
                    at = plane * stride
                    for kind, lo, hi in (
                        ("halo", at, at + COLS),
                        ("main", at + COLS, at + COLS + LANES),
                        ("halo", at + COLS + LANES, at + stride),
                    ):
                        lo, hi = max(lo, k * LANES), min(hi, (k + 1) * LANES)
                        if lo >= hi:
                            continue
                        if kind == "halo":
                            piece = ("halo", q)
                        else:
                            piece = ("main", plane)
                        if pieces and pieces[-1][1] == piece:
                            continue
                        pieces.append((lo - k * LANES, piece))
                if (k + 1) * LANES > total * stride:
                    pieces.append((total * stride - k * LANES, None))
                value = None
                for start, piece in pieces:
                    if piece is None:
                        tile = zero
                    elif piece[0] == "halo":
                        tile = halo[piece[1]]
                    else:
                        plane = piece[1]
                        if plane not in mains:
                            q, p = divmod(plane, planes)
                            mains[plane] = pltpu.roll(
                                src[slot(q), f * planes + p],
                                (plane * stride + COLS) % LANES,
                                1,
                            )
                        tile = mains[plane]
                    value = tile if value is None else jnp.where(lane >= start, tile, value)
                fields[f, k, row : row + SUB, :] = value
                if f < 3:
                    work[f, PAD + k, row : row + SUB, :] = value
                if f == 4:
                    press[PAD + k, row : row + SUB, :] = value

    assemble(own_ref, OWN)

    @pl.when(y_odd)
    def _():
        assemble(a_ref, OWN - SUB)
        assemble(b_ref, OWN + SUB)

    @pl.when(jnp.logical_not(y_odd))
    def _():
        assemble(b_ref, OWN - SUB)
        assemble(a_ref, OWN + SUB)

    def shift_reader(load, offset):
        jump, turn = divmod(offset, LANES)
        cache = {}

        def turned(k):
            if k not in cache:
                cache[k] = pltpu.roll(load(k), LANES - turn, 1)
            return cache[k]

        def tile(k):
            if turn == 0:
                return load(k + jump)
            return jnp.where(lane < LANES - turn, turned(k + jump), turned(k + jump + 1))

        return tile

    def make_shifts(base, count, rows, scale):
        for j in range(3):
            for row in rows:
                def load(k, j=j, row=row):
                    return work[j, PAD + base + k, row : row + SUB, :]

                readers = {}
                for a in range(3):
                    for c in range(3):
                        if (a, c) != (1, 1):
                            readers[a * 3 + c] = shift_reader(
                                load, ((a - 1) * stride + (c - 1)) * scale
                            )
                for k in range(count):
                    for n, reader in readers.items():
                        shifted[n, j, k, row : row + SUB, :] = reader(k)

    def apply(base, count, rows, scale, group, emit):
        def step(first, width):
            spots = [(first + g, row) for g in range(width) for row in rows]
            totals = [[None] * 3 for _ in spots]
            for a in range(3):
                for c in range(3):
                    for b in range(3):
                        for j in range(3):
                            values = []
                            for k, row in spots:
                                at = row + (b - 1) * scale
                                if (a, c) == (1, 1):
                                    v = work[j, PAD + base + k, at : at + SUB, :]
                                else:
                                    v = shifted[a * 3 + c, j, k, at : at + SUB, :]
                                values.append(v)
                            for i in range(3):
                                n = (9 * a + 3 * b + c) * 9 + i * 3 + j
                                coef = jnp.broadcast_to(coef_ref[n : n + 1, :], (SUB, LANES))
                                for s, v in enumerate(values):
                                    term = coef * v
                                    old = totals[s][i]
                                    totals[s][i] = term if old is None else old + term
            results = []
            for (k, row), sums_of in zip(spots, totals):
                results.append(emit(base + k, row, sums_of))
            for stores in results:
                for ref, index, value in stores:
                    ref[index] = value

        whole = count // group
        if whole > 1:
            def body(n, _):
                step(n * group, group)
                return 0

            lax.fori_loop(0, whole, body, 0)
        elif whole == 1:
            step(0, group)
        if count % group:
            step(whole * group, count % group)

    def inside(k, row):
        return fields[3, k, row : row + SUB, :] > 0.0

    def emit_first(k, row, sums_of):
        keep = inside(k, row)
        stores = []
        for i in range(3):
            f0 = fields[i, k, row : row + SUB, :]
            value = jnp.where(keep, (1.0 + carry + weight) * f0 - weight * sums_of[i], 0.0)
            stores.append((work, (i, PAD + k, pl.ds(row, SUB), slice(None)), value))
            stores.append((second_x, (i, k, pl.ds(row, SUB), slice(None)), value))
        return stores

    make_shifts(0, tiles, [OWN - SUB, OWN, OWN + SUB], 1)
    apply(0, tiles, [OWN - SUB, OWN, OWN + SUB], 1, 1, emit_first)

    def emit_resid(k, row, sums_of):
        eta = fields[3, k, row : row + SUB, :]
        stores = []
        for i in range(3):
            value = eta * (fields[i, k, row : row + SUB, :] - sums_of[i])
            at = row - (OWN - SUB // 2)
            stores.append((resid, (i, k, pl.ds(at, SUB), slice(None)), value))
        return stores

    make_shifts(0, tiles, [OWN - SUB, OWN, OWN + SUB], 1)
    apply(0, tiles, [OWN - SUB // 2, OWN + SUB // 2], 1, 1, emit_resid)

    lane_even = lane % 2 == 0
    row_even = lax.broadcasted_iota(jnp.int32, (SUB, LANES), 0) % 2 == 0
    for r in range(2):
        row = OWN - SUB // 2 + r * SUB
        for k in range(tiles):
            for f in range(4):
                if f < 3:
                    v = resid[f, k, r * SUB : (r + 1) * SUB, :]
                else:
                    v = fields[3, k, row : row + SUB, :]
                v = v + jnp.where(row_even, pltpu.roll(v, SUB - 1, 0), pltpu.roll(v, 1, 0))
                v = v + jnp.where(lane_even, pltpu.roll(v, LANES - 1, 1), pltpu.roll(v, 1, 1))
                sums[f, k, r * SUB : (r + 1) * SUB, :] = v
        scale_at = {}
        for f in (3, 0, 1, 2):
            def load(k, f=f, r=r):
                if 0 <= k < tiles:
                    return sums[f, k, r * SUB : (r + 1) * SUB, :]
                return zero

            ahead, behind = shift_reader(load, stride), shift_reader(load, -stride)
            for k in range(tiles):
                plane = k * LANES // stride
                edge = (plane + 1) * stride - k * LANES
                near, far = (ahead(k), behind(k))
                if plane % 2:
                    near, far = far, near
                other = jnp.where(lane < edge, near, far) if edge < LANES else near
                v = load(k) + other
                if f == 3:
                    scale_at[k] = jnp.where(v > 0.0, 4.0 / v, 0.0)
                else:
                    work[f, PAD + k, row : row + SUB, :] = v * scale_at[k]

    def emit_start(k, row, sums_of):
        keep = inside(k, row)
        stores = []
        for i in range(3):
            fc = work[i, PAD + k, row : row + SUB, :]
            value = second_x[i, k, row : row + SUB, :] + (1.0 + carry + weight) * fc
            value = jnp.where(keep, value - weight * sums_of[i], 0.0)
            stores.append((work, (i, PAD + k, pl.ds(row, SUB), slice(None)), value))
        return stores

    base, count = span(2)
    make_shifts(base, count, [OWN - SUB // 2, OWN + SUB // 2], 2)
    apply(base, count, [OWN - 2, OWN - 2 + SUB], 2, 1, emit_start)

    def emit_middle(k, row, sums_of):
        keep = inside(k, row)
        stores = []
        for i in range(3):
            step = jnp.where(keep, fields[i, k, row : row + SUB, :] - sums_of[i], 0.0)
            value = work[i, PAD + k, row : row + SUB, :] + step
            stores.append((work, (i, PAD + k, pl.ds(row, SUB), slice(None)), value))
            stores.append((second_x, (i, k, pl.ds(row, SUB), slice(None)), step))
        return stores

    base, count = span(1)
    make_shifts(base, count, [OWN - 2, OWN - 2 + SUB], 1)
    apply(base, count, [OWN - 1, OWN - 1 + SUB], 1, 2, emit_middle)
    press_base, press_count = base, count

    base, count = span(0)

    def emit_last(k, row, sums_of):
        stores = []
        for i in range(3):
            value = work[i, PAD + k, row : row + SUB, :]
            value = value + carry * second_x[i, k, row : row + SUB, :]
            value = value + weight * (fields[i, k, row : row + SUB, :] - sums_of[i])
            stores.append((out, (i, k - base), value))
        return stores

    make_shifts(base, count, [OWN - 1, OWN + 1], 1)
    apply(base, count, [OWN], 1, count, emit_last)

    def beside(base, row):
        def load(k):
            return press[PAD + base + k, row : row + SUB, :]

        readers = [shift_reader(load, o) for o in (-stride, stride, -1, 1)]

        def tile(k):
            v = press[PAD + base + k, row - 1 : row - 1 + SUB, :]
            v = v + press[PAD + base + k, row + 1 : row + 1 + SUB, :]
            for reader in readers:
                v = v + reader(k)
            return v

        return tile

    news = []
    for row in (OWN - 1, OWN - 1 + SUB):
        near = beside(press_base, row)
        for k in range(press_count):
            v = fields[4, press_base + k, row : row + SUB, :] * (4.0 / 3.0) + near(k) * (1.0 / 9.0)
            sums[0, k, row - OWN + 1 : row - OWN + 1 + SUB, :] = jnp.where(
                inside(press_base + k, row), v, 0.0
            )
    for r, row in enumerate((OWN - 1, OWN - 1 + SUB)):
        for k in range(press_count):
            press[PAD + press_base + k, row : row + SUB, :] = sums[
                0, k, r * SUB : (r + 1) * SUB, :
            ]
    near = beside(base, OWN)
    for k in range(count):
        v = press[PAD + base + k, OWN : OWN + SUB, :] * (1.0 / 3.0)
        out[3, k] = v + fields[4, base + k, OWN : OWN + SUB, :] + near(k) * (1.0 / 9.0)

    for p in range(planes):
        if paired:
            at, turn = divmod(p * stride + COLS, LANES)
            turn = turn + gx * (planes * stride % LANES)
            back = (2 * LANES - turn) % LANES
            keep = lane < LANES - turn
        else:
            flat = (blocks // 2 * planes + p) * stride + COLS
            at, turn = divmod(flat, LANES)
            at = at - base
            back = LANES - turn
            keep = lane < LANES - turn
        for f in range(4):
            first = pltpu.roll(out[f, at], back, 1)
            v = jnp.where(keep, first, pltpu.roll(out[f, at + 1], back, 1))
            if f < 3:
                vel_ref[f, p] = v
            else:
                press_ref[p] = v


def on_device(rhs_velocity, rhs_pressure, layer_ids, visc_table, stencil):
    planes, rows, depth = rhs_pressure.shape
    assert rows == SUB and depth == LANES
    x_count, y_count, z_count = (lax.axis_size(n) for n in ("gx", "gy", "gz"))
    kc = (stencil[13, 0, 0] + stencil[13, 1, 1] + stencil[13, 2, 2]) / 3.0
    table = jnp.stack([visc_table, 1.0 / (visc_table * kc)])
    coef = jnp.broadcast_to((stencil / kc).reshape(-1, 1), (stencil.size, LANES))

    tile = jax.ShapeDtypeStruct((FIELDS, SUB, LANES), jnp.float32)
    vmem = pl.BlockSpec(memory_space=pltpu.VMEM)
    main, z_first, z_second = pl.pallas_call(
        functools.partial(pack_kernel, planes),
        out_shape=(
            jax.ShapeDtypeStruct((FIELDS * planes, SUB, LANES), jnp.float32),
            tile,
            tile,
        ),
        in_specs=[pl.BlockSpec(memory_space=pltpu.SMEM), vmem, vmem, vmem],
        out_specs=(vmem, vmem, vmem),
        name="pack",
    )(table, rhs_velocity, rhs_pressure, layer_ids)

    halo = matched(z_first, "gz", first_pairs(z_count))
    halo = halo + matched(z_second, "gz", second_pairs(z_count))
    block = jnp.concatenate([main, halo])

    paired = x_count == 2
    if paired:
        frame = jnp.stack([block, lax.ppermute(block, "gx", [(0, 1), (1, 0)])])
        blocks = 2
    else:
        hops = -(-REACH // planes)
        parts = []
        for hop in range(-hops, hops + 1):
            pairs = [(i, i - hop) for i in range(x_count) if 0 <= i - hop < x_count]
            parts.append(block if hop == 0 else matched(block, "gx", pairs))
        frame = jnp.stack(parts)
        blocks = 2 * hops + 1

    y_first = matched(frame, "gy", first_pairs(y_count))
    y_second = matched(frame, "gy", second_pairs(y_count))

    stride = LANES + 2 * COLS
    tiles = -(-planes * blocks * stride // LANES)
    f32 = jnp.float32
    return pl.pallas_call(
        functools.partial(cycle_kernel, planes, blocks, paired),
        out_shape=(
            jax.ShapeDtypeStruct(rhs_velocity.shape, f32),
            jax.ShapeDtypeStruct(rhs_pressure.shape, f32),
        ),
        in_specs=[vmem] * 4,
        out_specs=(vmem, vmem),
        scratch_shapes=[
            pltpu.VMEM((FIELDS, tiles, ROWS, LANES), f32),
            pltpu.VMEM((3, tiles + 2 * PAD, ROWS, LANES), f32),
            pltpu.VMEM((9, 3, tiles, ROWS, LANES), f32),
            pltpu.VMEM((3, tiles, ROWS, LANES), f32),
            pltpu.VMEM((3, tiles, 2 * SUB, LANES), f32),
            pltpu.VMEM((4, tiles, 2 * SUB, LANES), f32),
            pltpu.VMEM((tiles + 2 * PAD, ROWS, LANES), f32),
            pltpu.VMEM((4, tiles + 1, SUB, LANES), f32),
        ],
        name="cycle",
    )(frame, y_first, y_second, coef)


def solution(mesh):
    placed = (P(None, "gx", "gy", "gz"), P("gx", "gy", "gz"), P("gx", "gy", "gz"), P(), P())
    return jax.shard_map(
        on_device,
        mesh=mesh,
        in_specs=placed,
        out_specs=(P(None, "gx", "gy", "gz"), P("gx", "gy", "gz")),
        check_vma=False,
    )
```

```python
import functools

import jax
import jax.numpy as jnp
from jax import lax
from jax.experimental import pallas as pl
from jax.experimental.pallas import tpu as pltpu
from jax.sharding import PartitionSpec as P

LOW_BOUND = 0.2
HIGH_BOUND = 1.8

SUB = 8
LANES = 128
COLS = 8
REACH = 6
FIELDS = 5
PAD = 3
ROWS = 5 * SUB
OWN = 2 * SUB
SMALL_VMEM = 4 * 1024 * 1024
CYCLE_VMEM = 32 * 1024 * 1024


def cheb_consts():
    theta = (HIGH_BOUND + LOW_BOUND) / 2.0
    delta = (HIGH_BOUND - LOW_BOUND) / 2.0
    sigma = theta / delta
    rho_zero = 1.0 / sigma
    rho_one = 1.0 / (2.0 * sigma - rho_zero)
    return (theta, delta, rho_zero, rho_one)


def first_pairs(count):
    return [(i, i ^ 1) for i in range(count) if i ^ 1 < count]


def second_pairs(count):
    pairs = []
    for i in range(1, count - 1, 2):
        pairs += [(i, i + 1), (i + 1, i)]
    return pairs


def matched(block, axis, pairs):
    if not pairs:
        return jnp.zeros_like(block)
    return lax.ppermute(block, axis, pairs)


def lane_iota():
    return lax.broadcasted_iota(jnp.int32, (SUB, LANES), 1)


def diagonal_mean(stencil_ref):
    middle = stencil_ref.shape[2] // 2
    return (stencil_ref[0, 0, middle] + stencil_ref[1, 1, middle] + stencil_ref[2, 2, middle]) / 3.0


def coef_kernel(stencil_ref, coef_ref):
    scale = 1.0 / jnp.full((1, LANES), diagonal_mean(stencil_ref), jnp.float32)
    for i in range(3):
        for j in range(3):
            for o in range(stencil_ref.shape[2]):
                n = o * 9 + i * 3 + j
                coef_ref[n : n + 1, :] = scale * stencil_ref[i, j, o]


def pack_kernel(
    planes,
    visc_hbm,
    stencil_hbm,
    rhs_hbm,
    press_hbm,
    ids_hbm,
    main_ref,
    a_ref,
    b_ref,
    visc_ref,
    stencil_ref,
    rhs_ref,
    press_ref,
    ids_ref,
    arrived,
):
    copies = [
        pltpu.make_async_copy(src, dst, arrived.at[n])
        for n, (src, dst) in enumerate(
            (
                (visc_hbm, visc_ref),
                (stencil_hbm, stencil_ref),
                (ids_hbm, ids_ref),
                (rhs_hbm, rhs_ref),
                (press_hbm, press_ref),
            )
        )
    ]
    for copy in copies:
        copy.start()
    for copy in copies:
        copy.wait()
    lane = lane_iota()
    odd = lax.axis_index("gz") % 2 == 1
    kc = jnp.full((SUB, LANES), diagonal_mean(stencil_ref), jnp.float32)
    up = [jnp.zeros((SUB, LANES), jnp.float32)] * FIELDS
    down = [jnp.zeros((SUB, LANES), jnp.float32)] * FIELDS
    width = 2 * COLS
    for p in range(planes):
        ids = ids_ref[p]
        eta = jnp.zeros((SUB, LANES), jnp.float32)
        for layer in range(visc_ref.shape[0]):
            eta = jnp.where(ids == layer, visc_ref[layer], eta)
        dinv = 1.0 / (eta * kc)
        values = [rhs_ref[j, p] * dinv for j in range(3)]
        values += [eta, eta * press_ref[p] * (1.0 / 9.0)]
        for f in range(FIELDS):
            main_ref[f * planes + p] = values[f]
            turned = pltpu.roll(values[f], (p * width + COLS) % LANES, 1)
            up[f] = jnp.where((lane >= p * width) & (lane < p * width + COLS), turned, up[f])
            down[f] = jnp.where(
                (lane >= p * width + COLS) & (lane < (p + 1) * width), turned, down[f]
            )
    for f in range(FIELDS):
        a_ref[f] = jnp.where(odd, down[f], up[f])
        b_ref[f] = jnp.where(odd, up[f], down[f])


def tile_span(planes_from, planes_to, stride):
    first = planes_from * stride // LANES
    last = ((planes_to + 1) * stride - 1) // LANES
    return first, last - first + 1


def cycle_kernel(
    planes,
    blocks,
    paired,
    own_ref,
    a_ref,
    b_ref,
    coef_ref,
    vel_ref,
    press_ref,
    fields,
    work,
    shifted,
    second_x,
    resid,
    sums,
    press,
    out,
):
    theta, delta, rho_zero, rho_one = cheb_consts()
    weight = 2.0 * rho_one / delta
    carry = rho_one * rho_zero
    total = planes * blocks
    stride = LANES + 2 * COLS
    tiles = fields.shape[1]
    lane = lane_iota()
    zero = jnp.zeros((SUB, LANES), jnp.float32)
    gx = lax.axis_index("gx")
    y_odd = lax.axis_index("gy") % 2 == 1

    def span(grow):
        if paired:
            low = tile_span(0, min(planes - 1 + grow, total - 1), stride)
            high = tile_span(max(planes - grow, 0), total - 1, stride)
            count = max(low[1], high[1])
            return low[0] + gx * (high[0] - low[0]), count
        own = blocks // 2
        lo = max(own * planes - grow, 0)
        hi = min((own + 1) * planes - 1 + grow, total - 1)
        return tile_span(lo, hi, stride)

    def slot(q):
        return (q + gx) % 2 if paired else q

    for k in list(range(PAD)) + list(range(PAD + tiles, 2 * PAD + tiles)):
        for r in range(1, 4):
            for j in range(3):
                work[j, k, r * SUB : (r + 1) * SUB, :] = zero
            press[k, r * SUB : (r + 1) * SUB, :] = zero

    def assemble(src, row):
        for f in range(FIELDS):
            halo = {}
            for q in range(blocks):
                tile = src[slot(q), FIELDS * planes + f]
                turn = (q * planes * 2 * COLS) % LANES
                halo[q] = pltpu.roll(tile, turn, 1) if turn else tile
            mains = {}
            for k in range(tiles):
                pieces = []
                for plane in range(total):
                    q, p = divmod(plane, planes)
                    at = plane * stride
                    for kind, lo, hi in (
                        ("halo", at, at + COLS),
                        ("main", at + COLS, at + COLS + LANES),
                        ("halo", at + COLS + LANES, at + stride),
                    ):
                        lo, hi = max(lo, k * LANES), min(hi, (k + 1) * LANES)
                        if lo >= hi:
                            continue
                        if kind == "halo":
                            piece = ("halo", q)
                        else:
                            piece = ("main", plane)
                        if pieces and pieces[-1][1] == piece:
                            continue
                        pieces.append((lo - k * LANES, piece))
                if (k + 1) * LANES > total * stride:
                    pieces.append((total * stride - k * LANES, None))
                value = None
                for start, piece in pieces:
                    if piece is None:
                        tile = zero
                    elif piece[0] == "halo":
                        tile = halo[piece[1]]
                    else:
                        plane = piece[1]
                        if plane not in mains:
                            q, p = divmod(plane, planes)
                            mains[plane] = pltpu.roll(
                                src[slot(q), f * planes + p],
                                (plane * stride + COLS) % LANES,
                                1,
                            )
                        tile = mains[plane]
                    value = tile if value is None else jnp.where(lane >= start, tile, value)
                fields[f, k, row : row + SUB, :] = value
                if f < 3:
                    work[f, PAD + k, row : row + SUB, :] = value
                if f == 4:
                    press[PAD + k, row : row + SUB, :] = value

    assemble(own_ref, OWN)

    @pl.when(y_odd)
    def _():
        assemble(a_ref, OWN - SUB)
        assemble(b_ref, OWN + SUB)

    @pl.when(jnp.logical_not(y_odd))
    def _():
        assemble(b_ref, OWN - SUB)
        assemble(a_ref, OWN + SUB)

    def shift_reader(load, offset):
        jump, turn = divmod(offset, LANES)
        cache = {}

        def turned(k):
            if k not in cache:
                cache[k] = pltpu.roll(load(k), LANES - turn, 1)
            return cache[k]

        def tile(k):
            if turn == 0:
                return load(k + jump)
            return jnp.where(lane < LANES - turn, turned(k + jump), turned(k + jump + 1))

        return tile

    def make_shifts(base, count, rows, scale):
        for j in range(3):
            for row in rows:
                def load(k, j=j, row=row):
                    return work[j, PAD + base + k, row : row + SUB, :]

                readers = {}
                for a in range(3):
                    for c in range(3):
                        if (a, c) != (1, 1):
                            readers[a * 3 + c] = shift_reader(
                                load, ((a - 1) * stride + (c - 1)) * scale
                            )
                for k in range(count):
                    for n, reader in readers.items():
                        shifted[n, j, k, row : row + SUB, :] = reader(k)

    def apply(base, count, rows, scale, group, emit):
        def step(first, width):
            spots = [(first + g, row) for g in range(width) for row in rows]
            totals = [[None] * 3 for _ in spots]
            for a in range(3):
                for c in range(3):
                    for b in range(3):
                        for j in range(3):
                            values = []
                            for k, row in spots:
                                at = row + (b - 1) * scale
                                if (a, c) == (1, 1):
                                    v = work[j, PAD + base + k, at : at + SUB, :]
                                else:
                                    v = shifted[a * 3 + c, j, k, at : at + SUB, :]
                                values.append(v)
                            for i in range(3):
                                n = (9 * a + 3 * b + c) * 9 + i * 3 + j
                                coef = jnp.broadcast_to(coef_ref[n : n + 1, :], (SUB, LANES))
                                for s, v in enumerate(values):
                                    term = coef * v
                                    old = totals[s][i]
                                    totals[s][i] = term if old is None else old + term
            results = []
            for (k, row), sums_of in zip(spots, totals):
                results.append(emit(base + k, row, sums_of))
            for stores in results:
                for ref, index, value in stores:
                    ref[index] = value

        whole = count // group
        if whole > 1:
            def body(n, _):
                step(n * group, group)
                return 0

            lax.fori_loop(0, whole, body, 0)
        elif whole == 1:
            step(0, group)
        if count % group:
            step(whole * group, count % group)

    def inside(k, row):
        return fields[3, k, row : row + SUB, :] > 0.0

    def emit_first(k, row, sums_of):
        keep = inside(k, row)
        stores = []
        for i in range(3):
            f0 = fields[i, k, row : row + SUB, :]
            value = jnp.where(keep, (1.0 + carry + weight) * f0 - weight * sums_of[i], 0.0)
            stores.append((work, (i, PAD + k, pl.ds(row, SUB), slice(None)), value))
            stores.append((second_x, (i, k, pl.ds(row, SUB), slice(None)), value))
        return stores

    make_shifts(0, tiles, [OWN - SUB, OWN, OWN + SUB], 1)
    apply(0, tiles, [OWN - SUB, OWN, OWN + SUB], 1, 1, emit_first)

    def emit_resid(k, row, sums_of):
        eta = fields[3, k, row : row + SUB, :]
        stores = []
        for i in range(3):
            value = eta * (fields[i, k, row : row + SUB, :] - sums_of[i])
            at = row - (OWN - SUB // 2)
            stores.append((resid, (i, k, pl.ds(at, SUB), slice(None)), value))
        return stores

    make_shifts(0, tiles, [OWN - SUB, OWN, OWN + SUB], 1)
    apply(0, tiles, [OWN - SUB // 2, OWN + SUB // 2], 1, 1, emit_resid)

    lane_even = lane % 2 == 0
    row_even = lax.broadcasted_iota(jnp.int32, (SUB, LANES), 0) % 2 == 0
    for r in range(2):
        row = OWN - SUB // 2 + r * SUB
        for k in range(tiles):
            for f in range(4):
                if f < 3:
                    v = resid[f, k, r * SUB : (r + 1) * SUB, :]
                else:
                    v = fields[3, k, row : row + SUB, :]
                v = v + jnp.where(row_even, pltpu.roll(v, SUB - 1, 0), pltpu.roll(v, 1, 0))
                v = v + jnp.where(lane_even, pltpu.roll(v, LANES - 1, 1), pltpu.roll(v, 1, 1))
                sums[f, k, r * SUB : (r + 1) * SUB, :] = v
        scale_at = {}
        for f in (3, 0, 1, 2):
            def load(k, f=f, r=r):
                if 0 <= k < tiles:
                    return sums[f, k, r * SUB : (r + 1) * SUB, :]
                return zero

            ahead, behind = shift_reader(load, stride), shift_reader(load, -stride)
            for k in range(tiles):
                plane = k * LANES // stride
                edge = (plane + 1) * stride - k * LANES
                near, far = (ahead(k), behind(k))
                if plane % 2:
                    near, far = far, near
                other = jnp.where(lane < edge, near, far) if edge < LANES else near
                v = load(k) + other
                if f == 3:
                    scale_at[k] = jnp.where(v > 0.0, 4.0 / v, 0.0)
                else:
                    work[f, PAD + k, row : row + SUB, :] = v * scale_at[k]

    def emit_start(k, row, sums_of):
        keep = inside(k, row)
        stores = []
        for i in range(3):
            fc = work[i, PAD + k, row : row + SUB, :]
            value = second_x[i, k, row : row + SUB, :] + (1.0 + carry + weight) * fc
            value = jnp.where(keep, value - weight * sums_of[i], 0.0)
            stores.append((work, (i, PAD + k, pl.ds(row, SUB), slice(None)), value))
        return stores

    base, count = span(2)
    make_shifts(base, count, [OWN - SUB // 2, OWN + SUB // 2], 2)
    apply(base, count, [OWN - 2, OWN - 2 + SUB], 2, 1, emit_start)

    def emit_middle(k, row, sums_of):
        keep = inside(k, row)
        stores = []
        for i in range(3):
            step = jnp.where(keep, fields[i, k, row : row + SUB, :] - sums_of[i], 0.0)
            value = work[i, PAD + k, row : row + SUB, :] + step
            stores.append((work, (i, PAD + k, pl.ds(row, SUB), slice(None)), value))
            stores.append((second_x, (i, k, pl.ds(row, SUB), slice(None)), step))
        return stores

    base, count = span(1)
    make_shifts(base, count, [OWN - 2, OWN - 2 + SUB], 1)
    apply(base, count, [OWN - 1, OWN - 1 + SUB], 1, 2, emit_middle)
    press_base, press_count = base, count

    base, count = span(0)

    def emit_last(k, row, sums_of):
        stores = []
        for i in range(3):
            value = work[i, PAD + k, row : row + SUB, :]
            value = value + carry * second_x[i, k, row : row + SUB, :]
            value = value + weight * (fields[i, k, row : row + SUB, :] - sums_of[i])
            stores.append((out, (i, k - base), value))
        return stores

    make_shifts(base, count, [OWN - 1, OWN + 1], 1)
    apply(base, count, [OWN], 1, count, emit_last)

    def beside(base, row):
        def load(k):
            return press[PAD + base + k, row : row + SUB, :]

        readers = [shift_reader(load, o) for o in (-stride, stride, -1, 1)]

        def tile(k):
            v = press[PAD + base + k, row - 1 : row - 1 + SUB, :]
            v = v + press[PAD + base + k, row + 1 : row + 1 + SUB, :]
            for reader in readers:
                v = v + reader(k)
            return v

        return tile

    news = []
    for row in (OWN - 1, OWN - 1 + SUB):
        near = beside(press_base, row)
        for k in range(press_count):
            v = fields[4, press_base + k, row : row + SUB, :] * (4.0 / 3.0) + near(k) * (1.0 / 9.0)
            sums[0, k, row - OWN + 1 : row - OWN + 1 + SUB, :] = jnp.where(
                inside(press_base + k, row), v, 0.0
            )
    for r, row in enumerate((OWN - 1, OWN - 1 + SUB)):
        for k in range(press_count):
            press[PAD + press_base + k, row : row + SUB, :] = sums[
                0, k, r * SUB : (r + 1) * SUB, :
            ]
    near = beside(base, OWN)
    for k in range(count):
        v = press[PAD + base + k, OWN : OWN + SUB, :] * (1.0 / 3.0)
        out[3, k] = v + fields[4, base + k, OWN : OWN + SUB, :] + near(k) * (1.0 / 9.0)

    for p in range(planes):
        if paired:
            at, turn = divmod(p * stride + COLS, LANES)
            turn = turn + gx * (planes * stride % LANES)
            back = (2 * LANES - turn) % LANES
            keep = lane < LANES - turn
        else:
            flat = (blocks // 2 * planes + p) * stride + COLS
            at, turn = divmod(flat, LANES)
            at = at - base
            back = LANES - turn
            keep = lane < LANES - turn
        for f in range(4):
            first = pltpu.roll(out[f, at], back, 1)
            v = jnp.where(keep, first, pltpu.roll(out[f, at + 1], back, 1))
            if f < 3:
                vel_ref[f, p] = v
            else:
                press_ref[p] = v


def on_device(rhs_velocity, rhs_pressure, layer_ids, visc_table, stencil):
    planes, rows, depth = rhs_pressure.shape
    assert rows == SUB and depth == LANES
    x_count, y_count, z_count = (lax.axis_size(n) for n in ("gx", "gy", "gz"))
    entries = jnp.transpose(stencil, (1, 2, 0))

    tile = jax.ShapeDtypeStruct((FIELDS, SUB, LANES), jnp.float32)
    vmem = pl.BlockSpec(memory_space=pltpu.VMEM)
    smem = pl.BlockSpec(memory_space=pltpu.SMEM)
    coef = pl.pallas_call(
        coef_kernel,
        out_shape=jax.ShapeDtypeStruct((stencil.size, LANES), jnp.float32),
        in_specs=[smem],
        out_specs=vmem,
        compiler_params=pltpu.CompilerParams(vmem_limit_bytes=SMALL_VMEM),
        name="coef",
    )(entries)
    main, z_first, z_second = pl.pallas_call(
        functools.partial(pack_kernel, planes),
        out_shape=(
            jax.ShapeDtypeStruct((FIELDS * planes, SUB, LANES), jnp.float32),
            tile,
            tile,
        ),
        in_specs=[pl.BlockSpec(memory_space=pltpu.HBM)] * 5,
        out_specs=(vmem, vmem, vmem),
        scratch_shapes=[
            pltpu.SMEM(visc_table.shape, visc_table.dtype),
            pltpu.SMEM(entries.shape, entries.dtype),
            pltpu.VMEM(rhs_velocity.shape, rhs_velocity.dtype),
            pltpu.VMEM(rhs_pressure.shape, rhs_pressure.dtype),
            pltpu.VMEM(layer_ids.shape, layer_ids.dtype),
            pltpu.SemaphoreType.DMA((5,)),
        ],
        compiler_params=pltpu.CompilerParams(vmem_limit_bytes=SMALL_VMEM),
        name="pack",
    )(
        *(
            pltpu.with_memory_space_constraint(v, pltpu.HBM)
            for v in (visc_table, entries, rhs_velocity, rhs_pressure, layer_ids)
        )
    )

    halo = matched(z_first, "gz", first_pairs(z_count))
    halo = halo + matched(z_second, "gz", second_pairs(z_count))
    block = jnp.concatenate([main, halo])

    paired = x_count == 2
    if paired:
        frame = jnp.stack([block, lax.ppermute(block, "gx", [(0, 1), (1, 0)])])
        blocks = 2
    else:
        hops = -(-REACH // planes)
        parts = []
        for hop in range(-hops, hops + 1):
            pairs = [(i, i - hop) for i in range(x_count) if 0 <= i - hop < x_count]
            parts.append(block if hop == 0 else matched(block, "gx", pairs))
        frame = jnp.stack(parts)
        blocks = 2 * hops + 1

    y_first = matched(frame, "gy", first_pairs(y_count))
    y_second = matched(frame, "gy", second_pairs(y_count))

    stride = LANES + 2 * COLS
    tiles = -(-planes * blocks * stride // LANES)
    f32 = jnp.float32
    return pl.pallas_call(
        functools.partial(cycle_kernel, planes, blocks, paired),
        out_shape=(
            jax.ShapeDtypeStruct(rhs_velocity.shape, f32),
            jax.ShapeDtypeStruct(rhs_pressure.shape, f32),
        ),
        in_specs=[vmem] * 4,
        out_specs=(vmem, vmem),
        scratch_shapes=[
            pltpu.VMEM((FIELDS, tiles, ROWS, LANES), f32),
            pltpu.VMEM((3, tiles + 2 * PAD, ROWS, LANES), f32),
            pltpu.VMEM((9, 3, tiles, ROWS, LANES), f32),
            pltpu.VMEM((3, tiles, ROWS, LANES), f32),
            pltpu.VMEM((3, tiles, 2 * SUB, LANES), f32),
            pltpu.VMEM((4, tiles, 2 * SUB, LANES), f32),
            pltpu.VMEM((tiles + 2 * PAD, ROWS, LANES), f32),
            pltpu.VMEM((4, tiles + 1, SUB, LANES), f32),
        ],
        compiler_params=pltpu.CompilerParams(vmem_limit_bytes=CYCLE_VMEM),
        name="cycle",
    )(frame, y_first, y_second, coef)


def solution(mesh):
    placed = (P(None, "gx", "gy", "gz"), P("gx", "gy", "gz"), P("gx", "gy", "gz"), P(), P())
    return jax.shard_map(
        on_device,
        mesh=mesh,
        in_specs=placed,
        out_specs=(P(None, "gx", "gy", "gz"), P("gx", "gy", "gz")),
        check_vma=False,
    )
```

```python
import functools

import jax
import jax.numpy as jnp
from jax import lax
from jax.experimental import pallas as pl
from jax.experimental.pallas import tpu as pltpu
from jax.sharding import PartitionSpec as P

LOW_BOUND = 0.2
HIGH_BOUND = 1.8

SUB = 8
LANES = 128
COLS = 8
REACH = 6
FIELDS = 5
PAD = 3
ROWS = 3 * SUB
OWN = SUB
ROWS_RESID = OWN - 4
ROWS_START = OWN - 2
ROWS_MIDDLE = OWN - 1
DEPTH = 2 * LANES
SMALL_VMEM = 4 * 1024 * 1024
CYCLE_VMEM = 32 * 1024 * 1024


def cheb_consts():
    theta = (HIGH_BOUND + LOW_BOUND) / 2.0
    delta = (HIGH_BOUND - LOW_BOUND) / 2.0
    sigma = theta / delta
    rho_zero = 1.0 / sigma
    rho_one = 1.0 / (2.0 * sigma - rho_zero)
    return (theta, delta, rho_zero, rho_one)


def first_pairs(count):
    return [(i, i ^ 1) for i in range(count) if i ^ 1 < count]


def second_pairs(count):
    pairs = []
    for i in range(1, count - 1, 2):
        pairs += [(i, i + 1), (i + 1, i)]
    return pairs


def matched(block, axis, pairs):
    if not pairs:
        return jnp.zeros_like(block)
    return lax.ppermute(block, axis, pairs)


def lane_iota():
    return lax.broadcasted_iota(jnp.int32, (SUB, LANES), 1)


def diagonal_mean(stencil_ref):
    middle = stencil_ref.shape[2] // 2
    return (stencil_ref[0, 0, middle] + stencil_ref[1, 1, middle] + stencil_ref[2, 2, middle]) / 3.0


def band_kernel(stencil_ref, smooth_ref, resid_ref, coarse_ref, middle_ref):
    scale = 1.0 / jnp.full((SUB, LANES), diagonal_mean(stencil_ref), jnp.float32)
    sub = lax.broadcasted_iota(jnp.int32, (SUB, LANES), 0)
    lane = lane_iota()
    parts = []
    for half in range(DEPTH // LANES):
        spot = lane + half * LANES
        chunk = jnp.zeros((SUB, LANES), jnp.int32)
        for n in range(1, DEPTH // ROWS + 1):
            chunk = jnp.where(spot >= n * ROWS, n, chunk)
        used = chunk < 9
        reach = jnp.where(used, spot - chunk * ROWS - sub, 1000)
        term = chunk // 3
        parts.append((reach, chunk - 3 * term, term == 2))
    for a in range(3):
        for c in range(3):
            for i in range(3):
                rows_of = []
                for b in range(3):
                    entry = [
                        scale * stencil_ref[i, j, 9 * a + 3 * b + c] for j in range(3)
                    ]
                    row = []
                    for reach, j_at, low_at in parts:
                        full = jnp.where(
                            j_at == 0, entry[0], jnp.where(j_at == 1, entry[1], entry[2])
                        )
                        high = full.astype(jnp.bfloat16).astype(jnp.float32)
                        row.append(jnp.where(low_at, full - high, high))
                    rows_of.append(row)
                for ref, start, step in (
                    (smooth_ref, 0, 1),
                    (resid_ref, ROWS_RESID, 1),
                    (coarse_ref, ROWS_START, 2),
                    (middle_ref, ROWS_MIDDLE, 1),
                ):
                    for r in range(ref.shape[1] // SUB):
                        for half, (reach, j_at, low_at) in enumerate(parts):
                            value = jnp.zeros((SUB, LANES), jnp.float32)
                            for b in range(3):
                                at = r * SUB + start + step * (b - 1)
                                value = jnp.where(reach == at, rows_of[b][half], value)
                            ref[
                                (3 * a + c) * 3 + i,
                                r * SUB : (r + 1) * SUB,
                                half * LANES : (half + 1) * LANES,
                            ] = value


def pack_kernel(
    planes,
    visc_hbm,
    stencil_hbm,
    rhs_hbm,
    press_hbm,
    ids_hbm,
    main_ref,
    a_ref,
    b_ref,
    visc_ref,
    stencil_ref,
    rhs_ref,
    press_ref,
    ids_ref,
    arrived,
):
    copies = [
        pltpu.make_async_copy(src, dst, arrived.at[n])
        for n, (src, dst) in enumerate(
            (
                (visc_hbm, visc_ref),
                (stencil_hbm, stencil_ref),
                (ids_hbm, ids_ref),
                (rhs_hbm, rhs_ref),
                (press_hbm, press_ref),
            )
        )
    ]
    for copy in copies:
        copy.start()
    for copy in copies:
        copy.wait()
    lane = lane_iota()
    odd = lax.axis_index("gz") % 2 == 1
    kc = jnp.full((SUB, LANES), diagonal_mean(stencil_ref), jnp.float32)
    up = [jnp.zeros((SUB, LANES), jnp.float32)] * FIELDS
    down = [jnp.zeros((SUB, LANES), jnp.float32)] * FIELDS
    width = 2 * COLS
    for p in range(planes):
        ids = ids_ref[p]
        eta = jnp.zeros((SUB, LANES), jnp.float32)
        for layer in range(visc_ref.shape[0]):
            eta = jnp.where(ids == layer, visc_ref[layer], eta)
        dinv = 1.0 / (eta * kc)
        values = [rhs_ref[j, p] * dinv for j in range(3)]
        values += [eta, eta * press_ref[p] * (1.0 / 9.0)]
        for f in range(FIELDS):
            main_ref[f * planes + p] = values[f]
            turned = pltpu.roll(values[f], (p * width + COLS) % LANES, 1)
            up[f] = jnp.where((lane >= p * width) & (lane < p * width + COLS), turned, up[f])
            down[f] = jnp.where(
                (lane >= p * width + COLS) & (lane < (p + 1) * width), turned, down[f]
            )
    for f in range(FIELDS):
        a_ref[f] = jnp.where(odd, down[f], up[f])
        b_ref[f] = jnp.where(odd, up[f], down[f])


def tile_span(planes_from, planes_to, stride):
    first = planes_from * stride // LANES
    last = ((planes_to + 1) * stride - 1) // LANES
    return first, last - first + 1


def cycle_kernel(
    planes,
    blocks,
    paired,
    own_ref,
    a_ref,
    b_ref,
    smooth_ref,
    resid_band,
    coarse_ref,
    middle_ref,
    vel_ref,
    press_ref,
    fields,
    work,
    split,
    products,
    second_x,
    resid,
    sums,
    press,
    out,
):
    theta, delta, rho_zero, rho_one = cheb_consts()
    weight = 2.0 * rho_one / delta
    carry = rho_one * rho_zero
    total = planes * blocks
    stride = LANES + 2 * COLS
    tiles = fields.shape[1]
    lane = lane_iota()
    zero = jnp.zeros((SUB, LANES), jnp.float32)
    gx = lax.axis_index("gx")
    y_odd = lax.axis_index("gy") % 2 == 1

    def span(grow):
        if paired:
            low = tile_span(0, min(planes - 1 + grow, total - 1), stride)
            high = tile_span(max(planes - grow, 0), total - 1, stride)
            count = max(low[1], high[1])
            return low[0] + gx * (high[0] - low[0]), count
        own = blocks // 2
        lo = max(own * planes - grow, 0)
        hi = min((own + 1) * planes - 1 + grow, total - 1)
        return tile_span(lo, hi, stride)

    def slot(q):
        return (q + gx) % 2 if paired else q

    edges = list(range(PAD)) + list(range(PAD + tiles, 2 * PAD + tiles))
    for k in edges:
        for r in range(3):
            press[k, r * SUB : (r + 1) * SUB, :] = zero
        for n in range(27):
            for r in range(2):
                products[k, (n * 2 + r) * SUB : (n * 2 + r + 1) * SUB, :] = zero
    for k in range(tiles):
        for r in range(3 * 3 * 3, DEPTH // SUB):
            split[r * SUB : (r + 1) * SUB, k * LANES : (k + 1) * LANES] = zero

    def assemble(src, row):
        for f in range(FIELDS):
            halo = {}
            for q in range(blocks):
                tile = src[slot(q), FIELDS * planes + f]
                turn = (q * planes * 2 * COLS) % LANES
                halo[q] = pltpu.roll(tile, turn, 1) if turn else tile
            mains = {}
            for k in range(tiles):
                pieces = []
                for plane in range(total):
                    q, p = divmod(plane, planes)
                    at = plane * stride
                    for kind, lo, hi in (
                        ("halo", at, at + COLS),
                        ("main", at + COLS, at + COLS + LANES),
                        ("halo", at + COLS + LANES, at + stride),
                    ):
                        lo, hi = max(lo, k * LANES), min(hi, (k + 1) * LANES)
                        if lo >= hi:
                            continue
                        if kind == "halo":
                            piece = ("halo", q)
                        else:
                            piece = ("main", plane)
                        if pieces and pieces[-1][1] == piece:
                            continue
                        pieces.append((lo - k * LANES, piece))
                if (k + 1) * LANES > total * stride:
                    pieces.append((total * stride - k * LANES, None))
                value = None
                for start, piece in pieces:
                    if piece is None:
                        tile = zero
                    elif piece[0] == "halo":
                        tile = halo[piece[1]]
                    else:
                        plane = piece[1]
                        if plane not in mains:
                            q, p = divmod(plane, planes)
                            mains[plane] = pltpu.roll(
                                src[slot(q), f * planes + p],
                                (plane * stride + COLS) % LANES,
                                1,
                            )
                        tile = mains[plane]
                    value = tile if value is None else jnp.where(lane >= start, tile, value)
                fields[f, k, row : row + SUB, :] = value
                if f < 3:
                    work[f, k, row : row + SUB, :] = value
                if f == 4:
                    press[PAD + k, row : row + SUB, :] = value

    assemble(own_ref, OWN)

    @pl.when(y_odd)
    def _():
        assemble(a_ref, OWN - SUB)
        assemble(b_ref, OWN + SUB)

    @pl.when(jnp.logical_not(y_odd))
    def _():
        assemble(b_ref, OWN - SUB)
        assemble(a_ref, OWN + SUB)

    def shift_reader(load, offset):
        jump, turn = divmod(offset, LANES)
        cache = {}

        def turned(k):
            if k not in cache:
                cache[k] = pltpu.roll(load(k), LANES - turn, 1)
            return cache[k]

        def tile(k):
            if turn == 0:
                return load(k + jump)
            return jnp.where(lane < LANES - turn, turned(k + jump), turned(k + jump + 1))

        return tile

    def apply(src, count, dst, spots, band_ref, first, rows, scale, emit):
        height = rows * SUB
        for j in range(3):
            for r in range(3):
                at = (j * 3 + r) * SUB
                for k in range(count):
                    v = work[j, src + k, r * SUB : (r + 1) * SUB, :]
                    high = v.astype(jnp.bfloat16).astype(jnp.float32)
                    lanes = slice(k * LANES, (k + 1) * LANES)
                    split[at : at + SUB, lanes] = high
                    split[at + 3 * ROWS : at + 3 * ROWS + SUB, lanes] = v - high
                    split[at + 6 * ROWS : at + 6 * ROWS + SUB, lanes] = high
        band = band_ref[:, first : first + height, :].reshape(27 * height, DEPTH)
        for k in range(0, count, 2):
            width = min(2, count - k)
            product = jnp.dot(
                band,
                split[:, k * LANES : (k + width) * LANES],
                preferred_element_type=jnp.float32,
                precision=lax.Precision.DEFAULT,
            )
            for w in range(width):
                products[PAD + k + w, : 27 * height, :] = product[:, w * LANES : (w + 1) * LANES]
        shift = dst - src
        if not isinstance(shift, int):
            for k in range(count, min(count + 2, tiles)):
                for n in range(27 * rows):
                    products[PAD + k, n * SUB : (n + 1) * SUB, :] = zero
        for r in range(rows):
            for i in range(3):
                readers = []
                for a in range(3):
                    for c in range(3):
                        row = ((3 * a + c) * 3 + i) * height + r * SUB

                        def load(k, row=row):
                            if isinstance(shift, int) and not 0 <= shift + k < count:
                                return zero
                            return products[PAD + shift + k, row : row + SUB, :]

                        offset = ((a - 1) * stride + (c - 1)) * scale
                        readers.append(shift_reader(load, offset))
                for k in range(spots):
                    total_of = readers[0](k)
                    for reader in readers[1:]:
                        total_of = total_of + reader(k)
                    emit(dst + k, r, i, total_of)

    def inside(k, row):
        return fields[3, k, row : row + SUB, :] > 0.0

    def emit_first(k, r, i, total_of):
        at = slice(r * SUB, (r + 1) * SUB)
        value = (1.0 + carry + weight) * fields[i, k, at, :] - weight * total_of
        value = jnp.where(inside(k, r * SUB), value, 0.0)
        work[i, k, at, :] = value
        second_x[i, k, at, :] = value

    apply(0, tiles, 0, tiles, smooth_ref, 0, 3, 1, emit_first)

    def emit_resid(k, r, i, total_of):
        at = slice(ROWS_RESID + r * SUB, ROWS_RESID + (r + 1) * SUB)
        value = fields[3, k, at, :] * (fields[i, k, at, :] - total_of)
        resid[i, k, r * SUB : (r + 1) * SUB, :] = value

    apply(0, tiles, 0, tiles, resid_band, 0, 2, 1, emit_resid)

    lane_even = lane % 2 == 0
    row_even = lax.broadcasted_iota(jnp.int32, (SUB, LANES), 0) % 2 == 0
    for r in range(2):
        row = ROWS_RESID + r * SUB
        for k in range(tiles):
            for f in range(4):
                if f < 3:
                    v = resid[f, k, r * SUB : (r + 1) * SUB, :]
                else:
                    v = fields[3, k, row : row + SUB, :]
                v = v + jnp.where(row_even, pltpu.roll(v, SUB - 1, 0), pltpu.roll(v, 1, 0))
                v = v + jnp.where(lane_even, pltpu.roll(v, LANES - 1, 1), pltpu.roll(v, 1, 1))
                sums[f, k, r * SUB : (r + 1) * SUB, :] = v
        scale_at = {}
        for f in (3, 0, 1, 2):
            def load(k, f=f, r=r):
                if 0 <= k < tiles:
                    return sums[f, k, r * SUB : (r + 1) * SUB, :]
                return zero

            ahead, behind = shift_reader(load, stride), shift_reader(load, -stride)
            for k in range(tiles):
                plane = k * LANES // stride
                edge = (plane + 1) * stride - k * LANES
                near, far = (ahead(k), behind(k))
                if plane % 2:
                    near, far = far, near
                other = jnp.where(lane < edge, near, far) if edge < LANES else near
                v = load(k) + other
                if f == 3:
                    scale_at[k] = jnp.where(v > 0.0, 4.0 / v, 0.0)
                else:
                    work[f, k, row : row + SUB, :] = v * scale_at[k]

    def emit_start(k, r, i, total_of):
        at = slice(ROWS_START + r * SUB, ROWS_START + (r + 1) * SUB)
        value = second_x[i, k, at, :] + (1.0 + carry + weight) * work[i, k, at, :]
        value = jnp.where(inside(k, ROWS_START + r * SUB), value - weight * total_of, 0.0)
        work[i, k, at, :] = value

    wide, wide_count = span(2)
    apply(0, tiles, wide, wide_count, coarse_ref, 0, 2, 2, emit_start)

    def emit_middle(k, r, i, total_of):
        at = slice(ROWS_MIDDLE + r * SUB, ROWS_MIDDLE + (r + 1) * SUB)
        step = jnp.where(inside(k, ROWS_MIDDLE + r * SUB), fields[i, k, at, :] - total_of, 0.0)
        work[i, k, at, :] = work[i, k, at, :] + step
        second_x[i, k, at, :] = step

    near_base, near_count = span(1)
    apply(wide, wide_count, near_base, near_count, middle_ref, 0, 2, 1, emit_middle)

    base, count = span(0)

    def emit_last(k, r, i, total_of):
        at = slice(OWN, OWN + SUB)
        value = work[i, k, at, :] + carry * second_x[i, k, at, :]
        out[i, k - base] = value + weight * (fields[i, k, at, :] - total_of)

    apply(near_base, near_count, base, count, smooth_ref, OWN, 1, 1, emit_last)
    press_base, press_count = near_base, near_count

    def beside(base, row):
        def load(k):
            return press[PAD + base + k, row : row + SUB, :]

        readers = [shift_reader(load, o) for o in (-stride, stride, -1, 1)]

        def tile(k):
            v = press[PAD + base + k, row - 1 : row - 1 + SUB, :]
            v = v + press[PAD + base + k, row + 1 : row + 1 + SUB, :]
            for reader in readers:
                v = v + reader(k)
            return v

        return tile

    starts = (OWN - 1, OWN + 1)
    for r, row in enumerate(starts):
        near = beside(press_base, row)
        for k in range(press_count):
            v = fields[4, press_base + k, row : row + SUB, :] * (4.0 / 3.0) + near(k) * (1.0 / 9.0)
            sums[r, k, :SUB, :] = jnp.where(inside(press_base + k, row), v, 0.0)
    for r, row in enumerate(starts):
        for k in range(press_count):
            press[PAD + press_base + k, row : row + SUB, :] = sums[r, k, :SUB, :]
    near = beside(base, OWN)
    for k in range(count):
        v = press[PAD + base + k, OWN : OWN + SUB, :] * (1.0 / 3.0)
        out[3, k] = v + fields[4, base + k, OWN : OWN + SUB, :] + near(k) * (1.0 / 9.0)

    for p in range(planes):
        if paired:
            at, turn = divmod(p * stride + COLS, LANES)
            turn = turn + gx * (planes * stride % LANES)
            back = (2 * LANES - turn) % LANES
            keep = lane < LANES - turn
        else:
            flat = (blocks // 2 * planes + p) * stride + COLS
            at, turn = divmod(flat, LANES)
            at = at - base
            back = LANES - turn
            keep = lane < LANES - turn
        for f in range(4):
            first = pltpu.roll(out[f, at], back, 1)
            v = jnp.where(keep, first, pltpu.roll(out[f, at + 1], back, 1))
            if f < 3:
                vel_ref[f, p] = v
            else:
                press_ref[p] = v


def on_device(rhs_velocity, rhs_pressure, layer_ids, visc_table, stencil):
    planes, rows, depth = rhs_pressure.shape
    assert rows == SUB and depth == LANES
    x_count, y_count, z_count = (lax.axis_size(n) for n in ("gx", "gy", "gz"))
    entries = jnp.transpose(stencil, (1, 2, 0))

    tile = jax.ShapeDtypeStruct((FIELDS, SUB, LANES), jnp.float32)
    vmem = pl.BlockSpec(memory_space=pltpu.VMEM)
    smem = pl.BlockSpec(memory_space=pltpu.SMEM)
    bands = pl.pallas_call(
        band_kernel,
        out_shape=tuple(
            jax.ShapeDtypeStruct((27, r * SUB, DEPTH), jnp.float32) for r in (3, 2, 2, 2)
        ),
        in_specs=[smem],
        out_specs=(vmem,) * 4,
        compiler_params=pltpu.CompilerParams(vmem_limit_bytes=SMALL_VMEM),
        name="bands",
    )(pltpu.with_memory_space_constraint(entries, pltpu.HBM))
    main, z_first, z_second = pl.pallas_call(
        functools.partial(pack_kernel, planes),
        out_shape=(
            jax.ShapeDtypeStruct((FIELDS * planes, SUB, LANES), jnp.float32),
            tile,
            tile,
        ),
        in_specs=[pl.BlockSpec(memory_space=pltpu.HBM)] * 5,
        out_specs=(vmem, vmem, vmem),
        scratch_shapes=[
            pltpu.SMEM(visc_table.shape, visc_table.dtype),
            pltpu.SMEM(entries.shape, entries.dtype),
            pltpu.VMEM(rhs_velocity.shape, rhs_velocity.dtype),
            pltpu.VMEM(rhs_pressure.shape, rhs_pressure.dtype),
            pltpu.VMEM(layer_ids.shape, layer_ids.dtype),
            pltpu.SemaphoreType.DMA((5,)),
        ],
        compiler_params=pltpu.CompilerParams(vmem_limit_bytes=SMALL_VMEM),
        name="pack",
    )(
        *(
            pltpu.with_memory_space_constraint(v, pltpu.HBM)
            for v in (visc_table, entries, rhs_velocity, rhs_pressure, layer_ids)
        )
    )

    halo = matched(z_first, "gz", first_pairs(z_count))
    halo = halo + matched(z_second, "gz", second_pairs(z_count))
    block = jnp.concatenate([main, halo])

    paired = x_count == 2
    if paired:
        frame = jnp.stack([block, lax.ppermute(block, "gx", [(0, 1), (1, 0)])])
        blocks = 2
    else:
        hops = -(-REACH // planes)
        parts = []
        for hop in range(-hops, hops + 1):
            pairs = [(i, i - hop) for i in range(x_count) if 0 <= i - hop < x_count]
            parts.append(block if hop == 0 else matched(block, "gx", pairs))
        frame = jnp.stack(parts)
        blocks = 2 * hops + 1

    y_first = matched(frame, "gy", first_pairs(y_count))
    y_second = matched(frame, "gy", second_pairs(y_count))

    stride = LANES + 2 * COLS
    tiles = -(-planes * blocks * stride // LANES)
    f32 = jnp.float32
    return pl.pallas_call(
        functools.partial(cycle_kernel, planes, blocks, paired),
        out_shape=(
            jax.ShapeDtypeStruct(rhs_velocity.shape, f32),
            jax.ShapeDtypeStruct(rhs_pressure.shape, f32),
        ),
        in_specs=[vmem] * 7,
        out_specs=(vmem, vmem),
        scratch_shapes=[
            pltpu.VMEM((FIELDS, tiles, ROWS, LANES), f32),
            pltpu.VMEM((3, tiles, ROWS, LANES), f32),
            pltpu.VMEM((DEPTH, tiles * LANES), f32),
            pltpu.VMEM((tiles + 2 * PAD, 27 * ROWS, LANES), f32),
            pltpu.VMEM((3, tiles, ROWS, LANES), f32),
            pltpu.VMEM((3, tiles, 2 * SUB, LANES), f32),
            pltpu.VMEM((4, tiles, 2 * SUB, LANES), f32),
            pltpu.VMEM((tiles + 2 * PAD, ROWS, LANES), f32),
            pltpu.VMEM((4, tiles + 1, SUB, LANES), f32),
        ],
        compiler_params=pltpu.CompilerParams(vmem_limit_bytes=CYCLE_VMEM),
        name="cycle",
    )(frame, y_first, y_second, *bands)


def solution(mesh):
    placed = (P(None, "gx", "gy", "gz"), P("gx", "gy", "gz"), P("gx", "gy", "gz"), P(), P())
    return jax.shard_map(
        on_device,
        mesh=mesh,
        in_specs=placed,
        out_specs=(P(None, "gx", "gy", "gz"), P("gx", "gy", "gz")),
        check_vma=False,
    )
```

```python
import functools

import jax
import jax.numpy as jnp
from jax import lax
from jax.experimental import pallas as pl
from jax.experimental.pallas import tpu as pltpu
from jax.sharding import PartitionSpec as P

LOW_BOUND = 0.2
HIGH_BOUND = 1.8

SUB = 8
LANES = 128
COLS = 8
REACH = 6
FIELDS = 5
LEAD = 2
STRIP = 4 * COLS
ROWS = 3 * SUB
OWN = SUB
ROWS_RESID = OWN - 4
ROWS_START = OWN - 2
ROWS_MIDDLE = OWN - 1
DEPTH = 2 * LANES
PIECE = 9 * SUB * 3
SMALL_VMEM = 4 * 1024 * 1024
CYCLE_VMEM = 32 * 1024 * 1024


def cheb_consts():
    theta = (HIGH_BOUND + LOW_BOUND) / 2.0
    delta = (HIGH_BOUND - LOW_BOUND) / 2.0
    sigma = theta / delta
    rho_zero = 1.0 / sigma
    rho_one = 1.0 / (2.0 * sigma - rho_zero)
    return (theta, delta, rho_zero, rho_one)


def first_pairs(count):
    return [(i, i ^ 1) for i in range(count) if i ^ 1 < count]


def second_pairs(count):
    pairs = []
    for i in range(1, count - 1, 2):
        pairs += [(i, i + 1), (i + 1, i)]
    return pairs


def matched(block, axis, pairs):
    if not pairs:
        return jnp.zeros_like(block)
    return lax.ppermute(block, axis, pairs)


def lane_iota():
    return lax.broadcasted_iota(jnp.int32, (SUB, LANES), 1)


def diagonal_mean(stencil_ref):
    middle = stencil_ref.shape[2] // 2
    return (stencil_ref[0, 0, middle] + stencil_ref[1, 1, middle] + stencil_ref[2, 2, middle]) / 3.0


def band_kernel(stencil_ref, smooth_ref, resid_ref, coarse_ref, middle_ref):
    scale = 1.0 / jnp.full((SUB, LANES), diagonal_mean(stencil_ref), jnp.float32)
    sub = lax.broadcasted_iota(jnp.int32, (SUB, LANES), 0)
    lane = lane_iota()
    zero = jnp.zeros((SUB, LANES), jnp.float32)
    halves = []
    for half in range(DEPTH // LANES):
        spot = lane + half * LANES
        groups = range(half * LANES // ROWS, min(((half + 1) * LANES - 1) // ROWS, 8) + 1)
        start = jnp.full((SUB, LANES), groups[0] * ROWS, jnp.int32)
        for n in groups[1:]:
            start = jnp.where(spot >= n * ROWS, n * ROWS, start)
        reach = jnp.where(spot < 9 * ROWS, spot - start - sub, 1000)
        halves.append((reach, [(n, start == n * ROWS) for n in groups]))
    for c in range(3):
        for i in range(3):
            rows_of = []
            for b in range(3):
                row = []
                for reach, groups in halves:
                    full = zero
                    for n, here in groups:
                        a, j = divmod(n, 3)
                        full = jnp.where(here, stencil_ref[i, j, 9 * a + 3 * b + c], full)
                    full = scale * full
                    high = full.astype(jnp.bfloat16).astype(jnp.float32)
                    row.append((high, full - high))
                rows_of.append(row)
            for ref, start, step in (
                (smooth_ref, 0, 1),
                (resid_ref, ROWS_RESID, 1),
                (coarse_ref, ROWS_START, 2),
                (middle_ref, ROWS_MIDDLE, 1),
            ):
                for r in range(ref.shape[1] // SUB):
                    for half, (reach, _) in enumerate(halves):
                        high, low = zero, zero
                        for b in range(3):
                            here = reach == r * SUB + start + step * (b - 1)
                            high = jnp.where(here, rows_of[b][half][0], high)
                            low = jnp.where(here, rows_of[b][half][1], low)
                        for term, value in enumerate((high, low, high)):
                            at = (2 * term + half) * LANES
                            ref[c * 3 + i, r * SUB : (r + 1) * SUB, at : at + LANES] = value


def pack_kernel(
    planes,
    visc_hbm,
    stencil_hbm,
    rhs_hbm,
    press_hbm,
    ids_hbm,
    main_ref,
    a_ref,
    b_ref,
    visc_ref,
    stencil_ref,
    rhs_ref,
    press_ref,
    ids_ref,
    arrived,
):
    copies = [
        pltpu.make_async_copy(src, dst, arrived.at[n])
        for n, (src, dst) in enumerate(
            (
                (visc_hbm, visc_ref),
                (stencil_hbm, stencil_ref),
                (ids_hbm, ids_ref),
                (rhs_hbm, rhs_ref),
                (press_hbm, press_ref),
            )
        )
    ]
    for copy in copies:
        copy.start()
    for copy in copies:
        copy.wait()
    lane = lane_iota()
    odd = lax.axis_index("gz") % 2 == 1
    kc = jnp.full((SUB, LANES), diagonal_mean(stencil_ref), jnp.float32)
    zero = jnp.zeros((SUB, LANES), jnp.float32)
    up, down, own = [zero] * FIELDS, [zero] * FIELDS, [zero] * FIELDS
    for p in range(planes):
        ids = ids_ref[p]
        eta = jnp.zeros((SUB, LANES), jnp.float32)
        for layer in range(visc_ref.shape[0]):
            eta = jnp.where(ids == layer, visc_ref[layer], eta)
        dinv = 1.0 / (eta * kc)
        values = [rhs_ref[j, p] * dinv for j in range(3)]
        values += [eta, eta * press_ref[p] * (1.0 / 9.0)]
        quarter = lane // COLS - p * (STRIP // COLS)
        for f in range(FIELDS):
            main_ref[f * planes + p] = values[f]
            near = pltpu.roll(values[f], (p * STRIP + COLS) % LANES, 1)
            far = pltpu.roll(values[f], (p * STRIP + 3 * COLS) % LANES, 1)
            up[f] = jnp.where(quarter == 0, near, up[f])
            own[f] = jnp.where(quarter == 1, near, jnp.where(quarter == 2, far, own[f]))
            down[f] = jnp.where(quarter == 3, far, down[f])
    for f in range(FIELDS):
        main_ref[FIELDS * planes + f] = own[f]
        a_ref[f] = jnp.where(odd, down[f], up[f])
        b_ref[f] = jnp.where(odd, up[f], down[f])


def cycle_kernel(
    planes,
    blocks,
    paired,
    own_ref,
    a_ref,
    b_ref,
    smooth_ref,
    resid_band,
    coarse_ref,
    middle_ref,
    vel_ref,
    press_ref,
    fields,
    work,
    split,
    products,
    edge,
    second_x,
    resid,
    press,
):
    theta, delta, rho_zero, rho_one = cheb_consts()
    weight = 2.0 * rho_one / delta
    carry = rho_one * rho_zero
    total = planes * blocks
    strips = total + 2 * LEAD
    lane = lane_iota()
    zero = jnp.zeros((SUB, LANES), jnp.float32)
    gx = lax.axis_index("gx")
    y_odd = lax.axis_index("gy") % 2 == 1

    def span(grow):
        if paired:
            low = (0, min(planes - 1 + grow, total - 1))
            high = max(planes - grow, 0)
            return gx * high, low[1] + 1
        own = blocks // 2
        lo = max(own * planes - grow, 0)
        return lo, min((own + 1) * planes + grow, total) - lo

    def place(plane):
        if isinstance(plane, int):
            return plane // planes, plane % planes
        block = lax.div(plane, planes)
        return block, plane - block * planes

    def slot(q):
        return (q + gx) % 2 if paired else q

    for k in [*range(LEAD), *range(LEAD + total, strips)]:
        for r in range(3):
            for j in range(3):
                work[j, k, r * SUB : (r + 1) * SUB, :] = zero
            press[k, r * SUB : (r + 1) * SUB, :] = zero

    def assemble(src, row):
        at = slice(row, row + SUB)
        for q in range(blocks):
            here = slot(q)
            for f in range(FIELDS):
                for p in range(planes + 1):
                    strip = p == planes
                    index = FIELDS * planes + f if strip else f * planes + p
                    value = src[here, index]
                    fields[f, total + q if strip else q * planes + p, at, :] = value
                    spot = strips + q if strip else LEAD + q * planes + p
                    if f < 3:
                        work[f, spot, at, :] = value
                    if f == 4:
                        press[spot, at, :] = value

    assemble(own_ref, OWN)

    @pl.when(y_odd)
    def _():
        assemble(a_ref, OWN - SUB)
        assemble(b_ref, OWN + SUB)

    @pl.when(jnp.logical_not(y_odd))
    def _():
        assemble(b_ref, OWN - SUB)
        assemble(a_ref, OWN + SUB)

    def strip_shift(tiles_of, offset):
        turn = (LANES - offset * STRIP) % LANES
        turned = [pltpu.roll(v, turn, 1) for v in tiles_of] + [zero]
        shifted = []
        for q in range(blocks):
            if offset > 0:
                shifted.append(jnp.where(lane < LANES - offset * STRIP, turned[q], turned[q + 1]))
            else:
                shifted.append(jnp.where(lane >= -offset * STRIP, turned[q], turned[q - 1]))
        return shifted

    def edge_source(ahead, behind, scale):
        moved = pltpu.roll(behind, 2 * COLS + 2 * scale, 1)
        far = lane % STRIP
        return jnp.where((far >= 3 * COLS + scale) & (far < 3 * COLS + 2 * scale), moved, ahead)

    def edge_turn(p, scale):
        return LANES - 3 * COLS - scale - STRIP * p

    def z_shifts(ahead, behind, source, p, scale):
        outer = pltpu.roll(source, edge_turn(p, scale), 1)
        ahead = pltpu.roll(ahead, LANES - scale, 1)
        behind = pltpu.roll(behind, scale, 1)
        return jnp.where(lane >= LANES - scale, outer, ahead) + jnp.where(
            lane < scale, outer, behind
        )

    def parts_of(v):
        high = v.astype(jnp.bfloat16).astype(jnp.float32)
        return high, v - high

    blank = jnp.zeros((DEPTH - PIECE, 2 * LANES), jnp.float32)

    def product(band, high, low):
        width = high.shape[1]
        return jnp.dot(
            band,
            jnp.concatenate(
                [high, blank[:, :width], high, blank[:, :width], low, blank[:, :width]]
            ),
            preferred_element_type=jnp.float32,
            precision=lax.Precision.DEFAULT,
        )

    def apply(base, count, band_ref, first, rows, scale, emit, with_strips=True):
        height = rows * SUB
        half = -(-count // 2)
        band = band_ref[:, first : first + height, :].reshape(9 * height, 3 * DEPTH)
        for n in range(half + 2 * scale):
            for side in range(2):
                for j in range(3):
                    for r in range(3):
                        spot = LEAD + base - scale + side * half + n
                        high, low = parts_of(work[j, spot, r * SUB : (r + 1) * SUB, :])
                        at = ((n * 3 + j) * 3 + r) * SUB
                        lanes = slice(side * LANES, (side + 1) * LANES)
                        split[0, at : at + SUB, lanes] = high
                        split[1, at : at + SUB, lanes] = low
        size = 9 * SUB
        for q in range(0, blocks, 2):
            width = min(2, blocks - q)
            pieces = []
            for a in range(3):
                for j in range(3):
                    for r in range(3):
                        tiles_of = [
                            work[j, strips + p, r * SUB : (r + 1) * SUB, :] for p in range(blocks)
                        ]
                        if a != 1:
                            tiles_of = strip_shift(tiles_of, (a - 1) * scale)
                        pieces.append([parts_of(v) for v in tiles_of[q : q + width]])
            high, low = (
                jnp.concatenate(
                    [jnp.concatenate([v[n] for v in piece], axis=1) for piece in pieces]
                )
                for n in range(2)
            )
            made = product(band, high, low)
            for w in range(width):
                products[total + 2 + q + w, : 9 * height, :] = made[:, w * LANES : (w + 1) * LANES]
        for n in range(half):
            high, low = (
                jnp.concatenate(
                    [
                        split[part, (n + a * scale) * size : (n + a * scale + 1) * size, :]
                        for a in range(3)
                    ]
                )
                for part in range(2)
            )
            made = product(band, high, low)
            for side in range(2):
                products[n + side * half, : 9 * height, :] = made[
                    :, side * LANES : (side + 1) * LANES
                ]

        def of(k, c, i, r):
            at = (c * 3 + i) * height + r * SUB
            return products[k, at : at + SUB, :]

        for i in range(3):
            for r in range(rows):
                for q in range(blocks):
                    behind, middle, ahead = (of(total + 2 + q, c, i, r) for c in range(3))
                    at = (i * 3 + r) * SUB
                    edge[q, at : at + SUB, :] = edge_source(ahead, behind, scale)
                    if with_strips:
                        middle = middle + pltpu.roll(ahead, LANES - scale, 1)
                        middle = middle + pltpu.roll(behind, scale, 1)
                        emit(total + q, strips + q, None, r, i, middle)
        for i in range(3):
            for r in range(rows):
                for k in range(count):
                    q, p = place(base + k)
                    behind, middle, ahead = (of(k, c, i, r) for c in range(3))
                    at = (i * 3 + r) * SUB
                    sides = z_shifts(ahead, behind, edge[q, at : at + SUB, :], p, scale)
                    emit(base + k, LEAD + base + k, k, r, i, middle + sides)

    def inside(t, row):
        return fields[3, t, row : row + SUB, :] > 0.0

    def emit_first(t, w, k, r, i, total_of):
        at = slice(r * SUB, (r + 1) * SUB)
        value = (1.0 + carry + weight) * fields[i, t, at, :] - weight * total_of
        value = jnp.where(inside(t, r * SUB), value, 0.0)
        work[i, w, at, :] = value
        second_x[i, t, at, :] = value

    apply(0, total, smooth_ref, 0, 3, 1, emit_first)

    lane_even = lane % 2 == 0
    row_even = lax.broadcasted_iota(jnp.int32, (SUB, LANES), 0) % 2 == 0

    def pair_sums(v):
        v = v + jnp.where(row_even, pltpu.roll(v, SUB - 1, 0), pltpu.roll(v, 1, 0))
        return v + jnp.where(lane_even, pltpu.roll(v, LANES - 1, 1), pltpu.roll(v, 1, 1))

    def emit_resid(t, w, k, r, i, total_of):
        at = slice(ROWS_RESID + r * SUB, ROWS_RESID + (r + 1) * SUB)
        value = fields[3, t, at, :] * (fields[i, t, at, :] - total_of)
        resid[i, t, r * SUB : (r + 1) * SUB, :] = pair_sums(value)

    apply(0, total, resid_band, 0, 2, 1, emit_resid)

    plane_even = lane // STRIP % 2 == 0
    for r in range(2):
        at = slice(ROWS_RESID + r * SUB, ROWS_RESID + (r + 1) * SUB)
        rows_at = slice(r * SUB, (r + 1) * SUB)
        for t in [*range(0, total, 2), *range(total, total + blocks)]:
            weigh = None
            for f in (3, 0, 1, 2):
                def load(k):
                    if f == 3:
                        return pair_sums(fields[3, k, at, :])
                    return resid[f, k, rows_at, :]

                v = load(t)
                if t < total:
                    v = v + load(t + 1)
                else:
                    ahead = pltpu.roll(v, LANES - STRIP, 1)
                    v = v + jnp.where(plane_even, ahead, pltpu.roll(v, STRIP, 1))
                if f == 3:
                    weigh = jnp.where(v > 0.0, 4.0 / v, 0.0)
                elif t < total:
                    work[f, LEAD + t, at, :] = v * weigh
                    work[f, LEAD + t + 1, at, :] = v * weigh
                else:
                    work[f, strips + t - total, at, :] = v * weigh

    def emit_start(t, w, k, r, i, total_of):
        at = slice(ROWS_START + r * SUB, ROWS_START + (r + 1) * SUB)
        value = second_x[i, t, at, :] + (1.0 + carry + weight) * work[i, w, at, :]
        value = jnp.where(inside(t, ROWS_START + r * SUB), value - weight * total_of, 0.0)
        work[i, w, at, :] = value

    apply(*span(2), coarse_ref, 0, 2, 2, emit_start)

    def emit_middle(t, w, k, r, i, total_of):
        at = slice(ROWS_MIDDLE + r * SUB, ROWS_MIDDLE + (r + 1) * SUB)
        step = jnp.where(inside(t, ROWS_MIDDLE + r * SUB), fields[i, t, at, :] - total_of, 0.0)
        work[i, w, at, :] = work[i, w, at, :] + step
        second_x[i, t, at, :] = step

    apply(*span(1), middle_ref, 0, 2, 1, emit_middle)

    own = slice(OWN, OWN + SUB)

    def emit_last(t, w, k, r, i, total_of):
        value = work[i, w, own, :] + carry * second_x[i, t, own, :]
        vel_ref[i, k] = value + weight * (fields[i, t, own, :] - total_of)

    apply(*span(0), smooth_ref, OWN, 1, 1, emit_last, with_strips=False)

    def strip_sides(row):
        return [press[strips + q, row : row + SUB, :] for q in range(blocks)]

    def beside(k, row, at):
        v = press[LEAD + k, row - 1 : row - 1 + SUB, :]
        v = v + press[LEAD + k, row + 1 : row + 1 + SUB, :]
        v = v + press[LEAD + k - 1, row : row + SUB, :] + press[LEAD + k + 1, row : row + SUB, :]
        q, p = place(k)
        here = press[LEAD + k, row : row + SUB, :]
        return v + z_shifts(here, here, edge[q, at : at + SUB, :], p, 1)

    def set_edges(row, at):
        for q in range(blocks):
            v = press[strips + q, row : row + SUB, :]
            edge[q, at : at + SUB, :] = edge_source(v, v, 1)

    starts = (OWN - 1, OWN + 1)
    base, count = span(1)
    news = []
    for n, row in enumerate(starts):
        set_edges(row, n * SUB)
        tiles_of = strip_sides(row)
        far = strip_shift(tiles_of, 1), strip_shift(tiles_of, -1)
        for q in range(blocks):
            v = press[strips + q, row - 1 : row - 1 + SUB, :]
            v = v + press[strips + q, row + 1 : row + 1 + SUB, :] + far[0][q] + far[1][q]
            v = v + pltpu.roll(tiles_of[q], LANES - 1, 1) + pltpu.roll(tiles_of[q], 1, 1)
            news.append((total + q, strips + q, row, v))
        for k in range(count):
            news.append((base + k, LEAD + base + k, row, beside(base + k, row, n * SUB)))
    for n, (t, w, row, near) in enumerate(news):
        v = fields[4, t, row : row + SUB, :] * (4.0 / 3.0) + near * (1.0 / 9.0)
        resid[0, n, :SUB, :] = jnp.where(inside(t, row), v, 0.0)
    for n, (t, w, row, near) in enumerate(news):
        press[w, row : row + SUB, :] = resid[0, n, :SUB, :]
    base, count = span(0)
    set_edges(OWN, 0)
    for k in range(count):
        v = press[LEAD + base + k, own, :] * (1.0 / 3.0) + fields[4, base + k, own, :]
        press_ref[k] = v + beside(base + k, OWN, 0) * (1.0 / 9.0)


def on_device(rhs_velocity, rhs_pressure, layer_ids, visc_table, stencil):
    planes, rows, depth = rhs_pressure.shape
    assert rows == SUB and depth == LANES and planes * STRIP == LANES
    x_count, y_count, z_count = (lax.axis_size(n) for n in ("gx", "gy", "gz"))
    entries = jnp.transpose(stencil, (1, 2, 0))

    tile = jax.ShapeDtypeStruct((FIELDS, SUB, LANES), jnp.float32)
    vmem = pl.BlockSpec(memory_space=pltpu.VMEM)
    smem = pl.BlockSpec(memory_space=pltpu.SMEM)
    bands = pl.pallas_call(
        band_kernel,
        out_shape=tuple(
            jax.ShapeDtypeStruct((9, r * SUB, 3 * DEPTH), jnp.float32) for r in (3, 2, 2, 2)
        ),
        in_specs=[smem],
        out_specs=(vmem,) * 4,
        compiler_params=pltpu.CompilerParams(vmem_limit_bytes=SMALL_VMEM),
        name="bands",
    )(pltpu.with_memory_space_constraint(entries, pltpu.HBM))
    main, z_first, z_second = pl.pallas_call(
        functools.partial(pack_kernel, planes),
        out_shape=(
            jax.ShapeDtypeStruct((FIELDS * (planes + 1), SUB, LANES), jnp.float32),
            tile,
            tile,
        ),
        in_specs=[pl.BlockSpec(memory_space=pltpu.HBM)] * 5,
        out_specs=(vmem, vmem, vmem),
        scratch_shapes=[
            pltpu.SMEM(visc_table.shape, visc_table.dtype),
            pltpu.SMEM(entries.shape, entries.dtype),
            pltpu.VMEM(rhs_velocity.shape, rhs_velocity.dtype),
            pltpu.VMEM(rhs_pressure.shape, rhs_pressure.dtype),
            pltpu.VMEM(layer_ids.shape, layer_ids.dtype),
            pltpu.SemaphoreType.DMA((5,)),
        ],
        compiler_params=pltpu.CompilerParams(vmem_limit_bytes=SMALL_VMEM),
        name="pack",
    )(
        *(
            pltpu.with_memory_space_constraint(v, pltpu.HBM)
            for v in (visc_table, entries, rhs_velocity, rhs_pressure, layer_ids)
        )
    )

    halo = matched(z_first, "gz", first_pairs(z_count))
    halo = halo + matched(z_second, "gz", second_pairs(z_count))
    inner = FIELDS * planes
    block = jnp.concatenate([main[:inner], main[inner:] + halo])

    paired = x_count == 2
    if paired:
        frame = jnp.stack([block, lax.ppermute(block, "gx", [(0, 1), (1, 0)])])
        blocks = 2
    else:
        hops = -(-REACH // planes)
        parts = []
        for hop in range(-hops, hops + 1):
            pairs = [(i, i - hop) for i in range(x_count) if 0 <= i - hop < x_count]
            parts.append(block if hop == 0 else matched(block, "gx", pairs))
        frame = jnp.stack(parts)
        blocks = 2 * hops + 1

    y_first = matched(frame, "gy", first_pairs(y_count))
    y_second = matched(frame, "gy", second_pairs(y_count))

    total = planes * blocks
    tiles = total + blocks
    f32 = jnp.float32
    return pl.pallas_call(
        functools.partial(cycle_kernel, planes, blocks, paired),
        out_shape=(
            jax.ShapeDtypeStruct(rhs_velocity.shape, f32),
            jax.ShapeDtypeStruct(rhs_pressure.shape, f32),
        ),
        in_specs=[vmem] * 7,
        out_specs=(vmem, vmem),
        scratch_shapes=[
            pltpu.VMEM((FIELDS, tiles, ROWS, LANES), f32),
            pltpu.VMEM((3, tiles + 2 * LEAD, ROWS, LANES), f32),
            pltpu.VMEM((2, (total // 2 + 2 * LEAD) * 9 * SUB, 2 * LANES), f32),
            pltpu.VMEM((tiles + 2, 9 * ROWS, LANES), f32),
            pltpu.VMEM((blocks, 3 * ROWS, LANES), f32),
            pltpu.VMEM((3, tiles, ROWS, LANES), f32),
            pltpu.VMEM((3, 2 * tiles, 2 * SUB, LANES), f32),
            pltpu.VMEM((tiles + 2 * LEAD, ROWS, LANES), f32),
        ],
        compiler_params=pltpu.CompilerParams(vmem_limit_bytes=CYCLE_VMEM),
        name="cycle",
    )(frame, y_first, y_second, *bands)


def solution(mesh):
    placed = (P(None, "gx", "gy", "gz"), P("gx", "gy", "gz"), P("gx", "gy", "gz"), P(), P())
    return jax.shard_map(
        on_device,
        mesh=mesh,
        in_specs=placed,
        out_specs=(P(None, "gx", "gy", "gz"), P("gx", "gy", "gz")),
        check_vma=False,
    )
```

```python
import functools

import jax
import jax.numpy as jnp
from jax import lax
from jax.experimental import pallas as pl
from jax.experimental.pallas import tpu as pltpu
from jax.sharding import PartitionSpec as P

LOW_BOUND = 0.2
HIGH_BOUND = 1.8

SUB = 8
LANES = 128
COLS = 8
REACH = 6
PRESS_REACH = 2
FIELDS = 5
LEAD = 2
STRIP = 4 * COLS
ROWS = 3 * SUB
OWN = SUB
ROWS_RESID = OWN - 4
ROWS_START = OWN - 2
ROWS_MIDDLE = OWN - 1
DEPTH = 2 * LANES
PIECE = 9 * SUB * 3
SMALL_VMEM = 4 * 1024 * 1024
CYCLE_VMEM = 32 * 1024 * 1024


def cheb_consts():
    theta = (HIGH_BOUND + LOW_BOUND) / 2.0
    delta = (HIGH_BOUND - LOW_BOUND) / 2.0
    sigma = theta / delta
    rho_zero = 1.0 / sigma
    rho_one = 1.0 / (2.0 * sigma - rho_zero)
    return (theta, delta, rho_zero, rho_one)


def first_pairs(count):
    return [(i, i ^ 1) for i in range(count) if i ^ 1 < count]


def second_pairs(count):
    pairs = []
    for i in range(1, count - 1, 2):
        pairs += [(i, i + 1), (i + 1, i)]
    return pairs


def matched(block, axis, pairs):
    if not pairs:
        return jnp.zeros_like(block)
    return lax.ppermute(block, axis, pairs)


def lane_iota():
    return lax.broadcasted_iota(jnp.int32, (SUB, LANES), 1)


def diagonal_mean(stencil_ref):
    middle = stencil_ref.shape[2] // 2
    return (stencil_ref[0, 0, middle] + stencil_ref[1, 1, middle] + stencil_ref[2, 2, middle]) / 3.0


def band_kernel(stencil_ref, smooth_ref, resid_ref, coarse_ref, middle_ref):
    scale = 1.0 / jnp.full((SUB, LANES), diagonal_mean(stencil_ref), jnp.float32)
    sub = lax.broadcasted_iota(jnp.int32, (SUB, LANES), 0)
    lane = lane_iota()
    zero = jnp.zeros((SUB, LANES), jnp.float32)
    halves = []
    for half in range(DEPTH // LANES):
        spot = lane + half * LANES
        groups = range(half * LANES // ROWS, min(((half + 1) * LANES - 1) // ROWS, 8) + 1)
        start = jnp.full((SUB, LANES), groups[0] * ROWS, jnp.int32)
        for n in groups[1:]:
            start = jnp.where(spot >= n * ROWS, n * ROWS, start)
        reach = jnp.where(spot < 9 * ROWS, spot - start - sub, 1000)
        halves.append((reach, [(n, start == n * ROWS) for n in groups]))
    for c in range(3):
        for i in range(3):
            rows_of = []
            for b in range(3):
                row = []
                for reach, groups in halves:
                    full = zero
                    for n, here in groups:
                        a, j = divmod(n, 3)
                        full = jnp.where(here, stencil_ref[i, j, 9 * a + 3 * b + c], full)
                    full = scale * full
                    high = full.astype(jnp.bfloat16).astype(jnp.float32)
                    row.append((high, full - high))
                rows_of.append(row)
            for ref, start, step in (
                (smooth_ref, 0, 1),
                (resid_ref, ROWS_RESID, 1),
                (coarse_ref, ROWS_START, 2),
                (middle_ref, ROWS_MIDDLE, 1),
            ):
                for r in range(ref.shape[1] // SUB):
                    for half, (reach, _) in enumerate(halves):
                        high, low = zero, zero
                        for b in range(3):
                            here = reach == r * SUB + start + step * (b - 1)
                            high = jnp.where(here, rows_of[b][half][0], high)
                            low = jnp.where(here, rows_of[b][half][1], low)
                        for term, value in enumerate((high, low, high)):
                            at = (2 * term + half) * LANES
                            ref[c * 3 + i, r * SUB : (r + 1) * SUB, at : at + LANES] = value


def pack_kernel(
    planes,
    visc_hbm,
    stencil_hbm,
    rhs_hbm,
    press_hbm,
    ids_hbm,
    main_ref,
    a_ref,
    b_ref,
    visc_ref,
    stencil_ref,
    rhs_ref,
    press_ref,
    ids_ref,
    arrived,
):
    copies = [
        pltpu.make_async_copy(src, dst, arrived.at[n])
        for n, (src, dst) in enumerate(
            (
                (visc_hbm, visc_ref),
                (stencil_hbm, stencil_ref),
                (ids_hbm, ids_ref),
                (rhs_hbm, rhs_ref),
                (press_hbm, press_ref),
            )
        )
    ]
    for copy in copies:
        copy.start()
    for copy in copies:
        copy.wait()
    lane = lane_iota()
    odd = lax.axis_index("gz") % 2 == 1
    kc = jnp.full((SUB, LANES), diagonal_mean(stencil_ref), jnp.float32)
    zero = jnp.zeros((SUB, LANES), jnp.float32)
    up, down, own = [zero] * FIELDS, [zero] * FIELDS, [zero] * FIELDS
    for p in range(planes):
        ids = ids_ref[p]
        eta = jnp.zeros((SUB, LANES), jnp.float32)
        for layer in range(visc_ref.shape[0]):
            eta = jnp.where(ids == layer, visc_ref[layer], eta)
        dinv = 1.0 / (eta * kc)
        values = [rhs_ref[j, p] * dinv for j in range(3)]
        values += [eta, eta * press_ref[p] * (1.0 / 9.0)]
        quarter = lane // COLS - p * (STRIP // COLS)
        for f in range(FIELDS):
            main_ref[f * planes + p] = values[f]
            near = pltpu.roll(values[f], (p * STRIP + COLS) % LANES, 1)
            far = pltpu.roll(values[f], (p * STRIP + 3 * COLS) % LANES, 1)
            up[f] = jnp.where(quarter == 0, near, up[f])
            own[f] = jnp.where(quarter == 1, near, jnp.where(quarter == 2, far, own[f]))
            down[f] = jnp.where(quarter == 3, far, down[f])
    for f in range(FIELDS):
        main_ref[FIELDS * planes + f] = own[f]
        a_ref[f] = jnp.where(odd, down[f], up[f])
        b_ref[f] = jnp.where(odd, up[f], down[f])


def packed_row(planes, f, p):
    if f < FIELDS - 1:
        return (f * (planes + 1) + p) * REACH
    return (FIELDS - 1) * (planes + 1) * REACH + p * PRESS_REACH


def packed_rows(planes):
    return -(-packed_row(planes, FIELDS - 1, planes + 1) // SUB) * SUB


def message_kernel(planes, blocks, *refs):
    parts, (a_ref, b_ref) = refs[:blocks], refs[blocks:]
    odd = lax.axis_index("gy") % 2 == 1
    rows = packed_rows(planes)

    def pack(to_low, to_high):
        for q in range(blocks):
            for ref in (to_low, to_high):
                ref[q, rows - SUB :, :] = jnp.zeros((SUB, LANES), jnp.float32)
            for f in range(FIELDS):
                count = REACH if f < FIELDS - 1 else PRESS_REACH
                for p in range(planes + 1):
                    index = FIELDS * planes + f if p == planes else f * planes + p
                    at = packed_row(planes, f, p)
                    to_low[q, at : at + count, :] = parts[q][index, :count, :]
                    to_high[q, at : at + count, :] = parts[q][index, SUB - count :, :]

    @pl.when(odd)
    def _():
        pack(a_ref, b_ref)

    @pl.when(jnp.logical_not(odd))
    def _():
        pack(b_ref, a_ref)


def cycle_kernel(
    planes,
    blocks,
    paired,
    own_ref,
    a_ref,
    b_ref,
    smooth_ref,
    resid_band,
    coarse_ref,
    middle_ref,
    vel_ref,
    press_ref,
    fields,
    work,
    split,
    products,
    edge,
    second_x,
    resid,
    press,
):
    _, delta, rho_zero, rho_one = cheb_consts()
    weight = 2.0 * rho_one / delta
    carry = rho_one * rho_zero
    total = planes * blocks
    strips = total + 2 * LEAD
    lane = lane_iota()
    zero = jnp.zeros((SUB, LANES), jnp.float32)
    gx = lax.axis_index("gx")
    y_odd = lax.axis_index("gy") % 2 == 1

    def span(grow):
        if paired:
            low = (0, min(planes - 1 + grow, total - 1))
            high = max(planes - grow, 0)
            return gx * high, low[1] + 1
        own = blocks // 2
        lo = max(own * planes - grow, 0)
        return lo, min((own + 1) * planes + grow, total) - lo

    def place(plane):
        if isinstance(plane, int):
            return plane // planes, plane % planes
        block = lax.div(plane, planes)
        return block, plane - block * planes

    def slot(q):
        return (q + gx) % 2 if paired else q

    for k in [*range(LEAD), *range(LEAD + total, strips)]:
        for r in range(3):
            for j in range(3):
                work[j, k, r * SUB : (r + 1) * SUB, :] = zero
            press[k, r * SUB : (r + 1) * SUB, :] = zero

    def assemble(row, tile_of):
        at = slice(row, row + SUB)
        for q in range(blocks):
            here = slot(q)
            for f in range(FIELDS):
                for p in range(planes + 1):
                    strip = p == planes
                    value = tile_of(here, f, p)
                    fields[f, total + q if strip else q * planes + p, at, :] = value
                    spot = strips + q if strip else LEAD + q * planes + p
                    if f < 3:
                        work[f, spot, at, :] = value
                    if f == 4:
                        press[spot, at, :] = value

    def own_tile(q, f, p):
        return own_ref[q, FIELDS * planes + f if p == planes else f * planes + p]

    def low_tile(ref):
        def tile(q, f, p):
            count = REACH if f < FIELDS - 1 else PRESS_REACH
            at = packed_row(planes, f, p) + count - SUB
            if at < 0:
                return pltpu.roll(ref[q, :SUB, :], -at, 0)
            return ref[q, at : at + SUB, :]

        return tile

    def high_tile(ref):
        def tile(q, f, p):
            at = packed_row(planes, f, p)
            over = max(at + SUB - ref.shape[1], 0)
            v = ref[q, at - over : at - over + SUB, :]
            return pltpu.roll(v, SUB - over, 0) if over else v

        return tile

    assemble(OWN, own_tile)

    @pl.when(y_odd)
    def _():
        assemble(OWN - SUB, low_tile(a_ref))
        assemble(OWN + SUB, high_tile(b_ref))

    @pl.when(jnp.logical_not(y_odd))
    def _():
        assemble(OWN - SUB, low_tile(b_ref))
        assemble(OWN + SUB, high_tile(a_ref))

    def strip_shift(tiles_of, offset):
        turn = (LANES - offset * STRIP) % LANES
        turned = [pltpu.roll(v, turn, 1) for v in tiles_of] + [zero]
        shifted = []
        for q in range(blocks):
            if offset > 0:
                shifted.append(jnp.where(lane < LANES - offset * STRIP, turned[q], turned[q + 1]))
            else:
                shifted.append(jnp.where(lane >= -offset * STRIP, turned[q], turned[q - 1]))
        return shifted

    def edge_source(ahead, behind, scale):
        moved = pltpu.roll(behind, 2 * COLS + 2 * scale, 1)
        far = lane % STRIP
        return jnp.where((far >= 3 * COLS + scale) & (far < 3 * COLS + 2 * scale), moved, ahead)

    def edge_turn(p, scale):
        return LANES - 3 * COLS - scale - STRIP * p

    def z_shifts(ahead, behind, source, p, scale):
        outer = pltpu.roll(source, edge_turn(p, scale), 1)
        ahead = pltpu.roll(ahead, LANES - scale, 1)
        behind = pltpu.roll(behind, scale, 1)
        return jnp.where(lane >= LANES - scale, outer, ahead) + jnp.where(
            lane < scale, outer, behind
        )

    def parts_of(v):
        high = v.astype(jnp.bfloat16).astype(jnp.float32)
        return high, v - high

    blank = jnp.zeros((DEPTH - PIECE, 2 * LANES), jnp.float32)

    def product(band_of, high, low):
        width = high.shape[1]
        return jnp.dot(
            band_of(),
            jnp.concatenate(
                [high, blank[:, :width], high, blank[:, :width], low, blank[:, :width]]
            ),
            preferred_element_type=jnp.float32,
            precision=lax.Precision.DEFAULT,
        )

    def apply(base, count, band_ref, first, rows, scale, emit, with_strips=True):
        height = rows * SUB
        half = -(-count // 2)

        def band_of():
            return band_ref[:, first : first + height, :].reshape(9 * height, 3 * DEPTH)

        for n in range(half + 2 * scale):
            for side in range(2):
                for j in range(3):
                    for r in range(3):
                        spot = LEAD + base - scale + side * half + n
                        high, low = parts_of(work[j, spot, r * SUB : (r + 1) * SUB, :])
                        at = ((n * 3 + j) * 3 + r) * SUB
                        lanes = slice(side * LANES, (side + 1) * LANES)
                        split[0, at : at + SUB, lanes] = high
                        split[1, at : at + SUB, lanes] = low
        size = 9 * SUB
        for q in range(0, blocks, 2):
            width = min(2, blocks - q)
            pieces = []
            for a in range(3):
                for j in range(3):
                    for r in range(3):
                        tiles_of = [
                            work[j, strips + p, r * SUB : (r + 1) * SUB, :] for p in range(blocks)
                        ]
                        if a != 1:
                            tiles_of = strip_shift(tiles_of, (a - 1) * scale)
                        pieces.append([parts_of(v) for v in tiles_of[q : q + width]])
            high, low = (
                jnp.concatenate(
                    [jnp.concatenate([v[n] for v in piece], axis=1) for piece in pieces]
                )
                for n in range(2)
            )
            made = product(band_of, high, low)
            for w in range(width):
                products[total + 2 + q + w, : 9 * height, :] = made[:, w * LANES : (w + 1) * LANES]

        def of(k, c, i, r):
            at = (c * 3 + i) * height + r * SUB
            return products[k, at : at + SUB, :]

        for i in range(3):
            for r in range(rows):
                for q in range(blocks):
                    behind, middle, ahead = (of(total + 2 + q, c, i, r) for c in range(3))
                    at = (i * 3 + r) * SUB
                    edge[q, at : at + SUB, :] = edge_source(ahead, behind, scale)
                    if with_strips:
                        middle = middle + pltpu.roll(ahead, LANES - scale, 1)
                        middle = middle + pltpu.roll(behind, scale, 1)
                        emit(total + q, strips + q, None, r, i, middle)

        def finish(k):
            q, p = place(base + k)
            for i in range(3):
                for r in range(rows):
                    behind, middle, ahead = (of(k, c, i, r) for c in range(3))
                    at = (i * 3 + r) * SUB
                    sides = z_shifts(ahead, behind, edge[q, at : at + SUB, :], p, scale)
                    emit(base + k, LEAD + base + k, k, r, i, middle + sides)

        for n in range(half + 1):
            if n < half:
                high, low = (
                    jnp.concatenate(
                        [
                            split[part, (n + a * scale) * size : (n + a * scale + 1) * size, :]
                            for a in range(3)
                        ]
                    )
                    for part in range(2)
                )
                made = product(band_of, high, low)
                for side in range(2):
                    products[n + side * half, : 9 * height, :] = made[
                        :, side * LANES : (side + 1) * LANES
                    ]
            for side in range(2):
                if n and n - 1 + side * half < count:
                    finish(n - 1 + side * half)

    def inside(t, row):
        return fields[3, t, row : row + SUB, :] > 0.0

    def emit_first(t, w, k, r, i, total_of):
        at = slice(r * SUB, (r + 1) * SUB)
        value = (1.0 + carry + weight) * fields[i, t, at, :] - weight * total_of
        value = jnp.where(inside(t, r * SUB), value, 0.0)
        work[i, w, at, :] = value
        second_x[i, t, at, :] = value

    apply(0, total, smooth_ref, 0, 3, 1, emit_first)

    lane_even = lane % 2 == 0
    row_even = lax.broadcasted_iota(jnp.int32, (SUB, LANES), 0) % 2 == 0

    def pair_sums(v):
        v = v + jnp.where(row_even, pltpu.roll(v, SUB - 1, 0), pltpu.roll(v, 1, 0))
        return v + jnp.where(lane_even, pltpu.roll(v, LANES - 1, 1), pltpu.roll(v, 1, 1))

    def emit_resid(t, w, k, r, i, total_of):
        at = slice(ROWS_RESID + r * SUB, ROWS_RESID + (r + 1) * SUB)
        value = fields[3, t, at, :] * (fields[i, t, at, :] - total_of)
        resid[i, t, r * SUB : (r + 1) * SUB, :] = pair_sums(value)

    apply(0, total, resid_band, 0, 2, 1, emit_resid)

    plane_even = lane // STRIP % 2 == 0
    for r in range(2):
        at = slice(ROWS_RESID + r * SUB, ROWS_RESID + (r + 1) * SUB)
        rows_at = slice(r * SUB, (r + 1) * SUB)
        for t in [*range(0, total, 2), *range(total, total + blocks)]:
            weigh = None
            for f in (3, 0, 1, 2):
                def load(k):
                    if f == 3:
                        return pair_sums(fields[3, k, at, :])
                    return resid[f, k, rows_at, :]

                v = load(t)
                if t < total:
                    v = v + load(t + 1)
                else:
                    ahead = pltpu.roll(v, LANES - STRIP, 1)
                    v = v + jnp.where(plane_even, ahead, pltpu.roll(v, STRIP, 1))
                if f == 3:
                    weigh = jnp.where(v > 0.0, 4.0 / v, 0.0)
                elif t < total:
                    work[f, LEAD + t, at, :] = v * weigh
                    work[f, LEAD + t + 1, at, :] = v * weigh
                else:
                    work[f, strips + t - total, at, :] = v * weigh

    def emit_start(t, w, k, r, i, total_of):
        at = slice(ROWS_START + r * SUB, ROWS_START + (r + 1) * SUB)
        value = second_x[i, t, at, :] + (1.0 + carry + weight) * work[i, w, at, :]
        value = jnp.where(inside(t, ROWS_START + r * SUB), value - weight * total_of, 0.0)
        work[i, w, at, :] = value

    apply(*span(2), coarse_ref, 0, 2, 2, emit_start)

    def emit_middle(t, w, k, r, i, total_of):
        at = slice(ROWS_MIDDLE + r * SUB, ROWS_MIDDLE + (r + 1) * SUB)
        step = jnp.where(inside(t, ROWS_MIDDLE + r * SUB), fields[i, t, at, :] - total_of, 0.0)
        work[i, w, at, :] = work[i, w, at, :] + step
        second_x[i, t, at, :] = step

    apply(*span(1), middle_ref, 0, 2, 1, emit_middle)

    own = slice(OWN, OWN + SUB)

    def emit_last(t, w, k, r, i, total_of):
        value = work[i, w, own, :] + carry * second_x[i, t, own, :]
        vel_ref[i, k] = value + weight * (fields[i, t, own, :] - total_of)

    apply(*span(0), smooth_ref, OWN, 1, 1, emit_last, with_strips=False)

    def strip_sides(row):
        return [press[strips + q, row : row + SUB, :] for q in range(blocks)]

    def beside(k, row, at):
        v = press[LEAD + k, row - 1 : row - 1 + SUB, :]
        v = v + press[LEAD + k, row + 1 : row + 1 + SUB, :]
        v = v + press[LEAD + k - 1, row : row + SUB, :] + press[LEAD + k + 1, row : row + SUB, :]
        q, p = place(k)
        here = press[LEAD + k, row : row + SUB, :]
        return v + z_shifts(here, here, edge[q, at : at + SUB, :], p, 1)

    def set_edges(row, at):
        for q in range(blocks):
            v = press[strips + q, row : row + SUB, :]
            edge[q, at : at + SUB, :] = edge_source(v, v, 1)

    starts = (OWN - 1, OWN + 1)
    base, count = span(1)
    news = []
    for n, row in enumerate(starts):
        set_edges(row, n * SUB)
        tiles_of = strip_sides(row)
        far = strip_shift(tiles_of, 1), strip_shift(tiles_of, -1)
        for q in range(blocks):
            v = press[strips + q, row - 1 : row - 1 + SUB, :]
            v = v + press[strips + q, row + 1 : row + 1 + SUB, :] + far[0][q] + far[1][q]
            v = v + pltpu.roll(tiles_of[q], LANES - 1, 1) + pltpu.roll(tiles_of[q], 1, 1)
            news.append((total + q, strips + q, row, v))
        for k in range(count):
            news.append((base + k, LEAD + base + k, row, beside(base + k, row, n * SUB)))
    for n, (t, w, row, near) in enumerate(news):
        v = fields[4, t, row : row + SUB, :] * (4.0 / 3.0) + near * (1.0 / 9.0)
        resid[0, n, :SUB, :] = jnp.where(inside(t, row), v, 0.0)
    for n, (t, w, row, near) in enumerate(news):
        press[w, row : row + SUB, :] = resid[0, n, :SUB, :]
    base, count = span(0)
    set_edges(OWN, 0)
    for k in range(count):
        v = press[LEAD + base + k, own, :] * (1.0 / 3.0) + fields[4, base + k, own, :]
        press_ref[k] = v + beside(base + k, OWN, 0) * (1.0 / 9.0)


def on_device(rhs_velocity, rhs_pressure, layer_ids, visc_table, stencil):
    planes, rows, depth = rhs_pressure.shape
    assert rows == SUB and depth == LANES and planes * STRIP == LANES
    x_count, y_count, z_count = (lax.axis_size(n) for n in ("gx", "gy", "gz"))
    entries = jnp.transpose(stencil, (1, 2, 0))

    tile = jax.ShapeDtypeStruct((FIELDS, SUB, LANES), jnp.float32)
    vmem = pl.BlockSpec(memory_space=pltpu.VMEM)
    smem = pl.BlockSpec(memory_space=pltpu.SMEM)
    bands = pl.pallas_call(
        band_kernel,
        out_shape=tuple(
            jax.ShapeDtypeStruct((9, r * SUB, 3 * DEPTH), jnp.float32) for r in (3, 2, 2, 2)
        ),
        in_specs=[smem],
        out_specs=(vmem,) * 4,
        compiler_params=pltpu.CompilerParams(vmem_limit_bytes=SMALL_VMEM),
        name="bands",
    )(pltpu.with_memory_space_constraint(entries, pltpu.HBM))
    main, z_first, z_second = pl.pallas_call(
        functools.partial(pack_kernel, planes),
        out_shape=(
            jax.ShapeDtypeStruct((FIELDS * (planes + 1), SUB, LANES), jnp.float32),
            tile,
            tile,
        ),
        in_specs=[pl.BlockSpec(memory_space=pltpu.HBM)] * 5,
        out_specs=(vmem, vmem, vmem),
        scratch_shapes=[
            pltpu.SMEM(visc_table.shape, visc_table.dtype),
            pltpu.SMEM(entries.shape, entries.dtype),
            pltpu.VMEM(rhs_velocity.shape, rhs_velocity.dtype),
            pltpu.VMEM(rhs_pressure.shape, rhs_pressure.dtype),
            pltpu.VMEM(layer_ids.shape, layer_ids.dtype),
            pltpu.SemaphoreType.DMA((5,)),
        ],
        compiler_params=pltpu.CompilerParams(vmem_limit_bytes=SMALL_VMEM),
        name="pack",
    )(
        *(
            pltpu.with_memory_space_constraint(v, pltpu.HBM)
            for v in (visc_table, entries, rhs_velocity, rhs_pressure, layer_ids)
        )
    )

    halo = matched(z_first, "gz", first_pairs(z_count))
    halo = halo + matched(z_second, "gz", second_pairs(z_count))
    inner = FIELDS * planes
    block = jnp.concatenate([main[:inner], main[inner:] + halo])

    paired = x_count == 2
    if paired:
        parts = [block, lax.ppermute(block, "gx", [(0, 1), (1, 0)])]
    else:
        hops = -(-REACH // planes)
        parts = []
        for hop in range(-hops, hops + 1):
            pairs = [(i, i - hop) for i in range(x_count) if 0 <= i - hop < x_count]
            parts.append(block if hop == 0 else matched(block, "gx", pairs))
    blocks = len(parts)
    frame = jnp.stack(parts)

    message = jax.ShapeDtypeStruct((blocks, packed_rows(planes), LANES), jnp.float32)
    y_first, y_second = pl.pallas_call(
        functools.partial(message_kernel, planes, blocks),
        out_shape=(message, message),
        in_specs=[vmem] * blocks,
        out_specs=(vmem, vmem),
        compiler_params=pltpu.CompilerParams(vmem_limit_bytes=SMALL_VMEM),
        name="message",
    )(*parts)
    y_first = matched(y_first, "gy", first_pairs(y_count))
    y_second = matched(y_second, "gy", second_pairs(y_count))

    total = planes * blocks
    tiles = total + blocks
    f32 = jnp.float32
    return pl.pallas_call(
        functools.partial(cycle_kernel, planes, blocks, paired),
        out_shape=(
            jax.ShapeDtypeStruct(rhs_velocity.shape, f32),
            jax.ShapeDtypeStruct(rhs_pressure.shape, f32),
        ),
        in_specs=[vmem] * 7,
        out_specs=(vmem, vmem),
        scratch_shapes=[
            pltpu.VMEM((FIELDS, tiles, ROWS, LANES), f32),
            pltpu.VMEM((3, tiles + 2 * LEAD, ROWS, LANES), f32),
            pltpu.VMEM((2, (total // 2 + 2 * LEAD) * 9 * SUB, 2 * LANES), f32),
            pltpu.VMEM((tiles + 2, 9 * ROWS, LANES), f32),
            pltpu.VMEM((blocks, 3 * ROWS, LANES), f32),
            pltpu.VMEM((3, tiles, ROWS, LANES), f32),
            pltpu.VMEM((3, 2 * tiles, 2 * SUB, LANES), f32),
            pltpu.VMEM((tiles + 2 * LEAD, ROWS, LANES), f32),
        ],
        compiler_params=pltpu.CompilerParams(vmem_limit_bytes=CYCLE_VMEM),
        name="cycle",
    )(frame, y_first, y_second, *bands)


def solution(mesh):
    placed = (P(None, "gx", "gy", "gz"), P("gx", "gy", "gz"), P("gx", "gy", "gz"), P(), P())
    return jax.shard_map(
        on_device,
        mesh=mesh,
        in_specs=placed,
        out_specs=(P(None, "gx", "gy", "gz"), P("gx", "gy", "gz")),
        check_vma=False,
    )
```

```python
import functools

import jax
import jax.numpy as jnp
from jax import lax
from jax.experimental import pallas as pl
from jax.experimental.pallas import tpu as pltpu
from jax.sharding import PartitionSpec as P

LOW_BOUND = 0.2
HIGH_BOUND = 1.8

SUB = 8
LANES = 128
COLS = 8
REACH = 6
PRESS_REACH = 2
FIELDS = 5
LEAD = 2
STRIP = 4 * COLS
ROWS = 3 * SUB
OWN = SUB
ROWS_RESID = OWN - 4
ROWS_START = OWN - 2
ROWS_MIDDLE = OWN - 1
DEPTH = 2 * LANES
PIECE = 9 * SUB * 3
SMALL_VMEM = 4 * 1024 * 1024
CYCLE_VMEM = 32 * 1024 * 1024


def cheb_consts():
    theta = (HIGH_BOUND + LOW_BOUND) / 2.0
    delta = (HIGH_BOUND - LOW_BOUND) / 2.0
    sigma = theta / delta
    rho_zero = 1.0 / sigma
    rho_one = 1.0 / (2.0 * sigma - rho_zero)
    return (theta, delta, rho_zero, rho_one)


def first_pairs(count):
    return [(i, i ^ 1) for i in range(count) if i ^ 1 < count]


def second_pairs(x_count, count):
    pairs = []
    for x in range(x_count):
        for i in range(1, count - 1, 2):
            here = x * count + i
            pairs += [(here, here + 1), (here + 1, here)]
    if pairs and wraps(x_count, count):
        for x in range(x_count):
            for i in (0, count - 1):
                pairs.append((x * count + i, (x ^ 1) * count + i))
    return pairs


def wraps(x_count, count):
    return x_count % 2 == 0 and count % 2 == 0


def matched(block, axis, pairs):
    if not pairs:
        return jnp.zeros_like(block)
    return lax.ppermute(block, axis, pairs)


def lane_iota():
    return lax.broadcasted_iota(jnp.int32, (SUB, LANES), 1)


def diagonal_mean(stencil_ref):
    middle = stencil_ref.shape[2] // 2
    return (stencil_ref[0, 0, middle] + stencil_ref[1, 1, middle] + stencil_ref[2, 2, middle]) / 3.0


def band_kernel(stencil_ref, smooth_ref, resid_ref, coarse_ref, middle_ref):
    scale = 1.0 / jnp.full((SUB, LANES), diagonal_mean(stencil_ref), jnp.float32)
    sub = lax.broadcasted_iota(jnp.int32, (SUB, LANES), 0)
    lane = lane_iota()
    zero = jnp.zeros((SUB, LANES), jnp.float32)
    halves = []
    for half in range(DEPTH // LANES):
        spot = lane + half * LANES
        groups = range(half * LANES // ROWS, min(((half + 1) * LANES - 1) // ROWS, 8) + 1)
        start = jnp.full((SUB, LANES), groups[0] * ROWS, jnp.int32)
        for n in groups[1:]:
            start = jnp.where(spot >= n * ROWS, n * ROWS, start)
        reach = jnp.where(spot < 9 * ROWS, spot - start - sub, 1000)
        halves.append((reach, [(n, start == n * ROWS) for n in groups]))
    for c in range(3):
        for i in range(3):
            rows_of = []
            for b in range(3):
                row = []
                for reach, groups in halves:
                    full = zero
                    for n, here in groups:
                        a, j = divmod(n, 3)
                        full = jnp.where(here, stencil_ref[i, j, 9 * a + 3 * b + c], full)
                    full = scale * full
                    high = full.astype(jnp.bfloat16).astype(jnp.float32)
                    row.append((high, full - high))
                rows_of.append(row)
            for ref, start, step in (
                (smooth_ref, 0, 1),
                (resid_ref, ROWS_RESID, 1),
                (coarse_ref, ROWS_START, 2),
                (middle_ref, ROWS_MIDDLE, 1),
            ):
                for r in range(ref.shape[1] // SUB):
                    for half, (reach, _) in enumerate(halves):
                        high, low = zero, zero
                        for b in range(3):
                            here = reach == r * SUB + start + step * (b - 1)
                            high = jnp.where(here, rows_of[b][half][0], high)
                            low = jnp.where(here, rows_of[b][half][1], low)
                        for term, value in enumerate((high, low, high)):
                            at = (2 * term + half) * LANES
                            ref[c * 3 + i, r * SUB : (r + 1) * SUB, at : at + LANES] = value


def pack_kernel(
    planes,
    visc_hbm,
    stencil_hbm,
    rhs_hbm,
    press_hbm,
    ids_hbm,
    main_ref,
    a_ref,
    b_ref,
    visc_ref,
    stencil_ref,
    rhs_ref,
    press_ref,
    ids_ref,
    arrived,
):
    copies = [
        pltpu.make_async_copy(src, dst, arrived.at[n])
        for n, (src, dst) in enumerate(
            (
                (visc_hbm, visc_ref),
                (stencil_hbm, stencil_ref),
                (ids_hbm, ids_ref),
                (rhs_hbm, rhs_ref),
                (press_hbm, press_ref),
            )
        )
    ]
    for copy in copies:
        copy.start()
    for copy in copies:
        copy.wait()
    lane = lane_iota()
    count, at = lax.axis_size("gz"), lax.axis_index("gz")
    odd = at % 2 == 1
    at_end = (at == 0) | (at == count - 1)
    kc = jnp.full((SUB, LANES), diagonal_mean(stencil_ref), jnp.float32)
    zero = jnp.zeros((SUB, LANES), jnp.float32)
    up, down, own = [zero] * FIELDS, [zero] * FIELDS, [zero] * FIELDS
    for p in range(planes):
        ids = ids_ref[p]
        eta = jnp.zeros((SUB, LANES), jnp.float32)
        for layer in range(visc_ref.shape[0]):
            eta = jnp.where(ids == layer, visc_ref[layer], eta)
        dinv = 1.0 / (eta * kc)
        values = [rhs_ref[j, p] * dinv for j in range(3)]
        values += [eta, eta * press_ref[p] * (1.0 / 9.0)]
        quarter = lane // COLS - p * (STRIP // COLS)
        for f in range(FIELDS):
            main_ref[f * planes + p] = values[f]
            near = pltpu.roll(values[f], (p * STRIP + COLS) % LANES, 1)
            far = pltpu.roll(values[f], (p * STRIP + 3 * COLS) % LANES, 1)
            up[f] = jnp.where(quarter == 0, near, up[f])
            own[f] = jnp.where(quarter == 1, near, jnp.where(quarter == 2, far, own[f]))
            down[f] = jnp.where(quarter == 3, far, down[f])
    for f in range(FIELDS):
        main_ref[FIELDS * planes + f] = own[f]
        a_ref[f] = jnp.where(odd, down[f], up[f])
        outer = jnp.where(odd, up[f], down[f])
        b_ref[f] = jnp.where(at_end, 0.0, outer) if wraps(lax.axis_size("gx"), count) else outer


def packed_row(planes, f, p):
    if f < FIELDS - 1:
        return (f * (planes + 1) + p) * REACH
    return (FIELDS - 1) * (planes + 1) * REACH + p * PRESS_REACH


def packed_rows(planes):
    return -(-packed_row(planes, FIELDS - 1, planes + 1) // SUB) * SUB


def message_kernel(planes, blocks, *refs):
    parts, (a_ref, b_ref) = refs[:blocks], refs[blocks:]
    odd = lax.axis_index("gy") % 2 == 1
    rows = packed_rows(planes)

    def pack(to_low, to_high):
        for q in range(blocks):
            for ref in (to_low, to_high):
                ref[q, rows - SUB :, :] = jnp.zeros((SUB, LANES), jnp.float32)
            for f in range(FIELDS):
                count = REACH if f < FIELDS - 1 else PRESS_REACH
                for p in range(planes + 1):
                    index = FIELDS * planes + f if p == planes else f * planes + p
                    at = packed_row(planes, f, p)
                    to_low[q, at : at + count, :] = parts[q][index, :count, :]
                    to_high[q, at : at + count, :] = parts[q][index, SUB - count :, :]

    @pl.when(odd)
    def _():
        pack(a_ref, b_ref)

    @pl.when(jnp.logical_not(odd))
    def _():
        pack(b_ref, a_ref)

    if wraps(lax.axis_size("gx"), lax.axis_size("gy")):
        at = lax.axis_index("gy")

        @pl.when((at == 0) | (at == lax.axis_size("gy") - 1))
        def _():
            b_ref[...] = jnp.zeros_like(b_ref)


def cycle_kernel(
    planes,
    blocks,
    paired,
    own_ref,
    a_ref,
    b_ref,
    smooth_ref,
    resid_band,
    coarse_ref,
    middle_ref,
    vel_ref,
    press_ref,
    fields,
    work,
    split,
    products,
    edge,
    second_x,
    resid,
    press,
):
    _, delta, rho_zero, rho_one = cheb_consts()
    weight = 2.0 * rho_one / delta
    carry = rho_one * rho_zero
    total = planes * blocks
    strips = total + 2 * LEAD
    lane = lane_iota()
    zero = jnp.zeros((SUB, LANES), jnp.float32)
    gx = lax.axis_index("gx")
    y_odd = lax.axis_index("gy") % 2 == 1

    def span(grow):
        if paired:
            low = (0, min(planes - 1 + grow, total - 1))
            high = max(planes - grow, 0)
            return gx * high, low[1] + 1
        own = blocks // 2
        lo = max(own * planes - grow, 0)
        return lo, min((own + 1) * planes + grow, total) - lo

    def place(plane):
        if isinstance(plane, int):
            return plane // planes, plane % planes
        block = lax.div(plane, planes)
        return block, plane - block * planes

    def slot(q):
        return (q + gx) % 2 if paired else q

    for k in [*range(LEAD), *range(LEAD + total, strips)]:
        for r in range(3):
            for j in range(3):
                work[j, k, r * SUB : (r + 1) * SUB, :] = zero
            press[k, r * SUB : (r + 1) * SUB, :] = zero

    def assemble(row, tile_of):
        at = slice(row, row + SUB)
        for q in range(blocks):
            here = slot(q)
            for f in range(FIELDS):
                for p in range(planes + 1):
                    strip = p == planes
                    value = tile_of(here, f, p)
                    fields[f, total + q if strip else q * planes + p, at, :] = value
                    spot = strips + q if strip else LEAD + q * planes + p
                    if f < 3:
                        work[f, spot, at, :] = value
                    if f == 4:
                        press[spot, at, :] = value

    def own_tile(q, f, p):
        return own_ref[q, FIELDS * planes + f if p == planes else f * planes + p]

    def low_tile(ref):
        def tile(q, f, p):
            count = REACH if f < FIELDS - 1 else PRESS_REACH
            at = packed_row(planes, f, p) + count - SUB
            if at < 0:
                return pltpu.roll(ref[q, :SUB, :], -at, 0)
            return ref[q, at : at + SUB, :]

        return tile

    def high_tile(ref):
        def tile(q, f, p):
            at = packed_row(planes, f, p)
            over = max(at + SUB - ref.shape[1], 0)
            v = ref[q, at - over : at - over + SUB, :]
            return pltpu.roll(v, SUB - over, 0) if over else v

        return tile

    assemble(OWN, own_tile)

    @pl.when(y_odd)
    def _():
        assemble(OWN - SUB, low_tile(a_ref))
        assemble(OWN + SUB, high_tile(b_ref))

    @pl.when(jnp.logical_not(y_odd))
    def _():
        assemble(OWN - SUB, low_tile(b_ref))
        assemble(OWN + SUB, high_tile(a_ref))

    def strip_shift(tiles_of, offset):
        turn = (LANES - offset * STRIP) % LANES
        turned = [pltpu.roll(v, turn, 1) for v in tiles_of] + [zero]
        shifted = []
        for q in range(blocks):
            if offset > 0:
                shifted.append(jnp.where(lane < LANES - offset * STRIP, turned[q], turned[q + 1]))
            else:
                shifted.append(jnp.where(lane >= -offset * STRIP, turned[q], turned[q - 1]))
        return shifted

    def edge_source(ahead, behind, scale):
        moved = pltpu.roll(behind, 2 * COLS + 2 * scale, 1)
        far = lane % STRIP
        return jnp.where((far >= 3 * COLS + scale) & (far < 3 * COLS + 2 * scale), moved, ahead)

    def edge_turn(p, scale):
        return LANES - 3 * COLS - scale - STRIP * p

    def z_shifts(ahead, behind, source, p, scale):
        outer = pltpu.roll(source, edge_turn(p, scale), 1)
        ahead = pltpu.roll(ahead, LANES - scale, 1)
        behind = pltpu.roll(behind, scale, 1)
        return jnp.where(lane >= LANES - scale, outer, ahead) + jnp.where(
            lane < scale, outer, behind
        )

    def parts_of(v):
        high = v.astype(jnp.bfloat16).astype(jnp.float32)
        return high, v - high

    blank = jnp.zeros((DEPTH - PIECE, 2 * LANES), jnp.float32)

    def product(band_of, high, low):
        width = high.shape[1]
        return jnp.dot(
            band_of(),
            jnp.concatenate(
                [high, blank[:, :width], high, blank[:, :width], low, blank[:, :width]]
            ),
            preferred_element_type=jnp.float32,
            precision=lax.Precision.DEFAULT,
        )

    def apply(base, count, band_ref, first, rows, scale, emit, with_strips=True):
        height = rows * SUB
        half = -(-count // 2)

        def band_of():
            return band_ref[:, first : first + height, :].reshape(9 * height, 3 * DEPTH)

        for n in range(half + 2 * scale):
            for side in range(2):
                for j in range(3):
                    for r in range(3):
                        spot = LEAD + base - scale + side * half + n
                        high, low = parts_of(work[j, spot, r * SUB : (r + 1) * SUB, :])
                        at = ((n * 3 + j) * 3 + r) * SUB
                        lanes = slice(side * LANES, (side + 1) * LANES)
                        split[0, at : at + SUB, lanes] = high
                        split[1, at : at + SUB, lanes] = low
        size = 9 * SUB
        for q in range(0, blocks, 2):
            width = min(2, blocks - q)
            pieces = []
            for a in range(3):
                for j in range(3):
                    for r in range(3):
                        tiles_of = [
                            work[j, strips + p, r * SUB : (r + 1) * SUB, :] for p in range(blocks)
                        ]
                        if a != 1:
                            tiles_of = strip_shift(tiles_of, (a - 1) * scale)
                        pieces.append([parts_of(v) for v in tiles_of[q : q + width]])
            high, low = (
                jnp.concatenate(
                    [jnp.concatenate([v[n] for v in piece], axis=1) for piece in pieces]
                )
                for n in range(2)
            )
            made = product(band_of, high, low)
            for w in range(width):
                products[total + 2 + q + w, : 9 * height, :] = made[:, w * LANES : (w + 1) * LANES]

        def of(k, c, i, r):
            at = (c * 3 + i) * height + r * SUB
            return products[k, at : at + SUB, :]

        for i in range(3):
            for r in range(rows):
                for q in range(blocks):
                    behind, middle, ahead = (of(total + 2 + q, c, i, r) for c in range(3))
                    at = (i * 3 + r) * SUB
                    edge[q, at : at + SUB, :] = edge_source(ahead, behind, scale)
                    if with_strips:
                        middle = middle + pltpu.roll(ahead, LANES - scale, 1)
                        middle = middle + pltpu.roll(behind, scale, 1)
                        emit(total + q, strips + q, None, r, i, middle)

        def finish(k):
            q, p = place(base + k)
            for i in range(3):
                for r in range(rows):
                    behind, middle, ahead = (of(k, c, i, r) for c in range(3))
                    at = (i * 3 + r) * SUB
                    sides = z_shifts(ahead, behind, edge[q, at : at + SUB, :], p, scale)
                    emit(base + k, LEAD + base + k, k, r, i, middle + sides)

        for n in range(half + 1):
            if n < half:
                high, low = (
                    jnp.concatenate(
                        [
                            split[part, (n + a * scale) * size : (n + a * scale + 1) * size, :]
                            for a in range(3)
                        ]
                    )
                    for part in range(2)
                )
                made = product(band_of, high, low)
                for side in range(2):
                    products[n + side * half, : 9 * height, :] = made[
                        :, side * LANES : (side + 1) * LANES
                    ]
            for side in range(2):
                if n and n - 1 + side * half < count:
                    finish(n - 1 + side * half)

    def inside(t, row):
        return fields[3, t, row : row + SUB, :] > 0.0

    def emit_first(t, w, k, r, i, total_of):
        at = slice(r * SUB, (r + 1) * SUB)
        value = (1.0 + carry + weight) * fields[i, t, at, :] - weight * total_of
        value = jnp.where(inside(t, r * SUB), value, 0.0)
        work[i, w, at, :] = value
        second_x[i, t, at, :] = value

    apply(0, total, smooth_ref, 0, 3, 1, emit_first)

    lane_even = lane % 2 == 0
    row_even = lax.broadcasted_iota(jnp.int32, (SUB, LANES), 0) % 2 == 0

    def pair_sums(v):
        v = v + jnp.where(row_even, pltpu.roll(v, SUB - 1, 0), pltpu.roll(v, 1, 0))
        return v + jnp.where(lane_even, pltpu.roll(v, LANES - 1, 1), pltpu.roll(v, 1, 1))

    def emit_resid(t, w, k, r, i, total_of):
        at = slice(ROWS_RESID + r * SUB, ROWS_RESID + (r + 1) * SUB)
        value = fields[3, t, at, :] * (fields[i, t, at, :] - total_of)
        resid[i, t, r * SUB : (r + 1) * SUB, :] = pair_sums(value)

    apply(0, total, resid_band, 0, 2, 1, emit_resid)

    plane_even = lane // STRIP % 2 == 0
    for r in range(2):
        at = slice(ROWS_RESID + r * SUB, ROWS_RESID + (r + 1) * SUB)
        rows_at = slice(r * SUB, (r + 1) * SUB)
        for t in [*range(0, total, 2), *range(total, total + blocks)]:
            weigh = None
            for f in (3, 0, 1, 2):
                def load(k):
                    if f == 3:
                        return pair_sums(fields[3, k, at, :])
                    return resid[f, k, rows_at, :]

                v = load(t)
                if t < total:
                    v = v + load(t + 1)
                else:
                    ahead = pltpu.roll(v, LANES - STRIP, 1)
                    v = v + jnp.where(plane_even, ahead, pltpu.roll(v, STRIP, 1))
                if f == 3:
                    weigh = jnp.where(v > 0.0, 4.0 / v, 0.0)
                elif t < total:
                    work[f, LEAD + t, at, :] = v * weigh
                    work[f, LEAD + t + 1, at, :] = v * weigh
                else:
                    work[f, strips + t - total, at, :] = v * weigh

    def emit_start(t, w, k, r, i, total_of):
        at = slice(ROWS_START + r * SUB, ROWS_START + (r + 1) * SUB)
        value = second_x[i, t, at, :] + (1.0 + carry + weight) * work[i, w, at, :]
        value = jnp.where(inside(t, ROWS_START + r * SUB), value - weight * total_of, 0.0)
        work[i, w, at, :] = value

    apply(*span(2), coarse_ref, 0, 2, 2, emit_start)

    def emit_middle(t, w, k, r, i, total_of):
        at = slice(ROWS_MIDDLE + r * SUB, ROWS_MIDDLE + (r + 1) * SUB)
        step = jnp.where(inside(t, ROWS_MIDDLE + r * SUB), fields[i, t, at, :] - total_of, 0.0)
        work[i, w, at, :] = work[i, w, at, :] + step
        second_x[i, t, at, :] = step

    apply(*span(1), middle_ref, 0, 2, 1, emit_middle)

    own = slice(OWN, OWN + SUB)

    def emit_last(t, w, k, r, i, total_of):
        value = work[i, w, own, :] + carry * second_x[i, t, own, :]
        vel_ref[i, k] = value + weight * (fields[i, t, own, :] - total_of)

    apply(*span(0), smooth_ref, OWN, 1, 1, emit_last, with_strips=False)

    def strip_sides(row):
        return [press[strips + q, row : row + SUB, :] for q in range(blocks)]

    def beside(k, row, at):
        v = press[LEAD + k, row - 1 : row - 1 + SUB, :]
        v = v + press[LEAD + k, row + 1 : row + 1 + SUB, :]
        v = v + press[LEAD + k - 1, row : row + SUB, :] + press[LEAD + k + 1, row : row + SUB, :]
        q, p = place(k)
        here = press[LEAD + k, row : row + SUB, :]
        return v + z_shifts(here, here, edge[q, at : at + SUB, :], p, 1)

    def set_edges(row, at):
        for q in range(blocks):
            v = press[strips + q, row : row + SUB, :]
            edge[q, at : at + SUB, :] = edge_source(v, v, 1)

    starts = (OWN - 1, OWN + 1)
    base, count = span(1)
    news = []
    for n, row in enumerate(starts):
        set_edges(row, n * SUB)
        tiles_of = strip_sides(row)
        far = strip_shift(tiles_of, 1), strip_shift(tiles_of, -1)
        for q in range(blocks):
            v = press[strips + q, row - 1 : row - 1 + SUB, :]
            v = v + press[strips + q, row + 1 : row + 1 + SUB, :] + far[0][q] + far[1][q]
            v = v + pltpu.roll(tiles_of[q], LANES - 1, 1) + pltpu.roll(tiles_of[q], 1, 1)
            news.append((total + q, strips + q, row, v))
        for k in range(count):
            news.append((base + k, LEAD + base + k, row, beside(base + k, row, n * SUB)))
    for n, (t, w, row, near) in enumerate(news):
        v = fields[4, t, row : row + SUB, :] * (4.0 / 3.0) + near * (1.0 / 9.0)
        resid[0, n, :SUB, :] = jnp.where(inside(t, row), v, 0.0)
    for n, (t, w, row, near) in enumerate(news):
        press[w, row : row + SUB, :] = resid[0, n, :SUB, :]
    base, count = span(0)
    set_edges(OWN, 0)
    for k in range(count):
        v = press[LEAD + base + k, own, :] * (1.0 / 3.0) + fields[4, base + k, own, :]
        press_ref[k] = v + beside(base + k, OWN, 0) * (1.0 / 9.0)


def on_device(rhs_velocity, rhs_pressure, layer_ids, visc_table, stencil):
    planes, rows, depth = rhs_pressure.shape
    assert rows == SUB and depth == LANES and planes * STRIP == LANES
    x_count, y_count, z_count = (lax.axis_size(n) for n in ("gx", "gy", "gz"))
    entries = jnp.transpose(stencil, (1, 2, 0))

    tile = jax.ShapeDtypeStruct((FIELDS, SUB, LANES), jnp.float32)
    vmem = pl.BlockSpec(memory_space=pltpu.VMEM)
    smem = pl.BlockSpec(memory_space=pltpu.SMEM)
    bands = pl.pallas_call(
        band_kernel,
        out_shape=tuple(
            jax.ShapeDtypeStruct((9, r * SUB, 3 * DEPTH), jnp.float32) for r in (3, 2, 2, 2)
        ),
        in_specs=[smem],
        out_specs=(vmem,) * 4,
        compiler_params=pltpu.CompilerParams(vmem_limit_bytes=SMALL_VMEM),
        name="bands",
    )(pltpu.with_memory_space_constraint(entries, pltpu.HBM))
    main, z_first, z_second = pl.pallas_call(
        functools.partial(pack_kernel, planes),
        out_shape=(
            jax.ShapeDtypeStruct((FIELDS * (planes + 1), SUB, LANES), jnp.float32),
            tile,
            tile,
        ),
        in_specs=[pl.BlockSpec(memory_space=pltpu.HBM)] * 5,
        out_specs=(vmem, vmem, vmem),
        scratch_shapes=[
            pltpu.SMEM(visc_table.shape, visc_table.dtype),
            pltpu.SMEM(entries.shape, entries.dtype),
            pltpu.VMEM(rhs_velocity.shape, rhs_velocity.dtype),
            pltpu.VMEM(rhs_pressure.shape, rhs_pressure.dtype),
            pltpu.VMEM(layer_ids.shape, layer_ids.dtype),
            pltpu.SemaphoreType.DMA((5,)),
        ],
        compiler_params=pltpu.CompilerParams(vmem_limit_bytes=SMALL_VMEM),
        name="pack",
    )(
        *(
            pltpu.with_memory_space_constraint(v, pltpu.HBM)
            for v in (visc_table, entries, rhs_velocity, rhs_pressure, layer_ids)
        )
    )

    halo = matched(z_first, "gz", first_pairs(z_count))
    halo = halo + matched(z_second, ("gx", "gz"), second_pairs(x_count, z_count))
    inner = FIELDS * planes
    block = jnp.concatenate([main[:inner], main[inner:] + halo])

    paired = x_count == 2
    if paired:
        parts = [block, lax.ppermute(block, "gx", [(0, 1), (1, 0)])]
    else:
        hops = -(-REACH // planes)
        parts = []
        for hop in range(-hops, hops + 1):
            pairs = [(i, i - hop) for i in range(x_count) if 0 <= i - hop < x_count]
            parts.append(block if hop == 0 else matched(block, "gx", pairs))
    blocks = len(parts)
    frame = jnp.stack(parts)

    message = jax.ShapeDtypeStruct((blocks, packed_rows(planes), LANES), jnp.float32)
    y_first, y_second = pl.pallas_call(
        functools.partial(message_kernel, planes, blocks),
        out_shape=(message, message),
        in_specs=[vmem] * blocks,
        out_specs=(vmem, vmem),
        compiler_params=pltpu.CompilerParams(vmem_limit_bytes=SMALL_VMEM),
        name="message",
    )(*parts)
    y_first = matched(y_first, "gy", first_pairs(y_count))
    y_second = matched(y_second, ("gx", "gy"), second_pairs(x_count, y_count))

    total = planes * blocks
    tiles = total + blocks
    f32 = jnp.float32
    return pl.pallas_call(
        functools.partial(cycle_kernel, planes, blocks, paired),
        out_shape=(
            jax.ShapeDtypeStruct(rhs_velocity.shape, f32),
            jax.ShapeDtypeStruct(rhs_pressure.shape, f32),
        ),
        in_specs=[vmem] * 7,
        out_specs=(vmem, vmem),
        scratch_shapes=[
            pltpu.VMEM((FIELDS, tiles, ROWS, LANES), f32),
            pltpu.VMEM((3, tiles + 2 * LEAD, ROWS, LANES), f32),
            pltpu.VMEM((2, (total // 2 + 2 * LEAD) * 9 * SUB, 2 * LANES), f32),
            pltpu.VMEM((tiles + 2, 9 * ROWS, LANES), f32),
            pltpu.VMEM((blocks, 3 * ROWS, LANES), f32),
            pltpu.VMEM((3, tiles, ROWS, LANES), f32),
            pltpu.VMEM((3, 2 * tiles, 2 * SUB, LANES), f32),
            pltpu.VMEM((tiles + 2 * LEAD, ROWS, LANES), f32),
        ],
        compiler_params=pltpu.CompilerParams(vmem_limit_bytes=CYCLE_VMEM),
        name="cycle",
    )(frame, y_first, y_second, *bands)


def solution(mesh):
    placed = (P(None, "gx", "gy", "gz"), P("gx", "gy", "gz"), P("gx", "gy", "gz"), P(), P())
    return jax.shard_map(
        on_device,
        mesh=mesh,
        in_specs=placed,
        out_specs=(P(None, "gx", "gy", "gz"), P("gx", "gy", "gz")),
        check_vma=False,
    )
```

```python
import functools

import jax
import jax.numpy as jnp
from jax import lax
from jax.experimental import pallas as pl
from jax.experimental.pallas import tpu as pltpu
from jax.sharding import PartitionSpec as P

LOW_BOUND = 0.2
HIGH_BOUND = 1.8

SUB = 8
LANES = 128
COLS = 8
REACH = 6
PRESS_REACH = 2
FIELDS = 5
LEAD = 2
STRIP = 4 * COLS
ROWS = 3 * SUB
OWN = SUB
ROWS_RESID = OWN - 4
ROWS_START = OWN - 2
ROWS_MIDDLE = OWN - 1
WINDOW = 2 * SUB
WINDOW_COARSE = ROWS_START - 2
WINDOW_MIDDLE = ROWS_MIDDLE - 1
WINDOW_LAST = OWN - 1
SMALL_VMEM = 4 * 1024 * 1024
CYCLE_VMEM = 32 * 1024 * 1024


def cheb_consts():
    theta = (HIGH_BOUND + LOW_BOUND) / 2.0
    delta = (HIGH_BOUND - LOW_BOUND) / 2.0
    sigma = theta / delta
    rho_zero = 1.0 / sigma
    rho_one = 1.0 / (2.0 * sigma - rho_zero)
    return (theta, delta, rho_zero, rho_one)


def first_pairs(count):
    return [(i, i ^ 1) for i in range(count) if i ^ 1 < count]


def second_pairs(x_count, count):
    pairs = []
    for x in range(x_count):
        for i in range(1, count - 1, 2):
            here = x * count + i
            pairs += [(here, here + 1), (here + 1, here)]
    if pairs and wraps(x_count, count):
        for x in range(x_count):
            for i in (0, count - 1):
                pairs.append((x * count + i, (x ^ 1) * count + i))
    return pairs


def wraps(x_count, count):
    return x_count % 2 == 0 and count % 2 == 0


def matched(block, axis, pairs):
    if not pairs:
        return jnp.zeros_like(block)
    return lax.ppermute(block, axis, pairs)


def lane_iota():
    return lax.broadcasted_iota(jnp.int32, (SUB, LANES), 1)


def diagonal_mean(stencil_ref):
    middle = stencil_ref.shape[2] // 2
    return (stencil_ref[0, 0, middle] + stencil_ref[1, 1, middle] + stencil_ref[2, 2, middle]) / 3.0


def band_kernel(stencil_ref, smooth_ref, resid_ref, coarse_ref, middle_ref):
    scale = 1.0 / jnp.full((SUB, LANES), diagonal_mean(stencil_ref), jnp.float32)
    sub = lax.broadcasted_iota(jnp.int32, (SUB, LANES), 0)
    lane = lane_iota()
    zero = jnp.zeros((SUB, LANES), jnp.float32)
    kinds = (
        (ROWS, ((smooth_ref, 0, 1), (resid_ref, ROWS_RESID, 1))),
        (WINDOW, ((coarse_ref, ROWS_START - WINDOW_COARSE, 2), (middle_ref, 1, 1))),
    )
    for depth, users in kinds:
        for half in range(-(-27 * depth // LANES)):
            spot = lane + half * LANES
            first = half * LANES // depth
            last = min(((half + 1) * LANES - 1) // depth, 26)
            start = jnp.full((SUB, LANES), first * depth, jnp.int32)
            for n in range(first + 1, last + 1):
                start = jnp.where(spot >= n * depth, n * depth, start)
            reach = spot - start - sub
            here = [(n, start == n * depth) for n in range(first, last + 1)]
            is_low = (start >= 9 * depth) & (start < 18 * depth)
            width = min(LANES, 27 * depth - half * LANES)
            lanes = slice(half * LANES, half * LANES + width)
            for c in range(3):
                for i in range(3):
                    rows_of = []
                    for b in range(3):
                        full = zero
                        for n, mask in here:
                            a, j = divmod(n % 9, 3)
                            entry = stencil_ref[i, j, 9 * a + 3 * b + c]
                            full = jnp.where(mask, entry, full)
                        full = scale * full
                        high = full.astype(jnp.bfloat16).astype(jnp.float32)
                        rows_of.append(jnp.where(is_low, full - high, high))
                    for ref, offset, step in users:
                        for r in range(ref.shape[1] // SUB):
                            value = zero
                            for b in range(3):
                                at = r * SUB + offset + step * (b - 1)
                                value = jnp.where(reach == at, rows_of[b], value)
                            ref[c * 3 + i, r * SUB : (r + 1) * SUB, lanes] = value[:, :width]


def pack_kernel(
    planes,
    visc_hbm,
    stencil_hbm,
    rhs_hbm,
    press_hbm,
    ids_hbm,
    main_ref,
    a_ref,
    b_ref,
    visc_ref,
    stencil_ref,
    rhs_ref,
    press_ref,
    ids_ref,
    arrived,
):
    copies = [
        pltpu.make_async_copy(src, dst, arrived.at[n])
        for n, (src, dst) in enumerate(
            (
                (visc_hbm, visc_ref),
                (stencil_hbm, stencil_ref),
                (ids_hbm, ids_ref),
                (rhs_hbm, rhs_ref),
                (press_hbm, press_ref),
            )
        )
    ]
    for copy in copies:
        copy.start()
    for copy in copies:
        copy.wait()
    lane = lane_iota()
    count, at = lax.axis_size("gz"), lax.axis_index("gz")
    odd = at % 2 == 1
    at_end = (at == 0) | (at == count - 1)
    kc = jnp.full((SUB, LANES), diagonal_mean(stencil_ref), jnp.float32)
    zero = jnp.zeros((SUB, LANES), jnp.float32)
    up, down, own = [zero] * FIELDS, [zero] * FIELDS, [zero] * FIELDS
    for p in range(planes):
        ids = ids_ref[p]
        eta = jnp.zeros((SUB, LANES), jnp.float32)
        for layer in range(visc_ref.shape[0]):
            eta = jnp.where(ids == layer, visc_ref[layer], eta)
        dinv = 1.0 / (eta * kc)
        values = [rhs_ref[j, p] * dinv for j in range(3)]
        values += [eta, eta * press_ref[p] * (1.0 / 9.0)]
        quarter = lane // COLS - p * (STRIP // COLS)
        for f in range(FIELDS):
            main_ref[f * planes + p] = values[f]
            near = pltpu.roll(values[f], (p * STRIP + COLS) % LANES, 1)
            far = pltpu.roll(values[f], (p * STRIP + 3 * COLS) % LANES, 1)
            up[f] = jnp.where(quarter == 0, near, up[f])
            own[f] = jnp.where(quarter == 1, near, jnp.where(quarter == 2, far, own[f]))
            down[f] = jnp.where(quarter == 3, far, down[f])
    for f in range(FIELDS):
        main_ref[FIELDS * planes + f] = own[f]
        a_ref[f] = jnp.where(odd, down[f], up[f])
        outer = jnp.where(odd, up[f], down[f])
        b_ref[f] = jnp.where(at_end, 0.0, outer) if wraps(lax.axis_size("gx"), count) else outer


def packed_row(planes, f, p):
    if f < FIELDS - 1:
        return (f * (planes + 1) + p) * REACH
    return (FIELDS - 1) * (planes + 1) * REACH + p * PRESS_REACH


def packed_rows(planes):
    return -(-packed_row(planes, FIELDS - 1, planes + 1) // SUB) * SUB


def message_kernel(planes, blocks, *refs):
    parts, (a_ref, b_ref) = refs[:blocks], refs[blocks:]
    odd = lax.axis_index("gy") % 2 == 1
    rows = packed_rows(planes)

    def pack(to_low, to_high):
        for q in range(blocks):
            for ref in (to_low, to_high):
                ref[q, rows - SUB :, :] = jnp.zeros((SUB, LANES), jnp.float32)
            for f in range(FIELDS):
                count = REACH if f < FIELDS - 1 else PRESS_REACH
                for p in range(planes + 1):
                    index = FIELDS * planes + f if p == planes else f * planes + p
                    at = packed_row(planes, f, p)
                    to_low[q, at : at + count, :] = parts[q][index, :count, :]
                    to_high[q, at : at + count, :] = parts[q][index, SUB - count :, :]

    @pl.when(odd)
    def _():
        pack(a_ref, b_ref)

    @pl.when(jnp.logical_not(odd))
    def _():
        pack(b_ref, a_ref)

    if wraps(lax.axis_size("gx"), lax.axis_size("gy")):
        at = lax.axis_index("gy")

        @pl.when((at == 0) | (at == lax.axis_size("gy") - 1))
        def _():
            b_ref[...] = jnp.zeros_like(b_ref)


def cycle_kernel(
    planes,
    blocks,
    paired,
    own_ref,
    a_ref,
    b_ref,
    smooth_ref,
    resid_band,
    coarse_ref,
    middle_ref,
    vel_ref,
    press_ref,
    fields,
    work,
    split,
    products,
    edge,
    second_x,
    resid,
    press,
):
    _, delta, rho_zero, rho_one = cheb_consts()
    weight = 2.0 * rho_one / delta
    carry = rho_one * rho_zero
    total = planes * blocks
    strips = total + 2 * LEAD
    lane = lane_iota()
    zero = jnp.zeros((SUB, LANES), jnp.float32)
    gx = lax.axis_index("gx")
    y_odd = lax.axis_index("gy") % 2 == 1

    def span(grow):
        if paired:
            low = (0, min(planes - 1 + grow, total - 1))
            high = max(planes - grow, 0)
            return gx * high, low[1] + 1
        own = blocks // 2
        lo = max(own * planes - grow, 0)
        return lo, min((own + 1) * planes + grow, total) - lo

    def place(plane):
        if isinstance(plane, int):
            return plane // planes, plane % planes
        block = lax.div(plane, planes)
        return block, plane - block * planes

    def slot(q):
        return (q + gx) % 2 if paired else q

    for k in [*range(LEAD), *range(LEAD + total, strips)]:
        for r in range(3):
            for j in range(3):
                work[j, k, r * SUB : (r + 1) * SUB, :] = zero
            press[k, r * SUB : (r + 1) * SUB, :] = zero

    def assemble(row, tile_of):
        at = slice(row, row + SUB)
        for q in range(blocks):
            here = slot(q)
            for f in range(FIELDS):
                for p in range(planes + 1):
                    strip = p == planes
                    value = tile_of(here, f, p)
                    fields[f, total + q if strip else q * planes + p, at, :] = value
                    spot = strips + q if strip else LEAD + q * planes + p
                    if f < 3:
                        work[f, spot, at, :] = value
                    if f == 4:
                        press[spot, at, :] = value

    def own_tile(q, f, p):
        return own_ref[q, FIELDS * planes + f if p == planes else f * planes + p]

    def low_tile(ref):
        def tile(q, f, p):
            count = REACH if f < FIELDS - 1 else PRESS_REACH
            at = packed_row(planes, f, p) + count - SUB
            if at < 0:
                return pltpu.roll(ref[q, :SUB, :], -at, 0)
            return ref[q, at : at + SUB, :]

        return tile

    def high_tile(ref):
        def tile(q, f, p):
            at = packed_row(planes, f, p)
            over = max(at + SUB - ref.shape[1], 0)
            v = ref[q, at - over : at - over + SUB, :]
            return pltpu.roll(v, SUB - over, 0) if over else v

        return tile

    assemble(OWN, own_tile)

    @pl.when(y_odd)
    def _():
        assemble(OWN - SUB, low_tile(a_ref))
        assemble(OWN + SUB, high_tile(b_ref))

    @pl.when(jnp.logical_not(y_odd))
    def _():
        assemble(OWN - SUB, low_tile(b_ref))
        assemble(OWN + SUB, high_tile(a_ref))

    def strip_shift(tiles_of, offset):
        turn = (LANES - offset * STRIP) % LANES
        turned = [pltpu.roll(v, turn, 1) for v in tiles_of] + [zero]
        shifted = []
        for q in range(blocks):
            if offset > 0:
                shifted.append(jnp.where(lane < LANES - offset * STRIP, turned[q], turned[q + 1]))
            else:
                shifted.append(jnp.where(lane >= -offset * STRIP, turned[q], turned[q - 1]))
        return shifted

    def edge_source(ahead, behind, scale):
        moved = pltpu.roll(behind, 2 * COLS + 2 * scale, 1)
        far = lane % STRIP
        return jnp.where((far >= 3 * COLS + scale) & (far < 3 * COLS + 2 * scale), moved, ahead)

    def edge_turn(p, scale):
        return LANES - 3 * COLS - scale - STRIP * p

    def z_shifts(ahead, behind, source, p, scale):
        outer = pltpu.roll(source, edge_turn(p, scale), 1)
        ahead = pltpu.roll(ahead, LANES - scale, 1)
        behind = pltpu.roll(behind, scale, 1)
        return jnp.where(lane >= LANES - scale, outer, ahead) + jnp.where(
            lane < scale, outer, behind
        )

    def parts_of(v):
        high = v.astype(jnp.bfloat16).astype(jnp.float32)
        return high, v - high

    def product(band_of, high, low):
        return jnp.dot(
            band_of(),
            jnp.concatenate([high, high, low]),
            preferred_element_type=jnp.float32,
            precision=lax.Precision.DEFAULT,
        )

    def apply(base, count, band_ref, window, rows, scale, emit, with_strips=True):
        height = rows * SUB
        half = -(-count // 2)
        depth = band_ref.shape[2] // 27
        inputs = [window + r * SUB for r in range(depth // SUB)]

        def band_of():
            return band_ref[:, :height, :].reshape(9 * height, 27 * depth)

        for n in range(half + 2 * scale):
            for side in range(2):
                for j in range(3):
                    for r, row in enumerate(inputs):
                        spot = LEAD + base - scale + side * half + n
                        high, low = parts_of(work[j, spot, row : row + SUB, :])
                        at = (n * 3 + j) * depth + r * SUB
                        lanes = slice(side * LANES, (side + 1) * LANES)
                        split[0, at : at + SUB, lanes] = high
                        split[1, at : at + SUB, lanes] = low
        size = 3 * depth
        for q in range(0, blocks, 2):
            width = min(2, blocks - q)
            pieces = []
            for a in range(3):
                for j in range(3):
                    for row in inputs:
                        tiles_of = [
                            work[j, strips + p, row : row + SUB, :] for p in range(blocks)
                        ]
                        if a != 1:
                            tiles_of = strip_shift(tiles_of, (a - 1) * scale)
                        pieces.append([parts_of(v) for v in tiles_of[q : q + width]])
            high, low = (
                jnp.concatenate(
                    [jnp.concatenate([v[n] for v in piece], axis=1) for piece in pieces]
                )
                for n in range(2)
            )
            made = product(band_of, high, low)
            for w in range(width):
                products[total + 2 + q + w, : 9 * height, :] = made[:, w * LANES : (w + 1) * LANES]

        def of(k, c, i, r):
            at = (c * 3 + i) * height + r * SUB
            return products[k, at : at + SUB, :]

        for i in range(3):
            for r in range(rows):
                for q in range(blocks):
                    behind, middle, ahead = (of(total + 2 + q, c, i, r) for c in range(3))
                    at = (i * 3 + r) * SUB
                    edge[q, at : at + SUB, :] = edge_source(ahead, behind, scale)
                    if with_strips:
                        middle = middle + pltpu.roll(ahead, LANES - scale, 1)
                        middle = middle + pltpu.roll(behind, scale, 1)
                        emit(total + q, strips + q, None, r, i, middle)

        def finish(k):
            q, p = place(base + k)
            for i in range(3):
                for r in range(rows):
                    behind, middle, ahead = (of(k, c, i, r) for c in range(3))
                    at = (i * 3 + r) * SUB
                    sides = z_shifts(ahead, behind, edge[q, at : at + SUB, :], p, scale)
                    emit(base + k, LEAD + base + k, k, r, i, middle + sides)

        for n in range(half + 1):
            if n < half:
                high, low = (
                    jnp.concatenate(
                        [
                            split[part, (n + a * scale) * size : (n + a * scale + 1) * size, :]
                            for a in range(3)
                        ]
                    )
                    for part in range(2)
                )
                made = product(band_of, high, low)
                for side in range(2):
                    products[n + side * half, : 9 * height, :] = made[
                        :, side * LANES : (side + 1) * LANES
                    ]
            for side in range(2):
                if n and n - 1 + side * half < count:
                    finish(n - 1 + side * half)

    def inside(t, row):
        return fields[3, t, row : row + SUB, :] > 0.0

    def emit_first(t, w, k, r, i, total_of):
        at = slice(r * SUB, (r + 1) * SUB)
        value = (1.0 + carry + weight) * fields[i, t, at, :] - weight * total_of
        value = jnp.where(inside(t, r * SUB), value, 0.0)
        work[i, w, at, :] = value
        second_x[i, t, at, :] = value

    apply(0, total, smooth_ref, 0, 3, 1, emit_first)

    lane_even = lane % 2 == 0
    row_even = lax.broadcasted_iota(jnp.int32, (SUB, LANES), 0) % 2 == 0

    def pair_sums(v):
        v = v + jnp.where(row_even, pltpu.roll(v, SUB - 1, 0), pltpu.roll(v, 1, 0))
        return v + jnp.where(lane_even, pltpu.roll(v, LANES - 1, 1), pltpu.roll(v, 1, 1))

    def emit_resid(t, w, k, r, i, total_of):
        at = slice(ROWS_RESID + r * SUB, ROWS_RESID + (r + 1) * SUB)
        value = fields[3, t, at, :] * (fields[i, t, at, :] - total_of)
        resid[i, t, r * SUB : (r + 1) * SUB, :] = pair_sums(value)

    apply(0, total, resid_band, 0, 2, 1, emit_resid)

    plane_even = lane // STRIP % 2 == 0
    for r in range(2):
        at = slice(ROWS_RESID + r * SUB, ROWS_RESID + (r + 1) * SUB)
        rows_at = slice(r * SUB, (r + 1) * SUB)
        for t in [*range(0, total, 2), *range(total, total + blocks)]:
            weigh = None
            for f in (3, 0, 1, 2):
                def load(k):
                    if f == 3:
                        return pair_sums(fields[3, k, at, :])
                    return resid[f, k, rows_at, :]

                v = load(t)
                if t < total:
                    v = v + load(t + 1)
                else:
                    ahead = pltpu.roll(v, LANES - STRIP, 1)
                    v = v + jnp.where(plane_even, ahead, pltpu.roll(v, STRIP, 1))
                if f == 3:
                    weigh = jnp.where(v > 0.0, 4.0 / v, 0.0)
                elif t < total:
                    work[f, LEAD + t, at, :] = v * weigh
                    work[f, LEAD + t + 1, at, :] = v * weigh
                else:
                    work[f, strips + t - total, at, :] = v * weigh

    def emit_start(t, w, k, r, i, total_of):
        at = slice(ROWS_START + r * SUB, ROWS_START + (r + 1) * SUB)
        value = second_x[i, t, at, :] + (1.0 + carry + weight) * work[i, w, at, :]
        value = jnp.where(inside(t, ROWS_START + r * SUB), value - weight * total_of, 0.0)
        work[i, w, at, :] = value

    apply(*span(2), coarse_ref, WINDOW_COARSE, 2, 2, emit_start)

    def emit_middle(t, w, k, r, i, total_of):
        at = slice(ROWS_MIDDLE + r * SUB, ROWS_MIDDLE + (r + 1) * SUB)
        step = jnp.where(inside(t, ROWS_MIDDLE + r * SUB), fields[i, t, at, :] - total_of, 0.0)
        work[i, w, at, :] = work[i, w, at, :] + step
        second_x[i, t, at, :] = step

    apply(*span(1), middle_ref, WINDOW_MIDDLE, 2, 1, emit_middle)

    own = slice(OWN, OWN + SUB)

    def strip_sides(row):
        return [press[strips + q, row : row + SUB, :] for q in range(blocks)]

    def beside(k, row, at):
        v = press[LEAD + k, row - 1 : row - 1 + SUB, :]
        v = v + press[LEAD + k, row + 1 : row + 1 + SUB, :]
        v = v + press[LEAD + k - 1, row : row + SUB, :] + press[LEAD + k + 1, row : row + SUB, :]
        q, p = place(k)
        here = press[LEAD + k, row : row + SUB, :]
        return v + z_shifts(here, here, edge[q, 9 * SUB + at : 10 * SUB + at, :], p, 1)

    def set_edges(row, at):
        for q in range(blocks):
            v = press[strips + q, row : row + SUB, :]
            edge[q, 9 * SUB + at : 10 * SUB + at, :] = edge_source(v, v, 1)

    starts = (OWN - 1, OWN + 1)
    base, count = span(1)
    news = []
    for n, row in enumerate(starts):
        set_edges(row, n * SUB)
        tiles_of = strip_sides(row)
        far = strip_shift(tiles_of, 1), strip_shift(tiles_of, -1)
        for q in range(blocks):
            v = press[strips + q, row - 1 : row - 1 + SUB, :]
            v = v + press[strips + q, row + 1 : row + 1 + SUB, :] + far[0][q] + far[1][q]
            v = v + pltpu.roll(tiles_of[q], LANES - 1, 1) + pltpu.roll(tiles_of[q], 1, 1)
            news.append((total + q, strips + q, row, v))
        for k in range(count):
            news.append((base + k, LEAD + base + k, row, beside(base + k, row, n * SUB)))
    for n, (t, w, row, near) in enumerate(news):
        v = fields[4, t, row : row + SUB, :] * (4.0 / 3.0) + near * (1.0 / 9.0)
        resid[0, n, :SUB, :] = jnp.where(inside(t, row), v, 0.0)
    for n, (t, w, row, near) in enumerate(news):
        press[w, row : row + SUB, :] = resid[0, n, :SUB, :]
    base, count = span(0)
    set_edges(OWN, 0)
    for k in range(count):
        v = press[LEAD + base + k, own, :] * (1.0 / 3.0) + fields[4, base + k, own, :]
        press_ref[k] = v + beside(base + k, OWN, 0) * (1.0 / 9.0)

    def emit_last(t, w, k, r, i, total_of):
        value = work[i, w, own, :] + carry * second_x[i, t, own, :]
        vel_ref[i, k] = value + weight * (fields[i, t, own, :] - total_of)

    apply(*span(0), middle_ref, WINDOW_LAST, 1, 1, emit_last, with_strips=False)


def on_device(rhs_velocity, rhs_pressure, layer_ids, visc_table, stencil):
    planes, rows, depth = rhs_pressure.shape
    assert rows == SUB and depth == LANES and planes * STRIP == LANES
    x_count, y_count, z_count = (lax.axis_size(n) for n in ("gx", "gy", "gz"))
    entries = jnp.transpose(stencil, (1, 2, 0))

    tile = jax.ShapeDtypeStruct((FIELDS, SUB, LANES), jnp.float32)
    vmem = pl.BlockSpec(memory_space=pltpu.VMEM)
    smem = pl.BlockSpec(memory_space=pltpu.SMEM)
    bands = pl.pallas_call(
        band_kernel,
        out_shape=tuple(
            jax.ShapeDtypeStruct((9, r * SUB, 27 * depth), jnp.float32)
            for r, depth in ((3, ROWS), (2, ROWS), (2, WINDOW), (2, WINDOW))
        ),
        in_specs=[smem],
        out_specs=(vmem,) * 4,
        compiler_params=pltpu.CompilerParams(vmem_limit_bytes=SMALL_VMEM),
        name="bands",
    )(pltpu.with_memory_space_constraint(entries, pltpu.HBM))
    main, z_first, z_second = pl.pallas_call(
        functools.partial(pack_kernel, planes),
        out_shape=(
            jax.ShapeDtypeStruct((FIELDS * (planes + 1), SUB, LANES), jnp.float32),
            tile,
            tile,
        ),
        in_specs=[pl.BlockSpec(memory_space=pltpu.HBM)] * 5,
        out_specs=(vmem, vmem, vmem),
        scratch_shapes=[
            pltpu.SMEM(visc_table.shape, visc_table.dtype),
            pltpu.SMEM(entries.shape, entries.dtype),
            pltpu.VMEM(rhs_velocity.shape, rhs_velocity.dtype),
            pltpu.VMEM(rhs_pressure.shape, rhs_pressure.dtype),
            pltpu.VMEM(layer_ids.shape, layer_ids.dtype),
            pltpu.SemaphoreType.DMA((5,)),
        ],
        compiler_params=pltpu.CompilerParams(vmem_limit_bytes=SMALL_VMEM),
        name="pack",
    )(
        *(
            pltpu.with_memory_space_constraint(v, pltpu.HBM)
            for v in (visc_table, entries, rhs_velocity, rhs_pressure, layer_ids)
        )
    )

    halo = matched(z_first, "gz", first_pairs(z_count))
    halo = halo + matched(z_second, ("gx", "gz"), second_pairs(x_count, z_count))
    inner = FIELDS * planes
    block = jnp.concatenate([main[:inner], main[inner:] + halo])

    paired = x_count == 2
    if paired:
        parts = [block, lax.ppermute(block, "gx", [(0, 1), (1, 0)])]
    else:
        hops = -(-REACH // planes)
        parts = []
        for hop in range(-hops, hops + 1):
            pairs = [(i, i - hop) for i in range(x_count) if 0 <= i - hop < x_count]
            parts.append(block if hop == 0 else matched(block, "gx", pairs))
    blocks = len(parts)
    frame = jnp.stack(parts)

    message = jax.ShapeDtypeStruct((blocks, packed_rows(planes), LANES), jnp.float32)
    y_first, y_second = pl.pallas_call(
        functools.partial(message_kernel, planes, blocks),
        out_shape=(message, message),
        in_specs=[vmem] * blocks,
        out_specs=(vmem, vmem),
        compiler_params=pltpu.CompilerParams(vmem_limit_bytes=SMALL_VMEM),
        name="message",
    )(*parts)
    y_first = matched(y_first, "gy", first_pairs(y_count))
    y_second = matched(y_second, ("gx", "gy"), second_pairs(x_count, y_count))

    total = planes * blocks
    tiles = total + blocks
    f32 = jnp.float32
    return pl.pallas_call(
        functools.partial(cycle_kernel, planes, blocks, paired),
        out_shape=(
            jax.ShapeDtypeStruct(rhs_velocity.shape, f32),
            jax.ShapeDtypeStruct(rhs_pressure.shape, f32),
        ),
        in_specs=[vmem] * 7,
        out_specs=(vmem, vmem),
        scratch_shapes=[
            pltpu.VMEM((FIELDS, tiles, ROWS, LANES), f32),
            pltpu.VMEM((3, tiles + 2 * LEAD, ROWS, LANES), f32),
            pltpu.VMEM((2, (total // 2 + 2 * LEAD) * 9 * SUB, 2 * LANES), f32),
            pltpu.VMEM((tiles + 2, 9 * ROWS, LANES), f32),
            pltpu.VMEM((blocks, 3 * ROWS + 2 * SUB, LANES), f32),
            pltpu.VMEM((3, tiles, ROWS, LANES), f32),
            pltpu.VMEM((3, 2 * tiles, 2 * SUB, LANES), f32),
            pltpu.VMEM((tiles + 2 * LEAD, ROWS, LANES), f32),
        ],
        compiler_params=pltpu.CompilerParams(vmem_limit_bytes=CYCLE_VMEM),
        name="cycle",
    )(frame, y_first, y_second, *bands)


def solution(mesh):
    placed = (P(None, "gx", "gy", "gz"), P("gx", "gy", "gz"), P("gx", "gy", "gz"), P(), P())
    return jax.shard_map(
        on_device,
        mesh=mesh,
        in_specs=placed,
        out_specs=(P(None, "gx", "gy", "gz"), P("gx", "gy", "gz")),
        check_vma=False,
    )
```

```python
import functools

import jax
import jax.numpy as jnp
from jax import lax
from jax.experimental import pallas as pl
from jax.experimental.pallas import tpu as pltpu
from jax.sharding import PartitionSpec as P

LOW_BOUND = 0.2
HIGH_BOUND = 1.8

SUB = 8
LANES = 128
COLS = 8
REACH = 6
REACHES = (6, 6, 6, 5, 2)
FIELDS = 5
LEAD = 2
STRIP = 4 * COLS
ROWS = 3 * SUB
OWN = SUB
ROWS_RESID = OWN - 4
ROWS_START = OWN - 2
ROWS_MIDDLE = OWN - 1
WINDOW = 2 * SUB
WINDOW_COARSE = ROWS_START - 2
WINDOW_MIDDLE = ROWS_MIDDLE - 1
WINDOW_LAST = OWN - 1
SMALL_VMEM = 4 * 1024 * 1024
CYCLE_VMEM = 32 * 1024 * 1024


def cheb_consts():
    theta = (HIGH_BOUND + LOW_BOUND) / 2.0
    delta = (HIGH_BOUND - LOW_BOUND) / 2.0
    sigma = theta / delta
    rho_zero = 1.0 / sigma
    rho_one = 1.0 / (2.0 * sigma - rho_zero)
    return (theta, delta, rho_zero, rho_one)


def first_pairs(count):
    return [(i, i ^ 1) for i in range(count) if i ^ 1 < count]


def second_pairs(x_count, count):
    pairs = []
    for x in range(x_count):
        for i in range(1, count - 1, 2):
            here = x * count + i
            pairs += [(here, here + 1), (here + 1, here)]
    if pairs and wraps(x_count, count):
        for x in range(x_count):
            for i in (0, count - 1):
                pairs.append((x * count + i, (x ^ 1) * count + i))
    return pairs


def wraps(x_count, count):
    return x_count % 2 == 0 and count % 2 == 0


def matched(block, axis, pairs):
    if not pairs:
        return jnp.zeros_like(block)
    return lax.ppermute(block, axis, pairs)


def lane_iota():
    return lax.broadcasted_iota(jnp.int32, (SUB, LANES), 1)


def diagonal_mean(stencil_ref):
    middle = stencil_ref.shape[2] // 2
    return (stencil_ref[0, 0, middle] + stencil_ref[1, 1, middle] + stencil_ref[2, 2, middle]) / 3.0


def band_kernel(stencil_ref, smooth_ref, resid_ref, coarse_ref, middle_ref):
    scale = 1.0 / jnp.full((SUB, LANES), diagonal_mean(stencil_ref), jnp.float32)
    sub = lax.broadcasted_iota(jnp.int32, (SUB, LANES), 0)
    lane = lane_iota()
    zero = jnp.zeros((SUB, LANES), jnp.float32)
    kinds = (
        (ROWS, ((smooth_ref, 0, 1), (resid_ref, ROWS_RESID, 1))),
        (WINDOW, ((coarse_ref, ROWS_START - WINDOW_COARSE, 2), (middle_ref, 1, 1))),
    )
    for depth, users in kinds:
        for half in range(-(-27 * depth // LANES)):
            spot = lane + half * LANES
            first = half * LANES // depth
            last = min(((half + 1) * LANES - 1) // depth, 26)
            start = jnp.full((SUB, LANES), first * depth, jnp.int32)
            for n in range(first + 1, last + 1):
                start = jnp.where(spot >= n * depth, n * depth, start)
            reach = spot - start - sub
            here = [(n, start == n * depth) for n in range(first, last + 1)]
            is_low = (start >= 9 * depth) & (start < 18 * depth)
            width = min(LANES, 27 * depth - half * LANES)
            lanes = slice(half * LANES, half * LANES + width)
            for c in range(3):
                for i in range(3):
                    rows_of = []
                    for b in range(3):
                        full = zero
                        for n, mask in here:
                            a, j = divmod(n % 9, 3)
                            entry = stencil_ref[i, j, 9 * a + 3 * b + c]
                            full = jnp.where(mask, entry, full)
                        full = scale * full
                        high = full.astype(jnp.bfloat16).astype(jnp.float32)
                        rows_of.append(jnp.where(is_low, full - high, high))
                    for ref, offset, step in users:
                        for r in range(ref.shape[1] // SUB):
                            value = zero
                            for b in range(3):
                                at = r * SUB + offset + step * (b - 1)
                                value = jnp.where(reach == at, rows_of[b], value)
                            ref[c * 3 + i, r * SUB : (r + 1) * SUB, lanes] = value[:, :width]


def pack_kernel(
    planes,
    visc_hbm,
    stencil_hbm,
    rhs_hbm,
    press_hbm,
    ids_hbm,
    main_ref,
    a_ref,
    b_ref,
    visc_ref,
    stencil_ref,
    rhs_ref,
    press_ref,
    ids_ref,
    arrived,
):
    copies = [
        pltpu.make_async_copy(src, dst, arrived.at[n])
        for n, (src, dst) in enumerate(
            (
                (visc_hbm, visc_ref),
                (stencil_hbm, stencil_ref),
                (ids_hbm, ids_ref),
                (rhs_hbm, rhs_ref),
                (press_hbm, press_ref),
            )
        )
    ]
    for copy in copies:
        copy.start()
    for copy in copies:
        copy.wait()
    lane = lane_iota()
    count, at = lax.axis_size("gz"), lax.axis_index("gz")
    odd = at % 2 == 1
    at_end = (at == 0) | (at == count - 1)
    kc = jnp.full((SUB, LANES), diagonal_mean(stencil_ref), jnp.float32)
    zero = jnp.zeros((SUB, LANES), jnp.float32)
    up, down, own = [zero] * FIELDS, [zero] * FIELDS, [zero] * FIELDS
    for p in range(planes):
        ids = ids_ref[p]
        eta = jnp.zeros((SUB, LANES), jnp.float32)
        for layer in range(visc_ref.shape[0]):
            eta = jnp.where(ids == layer, visc_ref[layer], eta)
        dinv = 1.0 / (eta * kc)
        values = [rhs_ref[j, p] * dinv for j in range(3)]
        values += [eta, eta * press_ref[p] * (1.0 / 9.0)]
        quarter = lane // COLS - p * (STRIP // COLS)
        for f in range(FIELDS):
            main_ref[f * planes + p] = values[f]
            near = pltpu.roll(values[f], (p * STRIP + COLS) % LANES, 1)
            far = pltpu.roll(values[f], (p * STRIP + 3 * COLS) % LANES, 1)
            up[f] = jnp.where(quarter == 0, near, up[f])
            own[f] = jnp.where(quarter == 1, near, jnp.where(quarter == 2, far, own[f]))
            down[f] = jnp.where(quarter == 3, far, down[f])
    for f in range(FIELDS):
        main_ref[FIELDS * planes + f] = own[f]
        a_ref[f] = jnp.where(odd, down[f], up[f])
        outer = jnp.where(odd, up[f], down[f])
        b_ref[f] = jnp.where(at_end, 0.0, outer) if wraps(lax.axis_size("gx"), count) else outer


def packed_row(planes, f, p):
    return sum(REACHES[:f]) * (planes + 1) + p * REACHES[f]


def packed_rows(planes):
    return -(-packed_row(planes, FIELDS - 1, planes + 1) // SUB) * SUB


def message_kernel(planes, blocks, *refs):
    parts, (a_ref, b_ref) = refs[:blocks], refs[blocks:]
    odd = lax.axis_index("gy") % 2 == 1
    rows = packed_rows(planes)

    def pack(to_low, to_high):
        for q in range(blocks):
            for ref in (to_low, to_high):
                ref[q, rows - SUB :, :] = jnp.zeros((SUB, LANES), jnp.float32)
            for f in range(FIELDS):
                count = REACHES[f]
                for p in range(planes + 1):
                    index = FIELDS * planes + f if p == planes else f * planes + p
                    at = packed_row(planes, f, p)
                    to_low[q, at : at + count, :] = parts[q][index, :count, :]
                    to_high[q, at : at + count, :] = parts[q][index, SUB - count :, :]

    @pl.when(odd)
    def _():
        pack(a_ref, b_ref)

    @pl.when(jnp.logical_not(odd))
    def _():
        pack(b_ref, a_ref)

    if wraps(lax.axis_size("gx"), lax.axis_size("gy")):
        at = lax.axis_index("gy")

        @pl.when((at == 0) | (at == lax.axis_size("gy") - 1))
        def _():
            b_ref[...] = jnp.zeros_like(b_ref)


def cycle_kernel(
    planes,
    blocks,
    paired,
    own_ref,
    a_ref,
    b_ref,
    smooth_ref,
    resid_band,
    coarse_ref,
    middle_ref,
    vel_ref,
    press_ref,
    fields,
    work,
    split,
    products,
    edge,
    second_x,
    resid,
    press,
):
    _, delta, rho_zero, rho_one = cheb_consts()
    weight = 2.0 * rho_one / delta
    carry = rho_one * rho_zero
    total = planes * blocks
    strips = total + 2 * LEAD
    lane = lane_iota()
    zero = jnp.zeros((SUB, LANES), jnp.float32)
    gx = lax.axis_index("gx")
    y_odd = lax.axis_index("gy") % 2 == 1

    def span(grow):
        if paired:
            low = (0, min(planes - 1 + grow, total - 1))
            high = max(planes - grow, 0)
            return gx * high, low[1] + 1
        own = blocks // 2
        lo = max(own * planes - grow, 0)
        return lo, min((own + 1) * planes + grow, total) - lo

    def place(plane):
        if isinstance(plane, int):
            return plane // planes, plane % planes
        block = lax.div(plane, planes)
        return block, plane - block * planes

    def slot(q):
        return (q + gx) % 2 if paired else q

    for k in [*range(LEAD), *range(LEAD + total, strips)]:
        for r in range(3):
            for j in range(3):
                work[j, k, r * SUB : (r + 1) * SUB, :] = zero
            press[k, r * SUB : (r + 1) * SUB, :] = zero

    def assemble(row, tile_of):
        at = slice(row, row + SUB)
        for q in range(blocks):
            here = slot(q)
            for f in range(FIELDS):
                for p in range(planes + 1):
                    strip = p == planes
                    value = tile_of(here, f, p)
                    fields[f, total + q if strip else q * planes + p, at, :] = value
                    spot = strips + q if strip else LEAD + q * planes + p
                    if f < 3:
                        work[f, spot, at, :] = value
                    if f == 4:
                        press[spot, at, :] = value

    def own_tile(q, f, p):
        return own_ref[q, FIELDS * planes + f if p == planes else f * planes + p]

    def low_tile(ref):
        def tile(q, f, p):
            at = packed_row(planes, f, p) + REACHES[f] - SUB
            if at < 0:
                return pltpu.roll(ref[q, :SUB, :], -at, 0)
            return ref[q, at : at + SUB, :]

        return tile

    def high_tile(ref):
        def tile(q, f, p):
            at = packed_row(planes, f, p)
            over = max(at + SUB - ref.shape[1], 0)
            v = ref[q, at - over : at - over + SUB, :]
            return pltpu.roll(v, SUB - over, 0) if over else v

        return tile

    assemble(OWN, own_tile)

    @pl.when(y_odd)
    def _():
        assemble(OWN - SUB, low_tile(a_ref))
        assemble(OWN + SUB, high_tile(b_ref))

    @pl.when(jnp.logical_not(y_odd))
    def _():
        assemble(OWN - SUB, low_tile(b_ref))
        assemble(OWN + SUB, high_tile(a_ref))

    def strip_shift(tiles_of, offset):
        turn = (LANES - offset * STRIP) % LANES
        turned = [pltpu.roll(v, turn, 1) for v in tiles_of] + [zero]
        shifted = []
        for q in range(blocks):
            if offset > 0:
                shifted.append(jnp.where(lane < LANES - offset * STRIP, turned[q], turned[q + 1]))
            else:
                shifted.append(jnp.where(lane >= -offset * STRIP, turned[q], turned[q - 1]))
        return shifted

    def edge_source(ahead, behind, scale):
        moved = pltpu.roll(behind, 2 * COLS + 2 * scale, 1)
        far = lane % STRIP
        return jnp.where((far >= 3 * COLS + scale) & (far < 3 * COLS + 2 * scale), moved, ahead)

    def edge_turn(p, scale):
        return LANES - 3 * COLS - scale - STRIP * p

    def z_shifts(ahead, behind, source, p, scale):
        outer = pltpu.roll(source, edge_turn(p, scale), 1)
        ahead = pltpu.roll(ahead, LANES - scale, 1)
        behind = pltpu.roll(behind, scale, 1)
        return jnp.where(lane >= LANES - scale, outer, ahead) + jnp.where(
            lane < scale, outer, behind
        )

    def parts_of(v):
        high = v.astype(jnp.bfloat16).astype(jnp.float32)
        return high, v - high

    def product(band_of, high, low):
        return jnp.dot(
            band_of(),
            jnp.concatenate([high, high, low]),
            preferred_element_type=jnp.float32,
            precision=lax.Precision.DEFAULT,
        )

    def apply(base, count, band_ref, window, rows, scale, emit, with_strips=True):
        height = rows * SUB
        half = -(-count // 2)
        depth = band_ref.shape[2] // 27
        inputs = [window + r * SUB for r in range(depth // SUB)]

        def band_of():
            return band_ref[:, :height, :].reshape(9 * height, 27 * depth)

        for n in range(half + 2 * scale):
            for side in range(2):
                for j in range(3):
                    for r, row in enumerate(inputs):
                        spot = LEAD + base - scale + side * half + n
                        high, low = parts_of(work[j, spot, row : row + SUB, :])
                        at = (n * 3 + j) * depth + r * SUB
                        lanes = slice(side * LANES, (side + 1) * LANES)
                        split[0, at : at + SUB, lanes] = high
                        split[1, at : at + SUB, lanes] = low
        size = 3 * depth
        for q in range(0, blocks, 2):
            width = min(2, blocks - q)
            pieces = []
            for a in range(3):
                for j in range(3):
                    for row in inputs:
                        tiles_of = [
                            work[j, strips + p, row : row + SUB, :] for p in range(blocks)
                        ]
                        if a != 1:
                            tiles_of = strip_shift(tiles_of, (a - 1) * scale)
                        pieces.append([parts_of(v) for v in tiles_of[q : q + width]])
            high, low = (
                jnp.concatenate(
                    [jnp.concatenate([v[n] for v in piece], axis=1) for piece in pieces]
                )
                for n in range(2)
            )
            made = product(band_of, high, low)
            for w in range(width):
                products[total + 2 + q + w, : 9 * height, :] = made[:, w * LANES : (w + 1) * LANES]

        def of(k, c, i, r):
            at = (c * 3 + i) * height + r * SUB
            return products[k, at : at + SUB, :]

        for i in range(3):
            for r in range(rows):
                for q in range(blocks):
                    behind, middle, ahead = (of(total + 2 + q, c, i, r) for c in range(3))
                    at = (i * 3 + r) * SUB
                    edge[q, at : at + SUB, :] = edge_source(ahead, behind, scale)
                    if with_strips:
                        middle = middle + pltpu.roll(ahead, LANES - scale, 1)
                        middle = middle + pltpu.roll(behind, scale, 1)
                        emit(total + q, strips + q, None, r, i, middle)

        def finish(k):
            q, p = place(base + k)
            for i in range(3):
                for r in range(rows):
                    behind, middle, ahead = (of(k, c, i, r) for c in range(3))
                    at = (i * 3 + r) * SUB
                    sides = z_shifts(ahead, behind, edge[q, at : at + SUB, :], p, scale)
                    emit(base + k, LEAD + base + k, k, r, i, middle + sides)

        for n in range(half + 1):
            if n < half:
                high, low = (
                    jnp.concatenate(
                        [
                            split[part, (n + a * scale) * size : (n + a * scale + 1) * size, :]
                            for a in range(3)
                        ]
                    )
                    for part in range(2)
                )
                made = product(band_of, high, low)
                for side in range(2):
                    products[n + side * half, : 9 * height, :] = made[
                        :, side * LANES : (side + 1) * LANES
                    ]
            for side in range(2):
                if n and n - 1 + side * half < count:
                    finish(n - 1 + side * half)

    def inside(t, row):
        return fields[3, t, row : row + SUB, :] > 0.0

    own = slice(OWN, OWN + SUB)

    def strip_sides(row):
        return [press[strips + q, row : row + SUB, :] for q in range(blocks)]

    def beside(k, row, at):
        v = press[LEAD + k, row - 1 : row - 1 + SUB, :]
        v = v + press[LEAD + k, row + 1 : row + 1 + SUB, :]
        v = v + press[LEAD + k - 1, row : row + SUB, :] + press[LEAD + k + 1, row : row + SUB, :]
        q, p = place(k)
        here = press[LEAD + k, row : row + SUB, :]
        return v + z_shifts(here, here, edge[q, 9 * SUB + at : 10 * SUB + at, :], p, 1)

    def set_edges(row, at):
        for q in range(blocks):
            v = press[strips + q, row : row + SUB, :]
            edge[q, 9 * SUB + at : 10 * SUB + at, :] = edge_source(v, v, 1)

    starts = (OWN - 1, OWN + 1)
    base, count = span(1)
    news = []
    for n, row in enumerate(starts):
        set_edges(row, n * SUB)
        tiles_of = strip_sides(row)
        far = strip_shift(tiles_of, 1), strip_shift(tiles_of, -1)
        for q in range(blocks):
            v = press[strips + q, row - 1 : row - 1 + SUB, :]
            v = v + press[strips + q, row + 1 : row + 1 + SUB, :] + far[0][q] + far[1][q]
            v = v + pltpu.roll(tiles_of[q], LANES - 1, 1) + pltpu.roll(tiles_of[q], 1, 1)
            news.append((total + q, strips + q, row, v))
        for k in range(count):
            news.append((base + k, LEAD + base + k, row, beside(base + k, row, n * SUB)))
    for n, (t, w, row, near) in enumerate(news):
        v = fields[4, t, row : row + SUB, :] * (4.0 / 3.0) + near * (1.0 / 9.0)
        resid[0, n, :SUB, :] = jnp.where(inside(t, row), v, 0.0)
    for n, (t, w, row, near) in enumerate(news):
        press[w, row : row + SUB, :] = resid[0, n, :SUB, :]
    base, count = span(0)
    set_edges(OWN, 0)
    for k in range(count):
        v = press[LEAD + base + k, own, :] * (1.0 / 3.0) + fields[4, base + k, own, :]
        press_ref[k] = v + beside(base + k, OWN, 0) * (1.0 / 9.0)

    def emit_first(t, w, k, r, i, total_of):
        at = slice(r * SUB, (r + 1) * SUB)
        value = (1.0 + carry + weight) * fields[i, t, at, :] - weight * total_of
        value = jnp.where(inside(t, r * SUB), value, 0.0)
        work[i, w, at, :] = value
        second_x[i, t, at, :] = value

    apply(0, total, smooth_ref, 0, 3, 1, emit_first)

    lane_even = lane % 2 == 0
    row_even = lax.broadcasted_iota(jnp.int32, (SUB, LANES), 0) % 2 == 0

    def pair_sums(v):
        v = v + jnp.where(row_even, pltpu.roll(v, SUB - 1, 0), pltpu.roll(v, 1, 0))
        return v + jnp.where(lane_even, pltpu.roll(v, LANES - 1, 1), pltpu.roll(v, 1, 1))

    def emit_resid(t, w, k, r, i, total_of):
        at = slice(ROWS_RESID + r * SUB, ROWS_RESID + (r + 1) * SUB)
        value = fields[3, t, at, :] * (fields[i, t, at, :] - total_of)
        resid[i, t, r * SUB : (r + 1) * SUB, :] = pair_sums(value)

    apply(0, total, resid_band, 0, 2, 1, emit_resid)

    plane_even = lane // STRIP % 2 == 0
    for r in range(2):
        at = slice(ROWS_RESID + r * SUB, ROWS_RESID + (r + 1) * SUB)
        rows_at = slice(r * SUB, (r + 1) * SUB)
        for t in [*range(0, total, 2), *range(total, total + blocks)]:
            weigh = None
            for f in (3, 0, 1, 2):
                def load(k):
                    if f == 3:
                        return pair_sums(fields[3, k, at, :])
                    return resid[f, k, rows_at, :]

                v = load(t)
                if t < total:
                    v = v + load(t + 1)
                else:
                    ahead = pltpu.roll(v, LANES - STRIP, 1)
                    v = v + jnp.where(plane_even, ahead, pltpu.roll(v, STRIP, 1))
                if f == 3:
                    weigh = jnp.where(v > 0.0, 4.0 / v, 0.0)
                elif t < total:
                    work[f, LEAD + t, at, :] = v * weigh
                    work[f, LEAD + t + 1, at, :] = v * weigh
                else:
                    work[f, strips + t - total, at, :] = v * weigh

    def emit_start(t, w, k, r, i, total_of):
        at = slice(ROWS_START + r * SUB, ROWS_START + (r + 1) * SUB)
        value = second_x[i, t, at, :] + (1.0 + carry + weight) * work[i, w, at, :]
        value = jnp.where(inside(t, ROWS_START + r * SUB), value - weight * total_of, 0.0)
        work[i, w, at, :] = value

    apply(*span(2), coarse_ref, WINDOW_COARSE, 2, 2, emit_start)

    def emit_middle(t, w, k, r, i, total_of):
        at = slice(ROWS_MIDDLE + r * SUB, ROWS_MIDDLE + (r + 1) * SUB)
        step = jnp.where(inside(t, ROWS_MIDDLE + r * SUB), fields[i, t, at, :] - total_of, 0.0)
        work[i, w, at, :] = work[i, w, at, :] + step
        second_x[i, t, at, :] = step

    apply(*span(1), middle_ref, WINDOW_MIDDLE, 2, 1, emit_middle)

    def emit_last(t, w, k, r, i, total_of):
        value = work[i, w, own, :] + carry * second_x[i, t, own, :]
        vel_ref[i, k] = value + weight * (fields[i, t, own, :] - total_of)

    apply(*span(0), middle_ref, WINDOW_LAST, 1, 1, emit_last, with_strips=False)


def on_device(rhs_velocity, rhs_pressure, layer_ids, visc_table, stencil):
    planes, rows, depth = rhs_pressure.shape
    assert rows == SUB and depth == LANES and planes * STRIP == LANES
    x_count, y_count, z_count = (lax.axis_size(n) for n in ("gx", "gy", "gz"))
    entries = jnp.transpose(stencil, (1, 2, 0))

    tile = jax.ShapeDtypeStruct((FIELDS, SUB, LANES), jnp.float32)
    vmem = pl.BlockSpec(memory_space=pltpu.VMEM)
    smem = pl.BlockSpec(memory_space=pltpu.SMEM)
    bands = pl.pallas_call(
        band_kernel,
        out_shape=tuple(
            jax.ShapeDtypeStruct((9, r * SUB, 27 * depth), jnp.float32)
            for r, depth in ((3, ROWS), (2, ROWS), (2, WINDOW), (2, WINDOW))
        ),
        in_specs=[smem],
        out_specs=(vmem,) * 4,
        compiler_params=pltpu.CompilerParams(vmem_limit_bytes=SMALL_VMEM),
        name="bands",
    )(pltpu.with_memory_space_constraint(entries, pltpu.HBM))
    main, z_first, z_second = pl.pallas_call(
        functools.partial(pack_kernel, planes),
        out_shape=(
            jax.ShapeDtypeStruct((FIELDS * (planes + 1), SUB, LANES), jnp.float32),
            tile,
            tile,
        ),
        in_specs=[pl.BlockSpec(memory_space=pltpu.HBM)] * 5,
        out_specs=(vmem, vmem, vmem),
        scratch_shapes=[
            pltpu.SMEM(visc_table.shape, visc_table.dtype),
            pltpu.SMEM(entries.shape, entries.dtype),
            pltpu.VMEM(rhs_velocity.shape, rhs_velocity.dtype),
            pltpu.VMEM(rhs_pressure.shape, rhs_pressure.dtype),
            pltpu.VMEM(layer_ids.shape, layer_ids.dtype),
            pltpu.SemaphoreType.DMA((5,)),
        ],
        compiler_params=pltpu.CompilerParams(vmem_limit_bytes=SMALL_VMEM),
        name="pack",
    )(
        *(
            pltpu.with_memory_space_constraint(v, pltpu.HBM)
            for v in (visc_table, entries, rhs_velocity, rhs_pressure, layer_ids)
        )
    )

    halo = matched(z_first, "gz", first_pairs(z_count))
    halo = halo + matched(z_second, ("gx", "gz"), second_pairs(x_count, z_count))
    inner = FIELDS * planes
    block = jnp.concatenate([main[:inner], main[inner:] + halo])

    paired = x_count == 2
    if paired:
        cut = (FIELDS - 1) * planes
        near = jnp.where(
            lax.axis_index("gx") == 0, block[inner - 2 : inner], block[cut : cut + 2]
        )
        sent = jnp.concatenate([block[:cut], near, block[inner:]])
        other = lax.ppermute(sent, "gx", [(0, 1), (1, 0)])
        near = [other[cut : cut + 2]] * (planes // 2)
        parts = [block, jnp.concatenate([other[:cut], *near, other[cut + 2 :]])]
    else:
        hops = -(-REACH // planes)
        parts = []
        for hop in range(-hops, hops + 1):
            pairs = [(i, i - hop) for i in range(x_count) if 0 <= i - hop < x_count]
            parts.append(block if hop == 0 else matched(block, "gx", pairs))
    blocks = len(parts)
    frame = jnp.stack(parts)

    message = jax.ShapeDtypeStruct((blocks, packed_rows(planes), LANES), jnp.float32)
    y_first, y_second = pl.pallas_call(
        functools.partial(message_kernel, planes, blocks),
        out_shape=(message, message),
        in_specs=[vmem] * blocks,
        out_specs=(vmem, vmem),
        compiler_params=pltpu.CompilerParams(vmem_limit_bytes=SMALL_VMEM),
        name="message",
    )(*parts)
    y_first = matched(y_first, "gy", first_pairs(y_count))
    y_second = matched(y_second, ("gx", "gy"), second_pairs(x_count, y_count))

    total = planes * blocks
    tiles = total + blocks
    f32 = jnp.float32
    return pl.pallas_call(
        functools.partial(cycle_kernel, planes, blocks, paired),
        out_shape=(
            jax.ShapeDtypeStruct(rhs_velocity.shape, f32),
            jax.ShapeDtypeStruct(rhs_pressure.shape, f32),
        ),
        in_specs=[vmem] * 7,
        out_specs=(vmem, vmem),
        scratch_shapes=[
            pltpu.VMEM((FIELDS, tiles, ROWS, LANES), f32),
            pltpu.VMEM((3, tiles + 2 * LEAD, ROWS, LANES), f32),
            pltpu.VMEM((2, (total // 2 + 2 * LEAD) * 9 * SUB, 2 * LANES), f32),
            pltpu.VMEM((tiles + 2, 9 * ROWS, LANES), f32),
            pltpu.VMEM((blocks, 3 * ROWS + 2 * SUB, LANES), f32),
            pltpu.VMEM((3, tiles, ROWS, LANES), f32),
            pltpu.VMEM((3, 2 * tiles, 2 * SUB, LANES), f32),
            pltpu.VMEM((tiles + 2 * LEAD, ROWS, LANES), f32),
        ],
        compiler_params=pltpu.CompilerParams(vmem_limit_bytes=CYCLE_VMEM),
        name="cycle",
    )(frame, y_first, y_second, *bands)


def solution(mesh):
    placed = (P(None, "gx", "gy", "gz"), P("gx", "gy", "gz"), P("gx", "gy", "gz"), P(), P())
    return jax.shard_map(
        on_device,
        mesh=mesh,
        in_specs=placed,
        out_specs=(P(None, "gx", "gy", "gz"), P("gx", "gy", "gz")),
        check_vma=False,
    )
```
